32 devices in a mesh: layer: 4 (over z), facet: 8 (over y, x, core).
Axes of the slice: x: 2, y: 2, z: 4, core: 2. Of those that a mesh axis runs over, the one named last changes fastest.
Arguments:
- model_strip: bfloat16 [8, 2, 64, 8192], P('facet', None, None, 'layer'), may hold values from -6 to 6
- screen_angle: bfloat16 [4, 8, 64, 8192], P('layer', 'facet'), may hold values from -3.140625 to 3.140625
- facet_window: float32 [8, 8192], P('facet'), may hold values from 0.04 to 0.16
- facet_shift: int32 [8], P('facet'), may hold values from 0 to 8191
- kernel_taps: float32 [7], replicated, may hold values from 0.2 to 0.6
- plane_angle: float32 [4, 8], P('layer'), may hold values from -3.140625 to 3.140625
- u_cell: int32 [4, 128, 512], P('layer', 'facet'), may hold values from 0 to 63
- v_cell: int32 [4, 128, 512], P('layer', 'facet'), may hold values from 0 to 63
- w_plane: int32 [4, 128, 512], P('layer', 'facet'), may hold values from 0 to 7
- observed: float32 [4, 128, 2, 512], P('layer', 'facet'), may hold values from -6 to 6
Outputs:
- residual: float32 [4, 128, 2, 512], P('layer', 'facet')
- gradient: float32 [8, 2, 64, 8192], P('facet', None, None, 'layer')
The draws below stay inside these ranges and needn't reach their ends.
All inputs are finite; a program needn't handle non-finite values.
Results may differ from the reference program's by a relative error of at most 0.009.
Values may be sent and summed in bfloat16 or wider, within the bound.
A program may use at most 64 MiB of HBM per device.

```python
import math
import jax
import jax.numpy as jnp
from jax import lax

STRIP_LEN = 8192
SUB_ROWS = 64
STRIP_COLS = 64
VIS = 512
PLANES = 8
TAPS = 7
SUBGRIDS = 128
LAYERS = 4
FACETS = 8


def touch_ends(entries, rng, low, largest):
    extent = entries.shape
    place = [jax.random.randint(jax.random.fold_in(rng, axis), (), 0, extent[axis]) for axis in range(len(extent))]
    entries = entries.at[tuple(place)].set(low)
    longest = extent.index(max(extent))
    place[longest] = (place[longest] + 1) % extent[longest]
    return entries.at[tuple(place)].set(largest)


def steps_of(stream_key, extent, shards, low, high):
    gain, own = 1.0, jax.random.fold_in(stream_key, 6)
    for dim, shards_of in shards:
        draws = jnp.exp(jax.random.uniform(jax.random.fold_in(own, dim), (shards_of,), jnp.float32, low / len(shards), high / len(shards)))
        gain = gain * jnp.repeat(draws, extent[dim] // shards_of).reshape([-1 if axis == dim else 1 for axis in range(len(extent))])
    return gain


def noise(stream_key, extent, deviation, reach, cuts=(), kind=jnp.bfloat16):
    factor_of = steps_of(stream_key, extent, cuts, -0.22, 0.18) if cuts else 1.0
    array = jax.random.normal(stream_key, extent, jnp.float32) * deviation * factor_of
    return jnp.minimum(jnp.maximum(array, -reach), reach).astype(kind)


def setup_inputs(seed: int = 0) -> dict:
    arg_keys = jax.random.split(jax.random.key(seed), 11)
    return {
        "model_strip": noise(arg_keys[0], (FACETS, 2, STRIP_COLS, STRIP_LEN), 1.0, 6.0, ((0, 8), (3, 4))),
        "screen_angle": jnp.clip(jax.random.uniform(arg_keys[1], (LAYERS, FACETS, STRIP_COLS, STRIP_LEN), jnp.float32, -3.140625, 3.140625), -3.140625, 3.140625).astype(jnp.bfloat16),
        "facet_window": jnp.clip(jnp.exp(math.log(0.16) - 1.3862944 * jax.random.uniform(arg_keys[2], (FACETS, STRIP_LEN), jnp.float32) ** steps_of(arg_keys[2], (FACETS, STRIP_LEN), ((0, 8),), -0.2, 0.2)), 0.04, 0.16),
        "facet_shift": touch_ends(jax.random.randint(arg_keys[3], (FACETS,), 0, STRIP_LEN), jax.random.fold_in(arg_keys[3], 1), 0, STRIP_LEN - 1).astype(jnp.int32),
        "kernel_taps": jnp.clip(jax.random.uniform(arg_keys[4], (TAPS,), jnp.float32, 0.2, 0.6), 0.2, 0.6),
        "plane_angle": jnp.clip(jax.random.uniform(arg_keys[5], (LAYERS, PLANES), jnp.float32, -3.140625, 3.140625), -3.140625, 3.140625),
        "u_cell": touch_ends(jax.random.randint(arg_keys[6], (LAYERS, SUBGRIDS, VIS), 0, SUB_ROWS), jax.random.fold_in(arg_keys[6], 1), 0, SUB_ROWS - 1).astype(jnp.int32),
        "v_cell": touch_ends(jax.random.randint(arg_keys[7], (LAYERS, SUBGRIDS, VIS), 0, STRIP_COLS), jax.random.fold_in(arg_keys[7], 1), 0, STRIP_COLS - 1).astype(jnp.int32),
        "w_plane": touch_ends(jax.random.randint(arg_keys[8], (LAYERS, SUBGRIDS, VIS), 0, PLANES), jax.random.fold_in(arg_keys[8], 1), 0, PLANES - 1).astype(jnp.int32),
        "observed": noise(arg_keys[9], (LAYERS, SUBGRIDS, 2, VIS), 1.0, 6.0, ((0, 4), (1, 8)), jnp.float32),
    }


back_gain = 8.0

def fourier_table(length):
    positions = jnp.arange(length, dtype=jnp.int32)
    turn_count = positions[:, None] * positions[None, :] % length
    angles = 2.0 * math.pi / length * turn_count.astype(jnp.float32)
    norm_scale = 1.0 / math.sqrt(length)
    return (jnp.stack([jnp.cos(angles), -jnp.sin(angles)]) * norm_scale).astype(jnp.bfloat16)

def twiddle():
    low_index = jnp.arange(SUB_ROWS, dtype=jnp.int32)
    high_index = jnp.arange(SUBGRIDS, dtype=jnp.int32)
    turn_count = low_index[:, None] * high_index[None, :] % STRIP_LEN
    angles = 2.0 * math.pi / STRIP_LEN * turn_count.astype(jnp.float32)
    return (jnp.cos(angles), -jnp.sin(angles))

def facet_factor(window, shift_cells):
    positions = jnp.arange(STRIP_LEN, dtype=jnp.int32)
    turn_count = positions * shift_cells.astype(jnp.int32) % STRIP_LEN
    angles = 2.0 * math.pi / STRIP_LEN * turn_count.astype(jnp.float32)
    factor_real = (window * jnp.cos(angles)).reshape(SUBGRIDS, SUB_ROWS, 1)
    factor_imag = (-window * jnp.sin(angles)).reshape(SUBGRIDS, SUB_ROWS, 1)
    return (factor_real, factor_imag)

def forward(screened, window, shift_cells):
    grid_view = screened.reshape(2, STRIP_COLS, SUB_ROWS, SUBGRIDS).astype(jnp.float32)
    section_one = jnp.einsum('tka,pcab->tpckb', fourier_table(SUB_ROWS).astype(jnp.float32), grid_view)
    real_part = section_one[0, 0] - section_one[1, 1]
    imag_part = section_one[0, 1] + section_one[1, 0]
    twist_real, twist_imag = twiddle()
    mixed = jnp.stack([real_part * twist_real - imag_part * twist_imag, real_part * twist_imag + imag_part * twist_real]).astype(jnp.bfloat16)
    section_two = jnp.einsum('tjb,pckb->tpjkc', fourier_table(SUBGRIDS).astype(jnp.float32), mixed.astype(jnp.float32))
    spec_real = section_two[0, 0] - section_two[1, 1]
    spec_imag = section_two[0, 1] + section_two[1, 0]
    factor_real, factor_imag = facet_factor(window, shift_cells)
    return jnp.concatenate([spec_real * factor_real - spec_imag * factor_imag, spec_real * factor_imag + spec_imag * factor_real], axis=2).astype(jnp.bfloat16)

def backward(all_grids, window, shift_cells, screen_phase):
    values = all_grids.astype(jnp.float32)
    grid_real = values[:, :, :STRIP_COLS]
    grid_imag = values[:, :, STRIP_COLS:]
    factor_real, factor_imag = facet_factor(window, shift_cells)
    spectral = jnp.stack([grid_real * factor_real + grid_imag * factor_imag, grid_imag * factor_real - grid_real * factor_imag]).astype(jnp.bfloat16)
    section_two = jnp.einsum('tjb,pjkc->tpckb', fourier_table(SUBGRIDS).astype(jnp.float32), spectral.astype(jnp.float32))
    half_real = section_two[0, 0] + section_two[1, 1]
    half_imag = section_two[0, 1] - section_two[1, 0]
    twist_real, twist_imag = twiddle()
    mixed = jnp.stack([half_real * twist_real + half_imag * twist_imag, half_imag * twist_real - half_real * twist_imag]).astype(jnp.bfloat16)
    section_one = jnp.einsum('tka,pckb->tpcab', fourier_table(SUB_ROWS).astype(jnp.float32), mixed.astype(jnp.float32))
    image_real = (section_one[0, 0] + section_one[1, 1]).reshape(STRIP_COLS, STRIP_LEN)
    image_imag = (section_one[0, 1] - section_one[1, 0]).reshape(STRIP_COLS, STRIP_LEN)
    phases = screen_phase.astype(jnp.float32)
    cosine = jnp.cos(phases)
    sine_part = jnp.sin(phases)
    return back_gain * jnp.stack([image_real * cosine + image_imag * sine_part, image_imag * cosine - image_real * sine_part])

def spread(cell_index, length, kernel_taps):
    tap_count = kernel_taps.shape[0]
    offset = (jnp.arange(length, dtype=jnp.int32)[None, :] - cell_index[:, None]) % length
    wanted = (jnp.arange(tap_count, dtype=jnp.int32) - tap_count // 2) % length
    matches = (offset[:, :, None] == wanted[None, None, :]).astype(jnp.float32)
    return lax.optimization_barrier(jnp.sum(matches * kernel_taps, axis=2))

def degrid(subgrid, row_cells, column_cells, plane, observed_vis, angle_table, kernel_taps):
    row_weights = spread(row_cells, SUB_ROWS, kernel_taps)
    column_weights = spread(column_cells, STRIP_COLS, kernel_taps)
    kernel_rows = jnp.dot(row_weights, subgrid, precision=lax.Precision.HIGHEST)
    model_real = lax.optimization_barrier(jnp.sum(kernel_rows[:, :STRIP_COLS] * column_weights, axis=1))
    model_imag = lax.optimization_barrier(jnp.sum(kernel_rows[:, STRIP_COLS:] * column_weights, axis=1))
    plane_pick = (plane[:, None] == jnp.arange(PLANES, dtype=jnp.int32)[None, :]).astype(jnp.float32)
    phase_angle = lax.optimization_barrier(jnp.sum(plane_pick * angle_table[None, :], axis=1))
    cosine = jnp.cos(phase_angle)
    sine_part = jnp.sin(phase_angle)
    residual_real = observed_vis[0] - (model_real * cosine - model_imag * sine_part)
    residual_imag = observed_vis[1] - (model_real * sine_part + model_imag * cosine)
    weighted = jnp.stack([residual_real * cosine + residual_imag * sine_part, residual_imag * cosine - residual_real * sine_part])
    spread_cols = jnp.concatenate([weighted[0][:, None] * column_weights, weighted[1][:, None] * column_weights], axis=1)
    adjoint = jnp.dot(row_weights.T, spread_cols, precision=lax.Precision.HIGHEST)
    return (jnp.stack([residual_real, residual_imag]), adjoint.astype(jnp.bfloat16))

def reference(model_strip, screen_angle, facet_window, facet_shift, kernel_taps, plane_angle, u_cell, v_cell, w_plane, observed):

    def screen_strip(layer_index, facet_index):
        strip_values = model_strip[facet_index].astype(jnp.float32)
        phases = screen_angle[layer_index, facet_index].astype(jnp.float32)
        cosine = jnp.cos(phases)
        sine_part = jnp.sin(phases)
        return jnp.stack([strip_values[0] * cosine - strip_values[1] * sine_part, strip_values[0] * sine_part + strip_values[1] * cosine]).astype(jnp.bfloat16)

    def layer_grids(layer_index):

        def add_facet(running, facet_index):
            screened = screen_strip(layer_index, facet_index)
            contrib = forward(screened, facet_window[facet_index], facet_shift[facet_index])
            return (running + contrib.astype(jnp.float32), None)
        start = jnp.zeros((SUBGRIDS, SUB_ROWS, 2 * STRIP_COLS), jnp.float32)
        running, _ = lax.scan(add_facet, start, jnp.arange(FACETS, dtype=jnp.int32))
        return running
    grids = lax.map(layer_grids, jnp.arange(LAYERS, dtype=jnp.int32))
    angle_rows = jnp.repeat(plane_angle, SUBGRIDS, axis=0)

    def one_subgrid(inputs):
        subgrid, row_cells, column_cells, plane, observed_vis, angle_table = inputs
        return degrid(subgrid, row_cells, column_cells, plane, observed_vis, angle_table, kernel_taps)
    residual, adjoint = lax.map(one_subgrid, (grids.reshape(LAYERS * SUBGRIDS, SUB_ROWS, 2 * STRIP_COLS), u_cell.reshape(LAYERS * SUBGRIDS, VIS), v_cell.reshape(LAYERS * SUBGRIDS, VIS), w_plane.reshape(LAYERS * SUBGRIDS, VIS), observed.reshape(LAYERS * SUBGRIDS, 2, VIS), angle_rows))
    residual = residual.reshape(LAYERS, SUBGRIDS, 2, VIS)
    adjoint = adjoint.reshape(LAYERS, SUBGRIDS, SUB_ROWS, 2 * STRIP_COLS)

    def facet_gradient(facet_index):

        def add_layer(running, layer_index):
            term = backward(adjoint[layer_index], facet_window[facet_index], facet_shift[facet_index], screen_angle[layer_index, facet_index])
            rounded = lax.optimization_barrier(term.astype(jnp.bfloat16))
            return (running + rounded.astype(jnp.float32), None)
        start = jnp.zeros((2, STRIP_COLS, STRIP_LEN), jnp.float32)
        running, _ = lax.scan(add_layer, start, jnp.arange(LAYERS, dtype=jnp.int32))
        return running
    gradient = lax.map(facet_gradient, jnp.arange(FACETS, dtype=jnp.int32))
    return (residual, gradient)
```

```python
import functools
import math

import jax
import jax.numpy as jnp
import numpy as np
from jax import lax
from jax.experimental import pallas as pl
from jax.experimental.pallas import tpu as pltpu
from jax.sharding import PartitionSpec as P

MESH = pl.DeviceIdType.MESH
BACK_GAIN = 8.0
CHUNKS = 8
MOVED = 3


def _fit(values, degree):
    nodes = np.cos(np.pi * (np.arange(64) + 0.5) / 64)
    y = (nodes + 1.0) * 0.5 * np.pi**2
    cheb = np.polynomial.chebyshev.Chebyshev.fit(y, values(np.sqrt(y)), degree, domain=[0, np.pi**2])
    return [float(v) for v in cheb.convert(kind=np.polynomial.Polynomial).coef]


COS = _fit(np.cos, 8)
SIN = _fit(lambda x: np.sinc(x / np.pi), 7)


def cos_sin(x):
    y = x * x
    c = jnp.full_like(y, COS[-1])
    for v in COS[-2::-1]:
        c = c * y + v
    s = jnp.full_like(y, SIN[-1])
    for v in SIN[-2::-1]:
        s = s * y + v
    return c, s * x


def dft(length):
    k = np.arange(length)
    angles = 2.0 * np.pi * ((k[:, None] * k[None, :]) % length) / length
    scale = 1.0 / math.sqrt(length)
    return np.cos(angles) * scale, -np.sin(angles) * scale


def barrier_line(i, n):
    sem = pltpu.get_barrier_semaphore()

    @pl.when(i > 0)
    def _():
        pl.semaphore_signal(sem, inc=1, device_id={"layer": i - 1}, device_id_type=MESH)

    @pl.when(i < n - 1)
    def _():
        pl.semaphore_signal(sem, inc=1, device_id={"layer": i + 1}, device_id_type=MESH)

    peers = jnp.where(i > 0, 1, 0) + jnp.where(i < n - 1, 1, 0)
    pl.semaphore_wait(sem, peers)


def forward_kernel(n, x_ref, ang_ref, f1_ref, g_ref, tw_ref, fac_ref, out_ref, buf, send_sem, recv_sem, own_sem):
    i = lax.axis_index("layer")
    cq = x_ref.shape[0] // CHUNKS
    subgrids = g_ref.shape[0] // 2
    rows = f1_ref.shape[0] // 2
    barrier_line(i, n)
    own = pltpu.make_async_copy(x_ref, buf.at[i], own_sem)
    own.start()

    def copy(direction, s, q):
        step = 1 if direction == 0 else -1
        origin = jnp.clip(i - step * s, 0, n - 1)
        cols = pl.ds(q * cq, cq)
        src = x_ref.at[cols] if s == 0 else buf.at[origin, cols]
        return pltpu.make_async_remote_copy(
            src_ref=src,
            dst_ref=buf.at[origin, cols],
            send_sem=send_sem.at[direction, s, q],
            recv_sem=recv_sem.at[direction, s, q],
            device_id={"layer": jnp.clip(i + step, 0, n - 1)},
            device_id_type=MESH,
        )

    def sends(direction, s):
        if direction == 0:
            return (i - s >= 0) & (i < n - 1)
        return (i + s <= n - 1) & (i > 0)

    def gets(direction, s):
        return i - 1 - s >= 0 if direction == 0 else i + 1 + s <= n - 1

    def compute(q):
        twr, twi = tw_ref[0], tw_ref[1]
        facr, faci = fac_ref[0], fac_ref[1]
        for pair in range(cq // 2):
            halves = []
            for c in (2 * pair, 2 * pair + 1):
                col = q * cq + c
                xr = jnp.concatenate([buf[l, col, 0] for l in range(n)], axis=0).astype(jnp.float32)
                xi = jnp.concatenate([buf[l, col, 1] for l in range(n)], axis=0).astype(jnp.float32)
                cosine, sine = cos_sin(ang_ref[col].astype(jnp.float32))
                x = jnp.concatenate([xr * cosine - xi * sine, xr * sine + xi * cosine], axis=0)
                h = jnp.dot(f1_ref[...], x.astype(jnp.bfloat16), preferred_element_type=jnp.float32)
                hr, hi = h[:rows], h[rows:]
                halves.append(
                    jnp.concatenate([hr * twr - hi * twi, hr * twi + hi * twr], axis=1).astype(jnp.bfloat16)
                )
            both = jnp.concatenate(halves, axis=0)
            spec = lax.dot_general(
                g_ref[...], both, (((1,), (1,)), ((), ())), preferred_element_type=jnp.float32
            )
            sr, si = spec[:subgrids], spec[subgrids:]
            at = q * (cq // 2) + pair
            out_ref[0, at] = (sr * facr - si * faci).astype(jnp.bfloat16)
            out_ref[1, at] = (sr * faci + si * facr).astype(jnp.bfloat16)

    def body(t, carry):
        @pl.when(t < CHUNKS)
        def _():
            for d in range(2):
                @pl.when(sends(d, 0))
                def _():
                    copy(d, 0, t).start()

        for s in range(n - 1):
            q = t - 1 - s
            @pl.when((q >= 0) & (q < CHUNKS))
            def _():
                for d in range(2):
                    @pl.when(gets(d, s))
                    def _():
                        copy(d, s, q).wait_recv()
                        if s + 1 < n - 1:
                            @pl.when(sends(d, s + 1))
                            def _():
                                copy(d, s + 1, q).start()

        @pl.when(t >= n - 1)
        def _():
            compute(t - (n - 1))

        return carry

    own.wait()
    lax.fori_loop(0, CHUNKS + n - 1, body, 0)

    def drain(q, carry):
        for d in range(2):
            for s in range(n - 1):
                @pl.when(sends(d, s))
                def _():
                    copy(d, s, q).wait_send()
        return carry

    lax.fori_loop(0, CHUNKS, drain, 0)


def backward_kernel(n, a_ref, ang_ref, g_ref, f2_ref, tw_ref, fac_ref, out_ref, term, sbuf, rbuf, send_sem, recv_sem):
    i = lax.axis_index("layer")
    cols = ang_ref.shape[0]
    cq = cols // CHUNKS
    fine = g_ref.shape[0] // 2
    rows = ang_ref.shape[1]
    part = rows // n
    barrier_line(i, n)

    def copy(direction, j, q):
        where = pl.ds(q * cq, cq)
        step = 1 if direction == 0 else -1
        return pltpu.make_async_remote_copy(
            src_ref=sbuf.at[direction, j, where],
            dst_ref=rbuf.at[direction, j, where],
            send_sem=send_sem.at[direction, j, q],
            recv_sem=recv_sem.at[direction, j, q],
            device_id={"layer": jnp.clip(i + step, 0, n - 1)},
            device_id_type=MESH,
        )

    def behind(direction):
        return i > 0 if direction == 0 else i < n - 1

    def compute(q):
        twr, twi = tw_ref[0], tw_ref[1]
        facr, faci = fac_ref[0], fac_ref[1]
        for pair in range(cq // 2):
            at = q * (cq // 2) + pair
            ar = a_ref[0, at].astype(jnp.float32)
            ai = a_ref[1, at].astype(jnp.float32)
            b = jnp.concatenate([ar * facr + ai * faci, ai * facr - ar * faci], axis=0).astype(jnp.bfloat16)
            h = jnp.dot(g_ref[...], b, preferred_element_type=jnp.float32)
            hr, hi = h[:fine], h[fine:]
            mixed = jnp.concatenate([hr * twr + hi * twi, hi * twr - hr * twi], axis=1).astype(jnp.bfloat16)
            image = lax.dot_general(
                f2_ref[...], mixed, (((1,), (1,)), ((), ())), preferred_element_type=jnp.float32
            )
            for c in range(2):
                col = q * cq + 2 * pair + c
                ir = image[2 * c * rows : (2 * c + 1) * rows]
                ii = image[(2 * c + 1) * rows : (2 * c + 2) * rows]
                cosine, sine = cos_sin(ang_ref[col].astype(jnp.float32))
                tr = (BACK_GAIN * (ir * cosine + ii * sine)).astype(jnp.bfloat16)
                ti = (BACK_GAIN * (ii * cosine - ir * sine)).astype(jnp.bfloat16)
                for l in range(n):
                    term[l, col, 0] = tr[l * part : (l + 1) * part]
                    term[l, col, 1] = ti[l * part : (l + 1) * part]

    def relay(direction, j, q):
        where = pl.ds(q * cq, cq)

        @pl.when(behind(direction))
        def _():
            copy(direction, j, q).wait_recv()
            total = term[j, where].astype(jnp.float32) + rbuf[direction, j, where].astype(jnp.float32)
            sbuf[direction, j, where] = total.astype(jnp.bfloat16)

        @pl.when(jnp.logical_not(behind(direction)))
        def _():
            sbuf[direction, j, where] = term[j, where]

        copy(direction, j, q).start()

    def body(t, carry):
        @pl.when(t < CHUNKS)
        def _():
            compute(t)

        for direction in range(2):
            q = t - i if direction == 0 else t - (n - 1 - i)

            @pl.when((q >= 0) & (q < CHUNKS))
            def _():
                for d in range(n - 1, 0, -1):
                    j = i + d if direction == 0 else i - d

                    @pl.when((j < n) & (j >= 0))
                    def _():
                        relay(direction, j, q)

        last = t - (n - 1)

        @pl.when(last >= 0)
        def _():
            where = pl.ds(last * cq, cq)
            out_ref[where] = term[i, where].astype(jnp.float32)
            for direction in range(2):
                @pl.when(behind(direction))
                def _():
                    copy(direction, i, last).wait_recv()
                    out_ref[where] += rbuf[direction, i, where].astype(jnp.float32)

        return carry

    lax.fori_loop(0, CHUNKS + n - 1, body, 0)

    def drain(q, carry):
        for direction in range(2):
            for d in range(1, n):
                j = i + d if direction == 0 else i - d

                @pl.when((j < n) & (j >= 0))
                def _():
                    copy(direction, j, q).wait_send()
        return carry

    lax.fori_loop(0, CHUNKS, drain, 0)


def facet_factor(window, shift_cells, subgrids):
    length = window.shape[0]
    rows = length // subgrids
    grid = window.reshape(subgrids, rows)
    grid = jnp.concatenate([grid, grid], axis=1)
    high = lax.broadcasted_iota(jnp.int32, grid.shape, 0)
    low = lax.broadcasted_iota(jnp.int32, grid.shape, 1) % rows
    turn_count = (high * rows + low) * shift_cells % length
    angles = 2.0 * math.pi / length * turn_count.astype(jnp.float32)
    return jnp.stack([grid * jnp.cos(angles), -grid * jnp.sin(angles)])


def spread(cells, length, taps):
    count = taps.shape[0]
    lanes = jnp.arange(length, dtype=jnp.int32)
    offset = (lanes - cells[..., None] + (count // 2 + length)) % length
    out = jnp.zeros(offset.shape, jnp.float32)
    for t in range(count):
        out = out + jnp.where(offset == t, taps[t], 0.0)
    return out


def middle(grids, u, v, plane, observed, angle, taps, rows, cols):
    row_weights = spread(u, rows, taps)
    column_weights = spread(v, cols, taps).astype(jnp.bfloat16)
    picked = jnp.einsum("sjc,sck->sjk", column_weights, grids.astype(jnp.bfloat16), preferred_element_type=jnp.float32)
    model_real = jnp.sum(picked[..., :rows] * row_weights, axis=2)
    model_imag = jnp.sum(picked[..., rows:] * row_weights, axis=2)
    pick = plane[..., None] == jnp.arange(angle.shape[0], dtype=jnp.int32)
    cosine = jnp.sum(jnp.where(pick, jnp.cos(angle), 0.0), axis=2)
    sine = jnp.sum(jnp.where(pick, jnp.sin(angle), 0.0), axis=2)
    res_real = observed[:, 0] - (model_real * cosine - model_imag * sine)
    res_imag = observed[:, 1] - (model_real * sine + model_imag * cosine)
    w_real = res_real * cosine + res_imag * sine
    w_imag = res_imag * cosine - res_real * sine
    spread_rows = jnp.concatenate(
        [w_real[..., None] * row_weights, w_imag[..., None] * row_weights], axis=2
    ).astype(jnp.bfloat16)
    adjoint = jnp.einsum("sjc,sjk->sck", column_weights, spread_rows, preferred_element_type=jnp.float32)
    return jnp.stack([res_real, res_imag], axis=1), adjoint.astype(jnp.bfloat16)


def fused_kernel(
    n, moved, x_ref, ang_ref, win_ref, u_ref, v_ref, plane_ref, obs_ref, f1_ref, g1_ref, tw_ref, g2_ref, f2_ref, tw2_ref,
    taps_ref, pang_ref, shift_ref, res_ref, out_ref,
    buf, angb, cs, fac, tmpx, tmpa, contrib, r0, acc0, r1, acc1, r2, outbox, inbox, fin, adj, phase, row_table, column_table,
    every, term, sbuf, rbuf, otmp,
    fs, fr, angs, angr, s0, d0, s1, d1, s2, d2, xs, xr, ys, yr, sa, da, sb, db, sc, dc, bs, br,
):
    cols, rows = angb.shape[0] - cs_extra(moved, angb.shape[0]), angb.shape[1]
    lanes = 2 * rows
    subgrids = g1_ref.shape[0] // 2
    block = rows // n
    per, vis = u_ref.shape
    pairs = cols // 2
    cq = cols // CHUNKS
    pq = cq // 2
    i = lax.axis_index("layer")
    f = lax.axis_index("facet")
    core = lax.rem(f, 2)
    chip = lax.div(f, 2)
    bits = (lax.rem(chip, 2), lax.div(chip, 2))
    other = f + 1 - 2 * core
    middle_layer = (i >= 1) & (i <= n - 2)

    def flip(b):
        return f + (1 - 2 * bits[b]) * (2 * (1 + b))

    def near(step):
        return jnp.clip(i + step, 0, n - 1)

    inner = jnp.where(i == 0, 1, n - 2)
    outer = jnp.where(i == 1, 0, n - 1)

    barrier = pltpu.get_barrier_semaphore()
    for peer in (other, flip(0), flip(1)):
        pl.semaphore_signal(barrier, inc=1, device_id={"facet": peer}, device_id_type=MESH)

    @pl.when(i > 0)
    def _():
        pl.semaphore_signal(barrier, inc=1, device_id={"layer": i - 1}, device_id_type=MESH)

    @pl.when(i < n - 1)
    def _():
        pl.semaphore_signal(barrier, inc=1, device_id={"layer": i + 1}, device_id_type=MESH)

    pl.semaphore_wait(barrier, 3 + jnp.where(i > 0, 1, 0) + jnp.where(i < n - 1, 1, 0))

    def is_moved(q):
        return (lax.rem(q, 2) == 1) & (q < 2 * moved)

    def bottom(q):
        return jnp.where(is_moved(q), 1, 0)

    def top(q):
        return jnp.where(is_moved(q), n - 2, n - 1)

    def has_own(q):
        return (i >= bottom(q)) & (i <= top(q))

    def has_extra(q):
        return middle_layer & is_moved(q)

    def remote(src, dst, send, recv, axis, device):
        return pltpu.make_async_remote_copy(
            src_ref=src, dst_ref=dst, send_sem=send, recv_sem=recv, device_id={axis: device}, device_id_type=MESH
        )

    def chunk(q):
        return pl.ds(pl.multiple_of(q * cq, cq), cq)

    def copy(direction, s, q):
        step = 1 if direction == 0 else -1
        origin = jnp.clip(i - step * s, 0, n - 1)
        ref = buf.at[origin, chunk(q)]
        return remote(ref, ref, fs.at[direction, s, q], fr.at[direction, s, q], "layer", near(step))

    def sends(direction, s, q):
        if direction == 0:
            return (i - s >= 0) & (i + 1 <= top(q))
        return (i + s <= n - 1) & (i - 1 >= bottom(q))

    def gets(direction, s, q):
        if direction == 0:
            return (i - 1 - s >= 0) & (i <= top(q))
        return (i + 1 + s <= n - 1) & (i >= bottom(q))

    def send_own(q):
        for d in range(2):
            @pl.when(sends(d, 0, q))
            def _():
                copy(d, 0, q).start()

    def angle_copy(m):
        src = angb.at[chunk(2 * m + 1)]
        dst = angb.at[chunk(CHUNKS + m)]
        return remote(src, dst, angs.at[m], angr.at[m], "layer", inner)

    def relayout(g, carry):
        at = pl.ds(pl.multiple_of(g * 2 * cq, 2 * cq), 2 * cq)
        for p in range(2):
            v = x_ref[p, at, :].astype(jnp.float32)
            for m in range(block):
                tmpx[p, pl.ds(m, 2 * cq, stride=block), :] = v[:, m * subgrids : (m + 1) * subgrids]
            buf[i, at, p] = tmpx[p].reshape(2 * cq, block, subgrids).astype(jnp.bfloat16)

        @pl.when(jnp.logical_not(middle_layer))
        def _():
            send_own(2 * g)
            send_own(2 * g + 1)

        @pl.when(middle_layer & (g == 0))
        def _():
            send_own(0)

        for m in range(rows):
            piece = ang_ref[at, m * subgrids : (m + 1) * subgrids].astype(jnp.float32)
            tmpa[pl.ds(m, 2 * cq, stride=rows), :] = piece
        angb[at] = tmpa[...].reshape(2 * cq, rows, subgrids).astype(jnp.bfloat16)

        if moved:
            @pl.when(jnp.logical_not(middle_layer) & (g < moved))
            def _():
                angle_copy(g).start()

        return carry

    lax.fori_loop(0, CHUNKS // 2, relayout, 0)

    window = win_ref[...]
    rolled = pltpu.roll(window, rows, axis=1)
    left = lax.broadcasted_iota(jnp.int32, window.shape, 1) < rows
    fac[0, pl.ds(0, subgrids // 2, stride=2), :] = jnp.where(left, window, rolled)
    fac[0, pl.ds(1, subgrids // 2, stride=2), :] = jnp.where(left, rolled, window)
    grid = fac[0]
    length = subgrids * rows
    high = lax.broadcasted_iota(jnp.int32, grid.shape, 0)
    low = lax.broadcasted_iota(jnp.int32, grid.shape, 1)
    low = jnp.where(low < rows, low, low - rows)
    turns = lax.rem((high * rows + low) * shift_ref[0], length)
    turns = jnp.where(turns * 2 >= length, turns - length, turns)
    cosine, sine = cos_sin(turns.astype(jnp.float32) * (2.0 * math.pi / length))
    fac[0] = grid * cosine
    fac[1] = -grid * sine

    plane = plane_ref[...]
    angle = jnp.zeros(plane.shape, jnp.float32)
    for k in range(pang_ref.shape[1]):
        angle = jnp.where(plane == k, pang_ref[0, k], angle)
    cosine, sine = cos_sin(angle)
    phase[0] = cosine
    phase[1] = sine

    def weights(cells, position, size):
        count = taps_ref.shape[0]
        offset = position - cells + count // 2
        offset = jnp.where(offset < 0, offset + size, jnp.where(offset >= size, offset - size, offset))
        out = jnp.zeros(offset.shape, jnp.float32)
        for t in range(count):
            out = jnp.where(offset == t, taps_ref[t], out)
        return out

    def prepare(s):
        at = pl.ds(s, 1)
        row = lax.broadcasted_iota(jnp.int32, (rows, vis), 0)
        half = lax.broadcasted_iota(jnp.int32, (pairs, vis), 0)
        col = jnp.concatenate([2 * half, 2 * half + 1], axis=0)
        row_table[s] = weights(u_ref[at, :], row, rows)
        column_table[s] = weights(v_ref[at, :], col, cols).astype(jnp.bfloat16)

    def place(p, device):
        b0, b1 = (device // 2) % 2, device // 4
        return (b0 * 2 + b1) if p == 0 else (b1 * 2 + b0)

    def compute_forward(q, unit):
        twr, twi = tw_ref[0], tw_ref[1]
        facr, faci = fac[0], fac[1]
        base = chunk(unit).start
        for pair in range(pq):
            halves = []
            for c in (2 * pair, 2 * pair + 1):
                col = q * cq + c
                xr_ = jnp.concatenate([buf[l, col, 0] for l in range(n)], axis=0).astype(jnp.float32)
                xi_ = jnp.concatenate([buf[l, col, 1] for l in range(n)], axis=0).astype(jnp.float32)
                cosine, sine = cos_sin(angb[base + c].astype(jnp.float32))
                cs[base + c, 0] = cosine
                cs[base + c, 1] = sine
                x = jnp.concatenate([xr_ * cosine - xi_ * sine, xr_ * sine + xi_ * cosine], axis=0)
                h = jnp.dot(f1_ref[...], x.astype(jnp.bfloat16), preferred_element_type=jnp.float32)
                hr, hi = h[:rows], h[rows:]
                halves.append(
                    jnp.concatenate([hr * twr - hi * twi, hr * twi + hi * twr], axis=1).astype(jnp.bfloat16)
                )
            both = jnp.concatenate(halves, axis=0)
            spec = lax.dot_general(
                g1_ref[...], both, (((1,), (1,)), ((), ())), preferred_element_type=jnp.float32
            )
            sr, si = spec[:subgrids], spec[subgrids:]
            parts = ((sr * facr - si * faci).astype(jnp.bfloat16), (sr * faci + si * facr).astype(jnp.bfloat16))
            for p in range(2):
                for device in range(8):
                    contrib[unit, device % 2, p, place(p, device), pair * per : (pair + 1) * per] = parts[p][
                        device * per : (device + 1) * per
                    ]

    def stage0(unit):
        return remote(contrib.at[unit, 1 - core], r0.at[unit], s0.at[unit], d0.at[unit], "facet", other)

    def stage1(unit, p):
        src = acc0.at[unit, p, pl.ds((1 - bits[p]) * 2, 2)]
        return remote(src, r1.at[unit, p], s1.at[unit, p], d1.at[unit, p], "facet", flip(p))

    def stage2(unit, p):
        src = acc1.at[unit, p, 1 - bits[1 - p]]
        return remote(src, r2.at[unit, p], s2.at[unit, p], d2.at[unit, p], "facet", flip(1 - p))

    def result(m):
        return remote(outbox.at[m], inbox.at[m], xs.at[m], xr.at[m], "layer", jnp.where(middle_layer, outer, inner))

    def add0(unit):
        stage0(unit).wait_recv()
        for p in range(2):
            total = contrib[unit, core, p].astype(jnp.float32) + r0[unit, p].astype(jnp.float32)
            acc0[unit, p] = total.astype(jnp.bfloat16)
            stage1(unit, p).start()

    def add1(unit):
        for p in range(2):
            stage1(unit, p).wait_recv()
            mine = acc0[unit, p, pl.ds(bits[p] * 2, 2)].astype(jnp.float32)
            acc1[unit, p] = (mine + r1[unit, p].astype(jnp.float32)).astype(jnp.bfloat16)
            stage2(unit, p).start()

    def store_fin(p, q, total):
        for t in range(pq):
            fin[p, pl.ds(q * pq + t, per, stride=pairs), :] = total[t * per : (t + 1) * per]

    def add2(q, unit, m):
        for p in range(2):
            stage2(unit, p).wait_recv()
            total = acc1[unit, p, bits[1 - p]].astype(jnp.float32) + r2[unit, p].astype(jnp.float32)
            if m is None:
                store_fin(p, q, total)
            else:
                outbox[m, p] = total.astype(jnp.bfloat16)
        if m is not None:
            result(m).start()

    def at_age(t, age, act):
        q = t - (n - 1) - age
        m = lax.div(q, 2)
        live = (q >= 0) & (q < CHUNKS)

        @pl.when(live & has_own(q))
        def _():
            act(q, q, None)

        if moved:
            @pl.when(live & has_extra(q))
            def _():
                act(q, CHUNKS + m, m)

    def run_forward(q, unit, m):
        if m is not None:
            angle_copy(m).wait_recv()
        compute_forward(q, unit)
        stage0(unit).start()

    def forward_step(t, carry):
        @pl.when((t > 0) & (t < CHUNKS) & middle_layer)
        def _():
            send_own(t)

        for s in range(n - 1):
            q = t - 1 - s

            @pl.when((q >= 0) & (q < CHUNKS))
            def _():
                for d in range(2):
                    @pl.when(gets(d, s, q))
                    def _():
                        copy(d, s, q).wait_recv()
                        if s + 1 < n - 1:
                            @pl.when(sends(d, s + 1, q))
                            def _():
                                copy(d, s + 1, q).start()

        @pl.when(t < per // 4)
        def _():
            for k in range(4):
                prepare(4 * t + k)

        at_age(t, 3, add2)
        at_age(t, 2, lambda q, unit, m: add1(unit))
        at_age(t, 1, lambda q, unit, m: add0(unit))
        at_age(t, 0, run_forward)
        return carry

    lax.fori_loop(0, CHUNKS + n - 1 + 3, forward_step, 0)

    if moved:
        @pl.when(jnp.logical_not(middle_layer))
        def _():
            for m in range(moved):
                result(m).wait_recv()
                for p in range(2):
                    store_fin(p, 2 * m + 1, inbox[m, p].astype(jnp.float32))

    def one(s):
        at = pl.ds(s, 1)
        where = pl.ds(pl.multiple_of(s * pairs, pairs), pairs)
        row_weights = row_table[s]
        column_weights = column_table[s]
        real, imag = fin[0, where, :], fin[1, where, :]
        grid = jnp.concatenate(
            [
                jnp.concatenate([real[:, :rows], imag[:, :rows]], axis=1),
                jnp.concatenate([real[:, rows:], imag[:, rows:]], axis=1),
            ],
            axis=0,
        )
        picked = lax.dot_general(
            grid.astype(jnp.bfloat16), column_weights, (((0,), (0,)), ((), ())),
            preferred_element_type=jnp.float32,
        )
        model_real = jnp.sum(picked[:rows] * row_weights, axis=0, keepdims=True)
        model_imag = jnp.sum(picked[rows:] * row_weights, axis=0, keepdims=True)
        cosine, sine = phase[0, at, :], phase[1, at, :]
        res_real = obs_ref[s, 0:1, :] - (model_real * cosine - model_imag * sine)
        res_imag = obs_ref[s, 1:2, :] - (model_real * sine + model_imag * cosine)
        res_ref[s, 0:1, :] = res_real
        res_ref[s, 1:2, :] = res_imag
        w_real = res_real * cosine + res_imag * sine
        w_imag = res_imag * cosine - res_real * sine
        spread_rows = jnp.concatenate([row_weights * w_real, row_weights * w_imag], axis=0).astype(jnp.bfloat16)
        back = lax.dot_general(
            column_weights, spread_rows, (((1,), (1,)), ((), ())), preferred_element_type=jnp.float32
        )
        adj[0, where, :] = jnp.concatenate([back[:pairs, :rows], back[pairs:, :rows]], axis=1)
        adj[1, where, :] = jnp.concatenate([back[:pairs, rows:], back[pairs:, rows:]], axis=1)

    def four(step, carry):
        for k in range(4):
            one(4 * step + k)
        return carry

    lax.fori_loop(0, per // 4, four, 0)

    def slot(p):
        return bits[p] * 2 + bits[1 - p]

    def own_block(unit, p):
        return every.at[unit, p, core, slot(p)]

    def give(m, p):
        ref = own_block(CHUNKS + m, p)
        return remote(ref, ref, ys.at[m, p], yr.at[m, p], "layer", jnp.where(middle_layer, outer, inner))

    def gather_a(unit, p):
        ref = own_block(unit, p)
        return remote(ref, ref, sa.at[unit, p], da.at[unit, p], "facet", flip(1 - p))

    def gather_b(unit, p):
        ref = every.at[unit, p, core, pl.ds(bits[p] * 2, 2)]
        return remote(ref, ref, sb.at[unit, p], db.at[unit, p], "facet", flip(p))

    def gather_c(unit, p):
        ref = every.at[unit, p, core]
        return remote(ref, ref, sc.at[unit, p], dc.at[unit, p], "facet", other)

    def fill(unit, q):
        for p in range(2):
            for t in range(pq):
                piece = adj[p, pl.ds(q * pq + t, per, stride=pairs), :].astype(jnp.bfloat16)
                every[unit, p, core, slot(p), t * per : (t + 1) * per] = piece

    def fill_step(q, carry):
        @pl.when(has_own(q))
        def _():
            fill(q, q)
            for p in range(2):
                gather_a(q, p).start()

        if moved:
            @pl.when(jnp.logical_not(has_own(q)))
            def _():
                m = lax.div(q, 2)
                fill(CHUNKS + m, q)
                for p in range(2):
                    give(m, p).start()

        return carry

    lax.fori_loop(0, CHUNKS, fill_step, 0)

    def back_copy(direction, j, q):
        step = 1 if direction == 0 else -1
        return remote(
            sbuf.at[direction, j, chunk(q)], rbuf.at[direction, j, chunk(q)],
            bs.at[direction, j, q], br.at[direction, j, q], "layer", near(step),
        )

    def behind(direction, q):
        return i > bottom(q) if direction == 0 else i < top(q)

    def compute_backward(q, unit, m):
        twr, twi = tw2_ref[0], tw2_ref[1]
        facr, faci = fac[0], fac[1]
        base = chunk(unit).start
        for pair in range(pq):
            where = slice(pair * per, (pair + 1) * per)
            grids = [
                jnp.concatenate(
                    [every[unit, p, device % 2, place(p, device), where] for device in range(8)], axis=0
                ).astype(jnp.float32)
                for p in range(2)
            ]
            ar, ai = grids
            b = jnp.concatenate([ar * facr + ai * faci, ai * facr - ar * faci], axis=0).astype(jnp.bfloat16)
            h = jnp.dot(g2_ref[...], b, preferred_element_type=jnp.float32)
            hr, hi = h[:subgrids], h[subgrids:]
            mixed = jnp.concatenate([hr * twr + hi * twi, hi * twr - hr * twi], axis=1).astype(jnp.bfloat16)
            image = lax.dot_general(
                f2_ref[...], mixed, (((1,), (1,)), ((), ())), preferred_element_type=jnp.float32
            )
            for c in range(2):
                col = q * cq + 2 * pair + c
                ir = image[2 * c * rows : (2 * c + 1) * rows]
                ii = image[(2 * c + 1) * rows : (2 * c + 2) * rows]
                cosine, sine = cs[base + 2 * pair + c, 0], cs[base + 2 * pair + c, 1]
                tr = (BACK_GAIN * (ir * cosine + ii * sine)).astype(jnp.bfloat16)
                ti = (BACK_GAIN * (ii * cosine - ir * sine)).astype(jnp.bfloat16)
                for l in range(n):
                    for part, value in ((0, tr), (1, ti)):
                        piece = value[l * block : (l + 1) * block]
                        if m is not None:
                            total = term[l, col, part].astype(jnp.float32) + piece.astype(jnp.float32)
                            piece = total.astype(jnp.bfloat16)
                        term[l, col, part] = piece

    def run_backward(q, unit, m):
        for p in range(2):
            gather_c(unit, p).wait_recv()
        compute_backward(q, unit, m)

    def relay(direction, j, q):
        where = chunk(q)

        @pl.when(behind(direction, q))
        def _():
            back_copy(direction, j, q).wait_recv()
            total = term[j, where].astype(jnp.float32) + rbuf[direction, j, where].astype(jnp.float32)
            sbuf[direction, j, where] = total.astype(jnp.bfloat16)

        @pl.when(jnp.logical_not(behind(direction, q)))
        def _():
            sbuf[direction, j, where] = term[j, where]

        back_copy(direction, j, q).start()

    def units_of(q, act):
        live = (q >= 0) & (q < CHUNKS)

        @pl.when(live & has_own(q))
        def _():
            act(q, q, None)

        if moved:
            @pl.when(live & has_extra(q))
            def _():
                m = lax.div(q, 2)
                act(q, CHUNKS + m, m)

    def to_b(q, unit, m):
        for p in range(2):
            gather_a(unit, p).wait_recv()
            gather_b(unit, p).start()

    def to_c(q, unit, m):
        for p in range(2):
            gather_b(unit, p).wait_recv()
            gather_c(unit, p).start()

    def backward_step(t, carry):
        if moved:
            early = t + 1

            @pl.when((early < CHUNKS) & has_extra(early))
            def _():
                m = lax.div(early, 2)
                for p in range(2):
                    give(m, p).wait_recv()
                    gather_a(CHUNKS + m, p).start()

        units_of(t, to_b)
        units_of(t - 1, to_c)
        units_of(t - 2, run_backward)
        now = t - 2
        for direction in range(2):
            q = now - i if direction == 0 else now - (n - 1 - i)

            @pl.when((q >= 0) & (q < CHUNKS) & has_own(q))
            def _():
                for d in range(n - 1, 0, -1):
                    j = i + d if direction == 0 else i - d

                    @pl.when((j < n) & (j >= 0))
                    def _():
                        relay(direction, j, q)

        last = now - (n - 1)

        @pl.when(last >= 0)
        def _():
            where = chunk(last)

            @pl.when(has_own(last))
            def _():
                for p in range(2):
                    otmp[p] = term[i, where, p].astype(jnp.float32).reshape(cq * block, subgrids)

            @pl.when(jnp.logical_not(has_own(last)))
            def _():
                otmp[...] = jnp.zeros(otmp.shape, jnp.float32)

            for direction in range(2):
                @pl.when(behind(direction, last))
                def _():
                    back_copy(direction, i, last).wait_recv()
                    for p in range(2):
                        got = rbuf[direction, i, where, p].astype(jnp.float32)
                        otmp[p] += got.reshape(cq * block, subgrids)

            for p in range(2):
                for m in range(block):
                    out_ref[p, where, m * subgrids : (m + 1) * subgrids] = otmp[p, pl.ds(m, cq, stride=block), :]

        return carry

    lax.fori_loop(0, CHUNKS + n - 1 + 2, backward_step, 0)

    def drain_unit(unit):
        stage0(unit).wait_send()
        for p in range(2):
            stage1(unit, p).wait_send()
            stage2(unit, p).wait_send()
            gather_a(unit, p).wait_send()
            gather_b(unit, p).wait_send()
            gather_c(unit, p).wait_send()

    def drain(q, carry):
        for d in range(2):
            for s in range(n - 1):
                @pl.when(sends(d, s, q))
                def _():
                    copy(d, s, q).wait_send()

        @pl.when(has_own(q))
        def _():
            drain_unit(q)
            for direction in range(2):
                for d in range(1, n):
                    j = i + d if direction == 0 else i - d

                    @pl.when((j < n) & (j >= 0))
                    def _():
                        back_copy(direction, j, q).wait_send()

        if moved:
            m = lax.div(q, 2)

            @pl.when(has_extra(q))
            def _():
                drain_unit(CHUNKS + m)
                result(m).wait_send()

            @pl.when(is_moved(q) & jnp.logical_not(middle_layer))
            def _():
                angle_copy(m).wait_send()
                for p in range(2):
                    give(m, p).wait_send()

        return carry

    lax.fori_loop(0, CHUNKS, drain, 0)


def cs_extra(moved, total):
    return total * moved // (CHUNKS + moved)


def fused(n, moved, x, angle, window, u, v, plane, observed, tables, taps, plane_angle, shift):
    _, cols, _ = x.shape
    per, vis = u.shape
    subgrids = tables[1].shape[0] // 2
    rows = tables[0].shape[0] // 2
    block = rows // n
    pairs = cols // 2
    cq = cols // CHUNKS
    units = CHUNKS + moved
    slab = (cq // 2) * per
    lanes = 2 * rows
    vmem = pl.BlockSpec(memory_space=pltpu.VMEM)
    smem = pl.BlockSpec(memory_space=pltpu.SMEM)
    bf = lambda *shape: pltpu.VMEM(shape, jnp.bfloat16)
    f32 = lambda *shape: pltpu.VMEM(shape, jnp.float32)
    dma = lambda *shape: pltpu.SemaphoreType.DMA(shape)
    box = max(moved, 1)
    return pl.pallas_call(
        functools.partial(fused_kernel, n, moved),
        out_shape=(
            jax.ShapeDtypeStruct((per, 2, vis), jnp.float32),
            jax.ShapeDtypeStruct(x.shape, jnp.float32),
        ),
        in_specs=[vmem] * 13 + [smem] * 3,
        out_specs=(vmem, vmem),
        scratch_shapes=[
            bf(n, cols, 2, block, subgrids), bf(cq * units, rows, subgrids), f32(cq * units, 2, rows, subgrids),
            f32(2, subgrids, lanes), f32(2, 2 * cq * block, subgrids), f32(2 * cq * rows, subgrids),
            bf(units, 2, 2, 4, slab, lanes), bf(units, 2, 4, slab, lanes), bf(units, 2, 4, slab, lanes),
            bf(units, 2, 2, slab, lanes), bf(units, 2, 2, slab, lanes), bf(units, 2, slab, lanes),
            bf(box, 2, slab, lanes), bf(box, 2, slab, lanes),
            f32(2, per * pairs, lanes), f32(2, per * pairs, lanes), f32(2, per, vis),
            f32(per, rows, vis), bf(per, cols, vis),
            bf(units, 2, 2, 4, slab, lanes), bf(n, cols, 2, block, subgrids),
            bf(2, n, cols, 2, block, subgrids), bf(2, n, cols, 2, block, subgrids), f32(2, cq * block, subgrids),
            dma(2, n - 1, CHUNKS), dma(2, n - 1, CHUNKS), dma(box), dma(box),
            dma(units), dma(units), dma(units, 2), dma(units, 2), dma(units, 2), dma(units, 2), dma(box), dma(box),
            dma(box, 2), dma(box, 2), dma(units, 2), dma(units, 2), dma(units, 2), dma(units, 2), dma(units, 2), dma(units, 2),
            dma(2, n, CHUNKS), dma(2, n, CHUNKS),
        ],
        compiler_params=pltpu.CompilerParams(
            collective_id=2, has_side_effects=True, vmem_limit_bytes=60 * 1024 * 1024
        ),
        name="fused_column",
    )(x, angle, window, u, v, plane, observed, *tables, taps, plane_angle, shift)


def local(n, nf, model_strip, screen_angle, facet_window, facet_shift, kernel_taps, plane_angle, u_cell, v_cell, w_plane, observed):
    _, _, cols, length = screen_angle.shape
    per = u_cell.shape[1]
    subgrids = per * nf
    rows = length // subgrids
    block = rows // n
    vmem = pl.BlockSpec(memory_space=pltpu.VMEM)
    fr, fi = dft(rows)
    gr, gi = dft(subgrids)
    turn = 2.0 * np.pi * (np.arange(rows)[:, None] * np.arange(subgrids)[None, :] % length) / length
    twist = np.stack([np.cos(turn), -np.sin(turn)]).astype(np.float32)
    bf = lambda a: jnp.asarray(a.astype(np.float32)).astype(jnp.bfloat16)
    f1 = bf(np.block([[fr, -fi], [fi, fr]]))
    g1 = bf(np.block([[gr, -gi], [gi, gr]]))
    g2 = bf(np.block([[gr.T, gi.T], [-gi.T, gr.T]]))
    zero = np.zeros_like(fr)
    f2 = bf(
        np.block(
            [
                [fr.T, zero, fi.T, zero],
                [-fi.T, zero, fr.T, zero],
                [zero, fr.T, zero, fi.T],
                [zero, -fi.T, zero, fr.T],
            ]
        )
    )
    tw2 = np.ascontiguousarray(np.tile(np.swapaxes(twist, 1, 2), (1, 1, 2)))
    if nf == 8 and n == 4 and per % 16 == 0 and 2 * rows == subgrids == 128 and cols % (2 * CHUNKS) == 0:
        tables = (f1, g1, jnp.asarray(twist), g2, f2, jnp.asarray(tw2))
        residual, gradient = fused(
            n, MOVED, model_strip[0], screen_angle[0, 0], facet_window.reshape(length // subgrids, subgrids),
            u_cell[0], v_cell[0], w_plane[0], observed[0], tables, kernel_taps, plane_angle, facet_shift,
        )
        return (residual[None], gradient[None])
    factor = facet_factor(facet_window[0], facet_shift[0], subgrids)
    x = model_strip[0].reshape(2, cols, block, subgrids).transpose(1, 0, 2, 3)
    angle = screen_angle[0, 0].reshape(cols, rows, subgrids)
    contrib = pl.pallas_call(
        functools.partial(forward_kernel, n),
        out_shape=jax.ShapeDtypeStruct((2, cols // 2, subgrids, 2 * rows), jnp.bfloat16),
        in_specs=[vmem] * 6,
        out_specs=vmem,
        scratch_shapes=[
            pltpu.VMEM((n, cols, 2, block, subgrids), jnp.bfloat16),
            pltpu.SemaphoreType.DMA((2, n - 1, CHUNKS)),
            pltpu.SemaphoreType.DMA((2, n - 1, CHUNKS)),
            pltpu.SemaphoreType.DMA,
        ],
        compiler_params=pltpu.CompilerParams(collective_id=0, has_side_effects=True),
        name="gather_forward",
    )(x, angle, f1, g1, jnp.asarray(twist), factor)
    parts = contrib.reshape(2, cols // 2, nf, per, 2 * rows)
    received = lax.all_to_all(parts, "facet", split_axis=2, concat_axis=2, tiled=True)
    grids = jnp.sum(received.astype(jnp.float32), axis=2)
    grids = grids.reshape(2, cols // 2, per, 2, rows).transpose(2, 1, 3, 0, 4).reshape(per, cols, 2 * rows)
    residual, adjoint = middle(
        grids, u_cell[0], v_cell[0], w_plane[0], observed[0], plane_angle[0], kernel_taps, rows, cols
    )
    adjoint = adjoint.reshape(per, cols // 2, 2, 2, rows).transpose(3, 1, 0, 2, 4).reshape(2, cols // 2, per, 2 * rows)
    every = lax.all_gather(adjoint, "facet", axis=2, tiled=True)
    gradient = pl.pallas_call(
        functools.partial(backward_kernel, n),
        out_shape=jax.ShapeDtypeStruct((cols, 2, block, subgrids), jnp.float32),
        in_specs=[vmem] * 6,
        out_specs=vmem,
        scratch_shapes=[
            pltpu.VMEM((n, cols, 2, block, subgrids), jnp.bfloat16),
            pltpu.VMEM((2, n, cols, 2, block, subgrids), jnp.bfloat16),
            pltpu.VMEM((2, n, cols, 2, block, subgrids), jnp.bfloat16),
            pltpu.SemaphoreType.DMA((2, n, CHUNKS)),
            pltpu.SemaphoreType.DMA((2, n, CHUNKS)),
        ],
        compiler_params=pltpu.CompilerParams(collective_id=1, has_side_effects=True),
        name="backward_scatter",
    )(every, angle, g2, f2, jnp.asarray(tw2), factor)
    gradient = gradient.transpose(1, 0, 2, 3).reshape(1, 2, cols, block * subgrids)
    return (residual[None], gradient)


def solution(mesh):
    return jax.shard_map(
        functools.partial(local, mesh.shape["layer"], mesh.shape["facet"]),
        mesh=mesh,
        in_specs=(
            P("facet", None, None, "layer"),
            P("layer", "facet", None, None),
            P("facet", None),
            P("facet"),
            P(),
            P("layer", None),
            P("layer", "facet", None),
            P("layer", "facet", None),
            P("layer", "facet", None),
            P("layer", "facet", None, None),
        ),
        out_specs=(P("layer", "facet", None, None), P("facet", None, None, "layer")),
        check_vma=False,
    )
```

```python
import functools
import math

import jax
import jax.numpy as jnp
import numpy as np
from jax import lax
from jax.experimental import pallas as pl
from jax.experimental.pallas import tpu as pltpu
from jax.sharding import PartitionSpec as P

MESH = pl.DeviceIdType.MESH
BACK_GAIN = 8.0
CHUNKS = 8
MOVED = 3
FIRST = 1
EARLY = 1
LEAD = 1
HOP = 2
AGES = (1, 3, 5)
SPREAD = (2, 3)
LAG = 2


def _fit(values, degree):
    nodes = np.cos(np.pi * (np.arange(64) + 0.5) / 64)
    y = (nodes + 1.0) * 0.5 * np.pi**2
    cheb = np.polynomial.chebyshev.Chebyshev.fit(y, values(np.sqrt(y)), degree, domain=[0, np.pi**2])
    return [float(v) for v in cheb.convert(kind=np.polynomial.Polynomial).coef]


COS = _fit(np.cos, 8)
SIN = _fit(lambda x: np.sinc(x / np.pi), 7)


def cos_sin(x):
    y = x * x
    c = jnp.full_like(y, COS[-1])
    for v in COS[-2::-1]:
        c = c * y + v
    s = jnp.full_like(y, SIN[-1])
    for v in SIN[-2::-1]:
        s = s * y + v
    return c, s * x


def dft(length):
    k = np.arange(length)
    angles = 2.0 * np.pi * ((k[:, None] * k[None, :]) % length) / length
    scale = 1.0 / math.sqrt(length)
    return np.cos(angles) * scale, -np.sin(angles) * scale


def barrier_line(i, n):
    sem = pltpu.get_barrier_semaphore()

    @pl.when(i > 0)
    def _():
        pl.semaphore_signal(sem, inc=1, device_id={"layer": i - 1}, device_id_type=MESH)

    @pl.when(i < n - 1)
    def _():
        pl.semaphore_signal(sem, inc=1, device_id={"layer": i + 1}, device_id_type=MESH)

    peers = jnp.where(i > 0, 1, 0) + jnp.where(i < n - 1, 1, 0)
    pl.semaphore_wait(sem, peers)


def forward_kernel(n, x_ref, ang_ref, f1_ref, g_ref, tw_ref, fac_ref, out_ref, buf, send_sem, recv_sem, own_sem):
    i = lax.axis_index("layer")
    cq = x_ref.shape[0] // CHUNKS
    subgrids = g_ref.shape[0] // 2
    rows = f1_ref.shape[0] // 2
    barrier_line(i, n)
    own = pltpu.make_async_copy(x_ref, buf.at[i], own_sem)
    own.start()

    def copy(direction, s, q):
        step = 1 if direction == 0 else -1
        origin = jnp.clip(i - step * s, 0, n - 1)
        cols = pl.ds(q * cq, cq)
        src = x_ref.at[cols] if s == 0 else buf.at[origin, cols]
        return pltpu.make_async_remote_copy(
            src_ref=src,
            dst_ref=buf.at[origin, cols],
            send_sem=send_sem.at[direction, s, q],
            recv_sem=recv_sem.at[direction, s, q],
            device_id={"layer": jnp.clip(i + step, 0, n - 1)},
            device_id_type=MESH,
        )

    def sends(direction, s):
        if direction == 0:
            return (i - s >= 0) & (i < n - 1)
        return (i + s <= n - 1) & (i > 0)

    def gets(direction, s):
        return i - 1 - s >= 0 if direction == 0 else i + 1 + s <= n - 1

    def compute(q):
        twr, twi = tw_ref[0], tw_ref[1]
        facr, faci = fac_ref[0], fac_ref[1]
        for pair in range(cq // 2):
            halves = []
            for c in (2 * pair, 2 * pair + 1):
                col = q * cq + c
                xr = jnp.concatenate([buf[l, col, 0] for l in range(n)], axis=0).astype(jnp.float32)
                xi = jnp.concatenate([buf[l, col, 1] for l in range(n)], axis=0).astype(jnp.float32)
                cosine, sine = cos_sin(ang_ref[col].astype(jnp.float32))
                x = jnp.concatenate([xr * cosine - xi * sine, xr * sine + xi * cosine], axis=0)
                h = jnp.dot(f1_ref[...], x.astype(jnp.bfloat16), preferred_element_type=jnp.float32)
                hr, hi = h[:rows], h[rows:]
                halves.append(
                    jnp.concatenate([hr * twr - hi * twi, hr * twi + hi * twr], axis=1).astype(jnp.bfloat16)
                )
            both = jnp.concatenate(halves, axis=0)
            spec = lax.dot_general(
                g_ref[...], both, (((1,), (1,)), ((), ())), preferred_element_type=jnp.float32
            )
            sr, si = spec[:subgrids], spec[subgrids:]
            at = q * (cq // 2) + pair
            out_ref[0, at] = (sr * facr - si * faci).astype(jnp.bfloat16)
            out_ref[1, at] = (sr * faci + si * facr).astype(jnp.bfloat16)

    def body(t, carry):
        @pl.when(t < CHUNKS)
        def _():
            for d in range(2):
                @pl.when(sends(d, 0))
                def _():
                    copy(d, 0, t).start()

        for s in range(n - 1):
            q = t - 1 - s
            @pl.when((q >= 0) & (q < CHUNKS))
            def _():
                for d in range(2):
                    @pl.when(gets(d, s))
                    def _():
                        copy(d, s, q).wait_recv()
                        if s + 1 < n - 1:
                            @pl.when(sends(d, s + 1))
                            def _():
                                copy(d, s + 1, q).start()

        @pl.when(t >= n - 1)
        def _():
            compute(t - (n - 1))

        return carry

    own.wait()
    lax.fori_loop(0, CHUNKS + n - 1, body, 0)

    def drain(q, carry):
        for d in range(2):
            for s in range(n - 1):
                @pl.when(sends(d, s))
                def _():
                    copy(d, s, q).wait_send()
        return carry

    lax.fori_loop(0, CHUNKS, drain, 0)


def backward_kernel(n, a_ref, ang_ref, g_ref, f2_ref, tw_ref, fac_ref, out_ref, term, sbuf, rbuf, send_sem, recv_sem):
    i = lax.axis_index("layer")
    cols = ang_ref.shape[0]
    cq = cols // CHUNKS
    fine = g_ref.shape[0] // 2
    rows = ang_ref.shape[1]
    part = rows // n
    barrier_line(i, n)

    def copy(direction, j, q):
        where = pl.ds(q * cq, cq)
        step = 1 if direction == 0 else -1
        return pltpu.make_async_remote_copy(
            src_ref=sbuf.at[direction, j, where],
            dst_ref=rbuf.at[direction, j, where],
            send_sem=send_sem.at[direction, j, q],
            recv_sem=recv_sem.at[direction, j, q],
            device_id={"layer": jnp.clip(i + step, 0, n - 1)},
            device_id_type=MESH,
        )

    def behind(direction):
        return i > 0 if direction == 0 else i < n - 1

    def compute(q):
        twr, twi = tw_ref[0], tw_ref[1]
        facr, faci = fac_ref[0], fac_ref[1]
        for pair in range(cq // 2):
            at = q * (cq // 2) + pair
            ar = a_ref[0, at].astype(jnp.float32)
            ai = a_ref[1, at].astype(jnp.float32)
            b = jnp.concatenate([ar * facr + ai * faci, ai * facr - ar * faci], axis=0).astype(jnp.bfloat16)
            h = jnp.dot(g_ref[...], b, preferred_element_type=jnp.float32)
            hr, hi = h[:fine], h[fine:]
            mixed = jnp.concatenate([hr * twr + hi * twi, hi * twr - hr * twi], axis=1).astype(jnp.bfloat16)
            image = lax.dot_general(
                f2_ref[...], mixed, (((1,), (1,)), ((), ())), preferred_element_type=jnp.float32
            )
            for c in range(2):
                col = q * cq + 2 * pair + c
                ir = image[2 * c * rows : (2 * c + 1) * rows]
                ii = image[(2 * c + 1) * rows : (2 * c + 2) * rows]
                cosine, sine = cos_sin(ang_ref[col].astype(jnp.float32))
                tr = (BACK_GAIN * (ir * cosine + ii * sine)).astype(jnp.bfloat16)
                ti = (BACK_GAIN * (ii * cosine - ir * sine)).astype(jnp.bfloat16)
                for l in range(n):
                    term[l, col, 0] = tr[l * part : (l + 1) * part]
                    term[l, col, 1] = ti[l * part : (l + 1) * part]

    def relay(direction, j, q):
        where = pl.ds(q * cq, cq)

        @pl.when(behind(direction))
        def _():
            copy(direction, j, q).wait_recv()
            total = term[j, where].astype(jnp.float32) + rbuf[direction, j, where].astype(jnp.float32)
            sbuf[direction, j, where] = total.astype(jnp.bfloat16)

        @pl.when(jnp.logical_not(behind(direction)))
        def _():
            sbuf[direction, j, where] = term[j, where]

        copy(direction, j, q).start()

    def body(t, carry):
        @pl.when(t < CHUNKS)
        def _():
            compute(t)

        for direction in range(2):
            q = t - i if direction == 0 else t - (n - 1 - i)

            @pl.when((q >= 0) & (q < CHUNKS))
            def _():
                for d in range(n - 1, 0, -1):
                    j = i + d if direction == 0 else i - d

                    @pl.when((j < n) & (j >= 0))
                    def _():
                        relay(direction, j, q)

        last = t - (n - 1)

        @pl.when(last >= 0)
        def _():
            where = pl.ds(last * cq, cq)
            out_ref[where] = term[i, where].astype(jnp.float32)
            for direction in range(2):
                @pl.when(behind(direction))
                def _():
                    copy(direction, i, last).wait_recv()
                    out_ref[where] += rbuf[direction, i, where].astype(jnp.float32)

        return carry

    lax.fori_loop(0, CHUNKS + n - 1, body, 0)

    def drain(q, carry):
        for direction in range(2):
            for d in range(1, n):
                j = i + d if direction == 0 else i - d

                @pl.when((j < n) & (j >= 0))
                def _():
                    copy(direction, j, q).wait_send()
        return carry

    lax.fori_loop(0, CHUNKS, drain, 0)


def facet_factor(window, shift_cells, subgrids):
    length = window.shape[0]
    rows = length // subgrids
    grid = window.reshape(subgrids, rows)
    grid = jnp.concatenate([grid, grid], axis=1)
    high = lax.broadcasted_iota(jnp.int32, grid.shape, 0)
    low = lax.broadcasted_iota(jnp.int32, grid.shape, 1) % rows
    turn_count = (high * rows + low) * shift_cells % length
    angles = 2.0 * math.pi / length * turn_count.astype(jnp.float32)
    return jnp.stack([grid * jnp.cos(angles), -grid * jnp.sin(angles)])


def spread(cells, length, taps):
    count = taps.shape[0]
    lanes = jnp.arange(length, dtype=jnp.int32)
    offset = (lanes - cells[..., None] + (count // 2 + length)) % length
    out = jnp.zeros(offset.shape, jnp.float32)
    for t in range(count):
        out = out + jnp.where(offset == t, taps[t], 0.0)
    return out


def middle(grids, u, v, plane, observed, angle, taps, rows, cols):
    row_weights = spread(u, rows, taps)
    column_weights = spread(v, cols, taps).astype(jnp.bfloat16)
    picked = jnp.einsum("sjc,sck->sjk", column_weights, grids.astype(jnp.bfloat16), preferred_element_type=jnp.float32)
    model_real = jnp.sum(picked[..., :rows] * row_weights, axis=2)
    model_imag = jnp.sum(picked[..., rows:] * row_weights, axis=2)
    pick = plane[..., None] == jnp.arange(angle.shape[0], dtype=jnp.int32)
    cosine = jnp.sum(jnp.where(pick, jnp.cos(angle), 0.0), axis=2)
    sine = jnp.sum(jnp.where(pick, jnp.sin(angle), 0.0), axis=2)
    res_real = observed[:, 0] - (model_real * cosine - model_imag * sine)
    res_imag = observed[:, 1] - (model_real * sine + model_imag * cosine)
    w_real = res_real * cosine + res_imag * sine
    w_imag = res_imag * cosine - res_real * sine
    spread_rows = jnp.concatenate(
        [w_real[..., None] * row_weights, w_imag[..., None] * row_weights], axis=2
    ).astype(jnp.bfloat16)
    adjoint = jnp.einsum("sjc,sjk->sck", column_weights, spread_rows, preferred_element_type=jnp.float32)
    return jnp.stack([res_real, res_imag], axis=1), adjoint.astype(jnp.bfloat16)


def fused_kernel(
    n, moved, x_ref, ang_ref, win_ref, u_ref, v_ref, plane_ref, obs_ref, f1_ref, g1_ref, tw_ref, g2_ref, f2_ref, tw2_ref,
    taps_ref, pang_ref, shift_ref, res_ref, out_ref,
    buf, angb, cs, fac, tmpx, tmpa, contrib, r0, acc0, r1, acc1, r2, outbox, inbox, fin, adj, phase, row_table, column_table,
    every, term, sbuf, rbuf, otmp,
    fs, fr, angs, angr, s0, d0, s1, d1, s2, d2, xs, xr, ys, yr, sa, da, sb, db, sc, dc, bs, br,
):
    cols, rows = angb.shape[0] - cs_extra(moved, angb.shape[0]), angb.shape[1]
    lanes = 2 * rows
    subgrids = g1_ref.shape[0] // 2
    block = rows // n
    per, vis = u_ref.shape
    pairs = cols // 2
    cq = cols // CHUNKS
    pq = cq // 2
    i = lax.axis_index("layer")
    f = lax.axis_index("facet")
    core = lax.rem(f, 2)
    chip = lax.div(f, 2)
    bits = (lax.rem(chip, 2), lax.div(chip, 2))
    other = f + 1 - 2 * core
    middle_layer = (i >= 1) & (i <= n - 2)

    def flip(b):
        return f + (1 - 2 * bits[b]) * (2 * (1 + b))

    def near(step):
        return jnp.clip(i + step, 0, n - 1)

    inner = jnp.where(i == 0, 1, n - 2)
    outer = jnp.where(i == 1, 0, n - 1)

    barrier = pltpu.get_barrier_semaphore()
    for peer in (other, flip(0), flip(1)):
        pl.semaphore_signal(barrier, inc=1, device_id={"facet": peer}, device_id_type=MESH)

    @pl.when(i > 0)
    def _():
        pl.semaphore_signal(barrier, inc=1, device_id={"layer": i - 1}, device_id_type=MESH)

    @pl.when(i < n - 1)
    def _():
        pl.semaphore_signal(barrier, inc=1, device_id={"layer": i + 1}, device_id_type=MESH)

    pl.semaphore_wait(barrier, 3 + jnp.where(i > 0, 1, 0) + jnp.where(i < n - 1, 1, 0))

    def is_moved(q):
        return (lax.rem(q, 2) == 1) & (q >= FIRST) & (q < FIRST + 2 * moved)

    def moved_index(q):
        return lax.div(q - FIRST, 2)

    def bottom(q):
        return jnp.where(is_moved(q), 1, 0)

    def top(q):
        return jnp.where(is_moved(q), n - 2, n - 1)

    def has_own(q):
        return (i >= bottom(q)) & (i <= top(q))

    def has_extra(q):
        return middle_layer & is_moved(q)

    def remote(src, dst, send, recv, axis, device):
        return pltpu.make_async_remote_copy(
            src_ref=src, dst_ref=dst, send_sem=send, recv_sem=recv, device_id={axis: device}, device_id_type=MESH
        )

    def chunk(q):
        return pl.ds(pl.multiple_of(q * cq, cq), cq)

    def copy(direction, s, q):
        step = 1 if direction == 0 else -1
        origin = jnp.clip(i - step * s, 0, n - 1)
        ref = buf.at[origin, chunk(q)]
        return remote(ref, ref, fs.at[direction, s], fr.at[direction, s, q], "layer", near(step))

    def sends(direction, s, q):
        if direction == 0:
            return (i - s >= 0) & (i + 1 <= top(q))
        return (i + s <= n - 1) & (i - 1 >= bottom(q))

    def gets(direction, s, q):
        if direction == 0:
            return (i - 1 - s >= 0) & (i <= top(q))
        return (i + 1 + s <= n - 1) & (i >= bottom(q))

    def send_own(q):
        for d in range(2):
            @pl.when(sends(d, 0, q))
            def _():
                copy(d, 0, q).start()

    def angle_copy(m):
        src = angb.at[chunk(2 * m + FIRST)]
        dst = angb.at[chunk(CHUNKS + m)]
        return remote(src, dst, angs.at[0], angr.at[m], "layer", inner)

    def relayout(g, carry):
        at = pl.ds(pl.multiple_of(g * 2 * cq, 2 * cq), 2 * cq)
        for p in range(2):
            v = x_ref[p, at, :].astype(jnp.float32)
            for m in range(block):
                tmpx[p, pl.ds(m, 2 * cq, stride=block), :] = v[:, m * subgrids : (m + 1) * subgrids]
            buf[i, at, p] = tmpx[p].reshape(2 * cq, block, subgrids).astype(jnp.bfloat16)

        for k in range(2):
            @pl.when(jnp.logical_not(middle_layer) | (2 * g + k < LEAD))
            def _():
                send_own(2 * g + k)

        @pl.when(jnp.logical_not(middle_layer))
        def _():
            angle_relayout(g)

        return carry

    def angle_relayout(g):
        at = pl.ds(pl.multiple_of(g * 2 * cq, 2 * cq), 2 * cq)
        for m in range(rows):
            piece = ang_ref[at, m * subgrids : (m + 1) * subgrids].astype(jnp.float32)
            tmpa[pl.ds(m, 2 * cq, stride=rows), :] = piece
        angb[at] = tmpa[...].reshape(2 * cq, rows, subgrids).astype(jnp.bfloat16)

        if moved:
            m = g - FIRST // 2

            @pl.when(jnp.logical_not(middle_layer) & (m >= 0) & (m < moved))
            def _():
                angle_copy(m).start()

    lax.fori_loop(0, CHUNKS // 2, relayout, 0)

    window = win_ref[...]
    rolled = pltpu.roll(window, rows, axis=1)
    left = lax.broadcasted_iota(jnp.int32, window.shape, 1) < rows
    fac[0, pl.ds(0, subgrids // 2, stride=2), :] = jnp.where(left, window, rolled)
    fac[0, pl.ds(1, subgrids // 2, stride=2), :] = jnp.where(left, rolled, window)
    grid = fac[0]
    length = subgrids * rows
    high = lax.broadcasted_iota(jnp.int32, grid.shape, 0)
    low = lax.broadcasted_iota(jnp.int32, grid.shape, 1)
    low = jnp.where(low < rows, low, low - rows)
    turns = lax.rem((high * rows + low) * shift_ref[0], length)
    turns = jnp.where(turns * 2 >= length, turns - length, turns)
    cosine, sine = cos_sin(turns.astype(jnp.float32) * (2.0 * math.pi / length))
    fac[0] = grid * cosine
    fac[1] = -grid * sine

    plane = plane_ref[...]
    angle = jnp.zeros(plane.shape, jnp.float32)
    for k in range(pang_ref.shape[1]):
        angle = jnp.where(plane == k, pang_ref[0, k], angle)
    cosine, sine = cos_sin(angle)
    phase[0] = cosine
    phase[1] = sine

    def weights(cells, position, size):
        count = taps_ref.shape[0]
        offset = position - cells + count // 2
        offset = jnp.where(offset < 0, offset + size, jnp.where(offset >= size, offset - size, offset))
        out = jnp.zeros(offset.shape, jnp.float32)
        for t in range(count):
            out = jnp.where(offset == t, taps_ref[t], out)
        return out

    def prepare(s):
        at = pl.ds(s, 1)
        row = lax.broadcasted_iota(jnp.int32, (rows, vis), 0)
        half = lax.broadcasted_iota(jnp.int32, (pairs, vis), 0)
        col = jnp.concatenate([2 * half, 2 * half + 1], axis=0)
        row_table[s] = weights(u_ref[at, :], row, rows)
        column_table[s] = weights(v_ref[at, :], col, cols).astype(jnp.bfloat16)

    def place(p, device):
        b0, b1 = (device // 2) % 2, device // 4
        return (b0 * 2 + b1) if p == 0 else (b1 * 2 + b0)

    def compute_forward(q, unit):
        twr, twi = tw_ref[0], tw_ref[1]
        facr, faci = fac[0], fac[1]
        base = chunk(unit).start
        for pair in range(pq):
            halves = []
            for c in (2 * pair, 2 * pair + 1):
                col = q * cq + c
                xr_ = jnp.concatenate([buf[l, col, 0] for l in range(n)], axis=0).astype(jnp.float32)
                xi_ = jnp.concatenate([buf[l, col, 1] for l in range(n)], axis=0).astype(jnp.float32)
                cosine, sine = cos_sin(angb[base + c].astype(jnp.float32))
                cs[base + c, 0] = cosine
                cs[base + c, 1] = sine
                x = jnp.concatenate([xr_ * cosine - xi_ * sine, xr_ * sine + xi_ * cosine], axis=0)
                h = jnp.dot(f1_ref[...], x.astype(jnp.bfloat16), preferred_element_type=jnp.float32)
                hr, hi = h[:rows], h[rows:]
                halves.append(
                    jnp.concatenate([hr * twr - hi * twi, hr * twi + hi * twr], axis=1).astype(jnp.bfloat16)
                )
            both = jnp.concatenate(halves, axis=0)
            spec = lax.dot_general(
                g1_ref[...], both, (((1,), (1,)), ((), ())), preferred_element_type=jnp.float32
            )
            sr, si = spec[:subgrids], spec[subgrids:]
            parts = ((sr * facr - si * faci).astype(jnp.bfloat16), (sr * faci + si * facr).astype(jnp.bfloat16))
            for p in range(2):
                for device in range(8):
                    contrib[unit, device % 2, p, place(p, device), pair * per : (pair + 1) * per] = parts[p][
                        device * per : (device + 1) * per
                    ]

    def stage0(unit):
        return remote(contrib.at[unit, 1 - core], r0.at[unit], s0.at[0], d0.at[unit], "facet", other)

    def stage1(unit, p):
        src = acc0.at[unit, p, pl.ds((1 - bits[p]) * 2, 2)]
        return remote(src, r1.at[unit, p], s1.at[p], d1.at[unit, p], "facet", flip(p))

    def stage2(unit, p):
        src = acc1.at[unit, p, 1 - bits[1 - p]]
        return remote(src, r2.at[unit, p], s2.at[p], d2.at[unit, p], "facet", flip(1 - p))

    def result(m):
        return remote(outbox.at[m], inbox.at[m], xs.at[0], xr.at[m], "layer", jnp.where(middle_layer, outer, inner))

    def add0(unit):
        stage0(unit).wait_recv()
        for p in range(2):
            total = contrib[unit, core, p].astype(jnp.float32) + r0[unit, p].astype(jnp.float32)
            acc0[unit, p] = total.astype(jnp.bfloat16)
            stage1(unit, p).start()

    def add1(unit):
        for p in range(2):
            stage1(unit, p).wait_recv()
            mine = acc0[unit, p, pl.ds(bits[p] * 2, 2)].astype(jnp.float32)
            acc1[unit, p] = (mine + r1[unit, p].astype(jnp.float32)).astype(jnp.bfloat16)
            stage2(unit, p).start()

    def store_fin(p, q, total):
        for t in range(pq):
            fin[p, pl.ds(q * pq + t, per, stride=pairs), :] = total[t * per : (t + 1) * per]

    def add2(q, unit, m):
        for p in range(2):
            stage2(unit, p).wait_recv()
            total = acc1[unit, p, bits[1 - p]].astype(jnp.float32) + r2[unit, p].astype(jnp.float32)
            if m is None:
                store_fin(p, q, total)
            else:
                outbox[m, p] = total.astype(jnp.bfloat16)
        if m is not None:
            result(m).start()

    def at_age(t, age, act):
        q = t - ready - age
        m = moved_index(q)
        live = (q >= 0) & (q < CHUNKS)

        @pl.when(live & has_own(q))
        def _():
            act(q, q, None)

        if moved:
            @pl.when(live & has_extra(q))
            def _():
                act(q, CHUNKS + m, m)

    def run_forward(q, unit, m):
        if m is not None:
            angle_copy(m).wait_recv()
        compute_forward(q, unit)
        stage0(unit).start()

    ready = 1 + HOP * (n - 2 - jnp.where(middle_layer, 1, 0))

    def forward_step(t, carry):
        @pl.when((t + LEAD < CHUNKS) & middle_layer)
        def _():
            send_own(t + LEAD)

        @pl.when((t < CHUNKS // 2) & middle_layer)
        def _():
            angle_relayout(t)

        for s in range(n - 1):
            q = t - 1 - HOP * s

            @pl.when((q >= 0) & (q < CHUNKS))
            def _():
                for d in range(2):
                    @pl.when(gets(d, s, q))
                    def _():
                        copy(d, s, q).wait_recv()
                        if s + 1 < n - 1:
                            @pl.when(sends(d, s + 1, q))
                            def _():
                                copy(d, s + 1, q).start()

        @pl.when(t < per // 4)
        def _():
            for k in range(4):
                prepare(4 * t + k)

        at_age(t, AGES[2], add2)
        at_age(t, AGES[1], lambda q, unit, m: add1(unit))
        at_age(t, AGES[0], lambda q, unit, m: add0(unit))
        at_age(t, 0, run_forward)
        return carry

    lax.fori_loop(0, CHUNKS + 1 + HOP * (n - 2) + AGES[2], forward_step, 0)

    if moved:
        @pl.when(jnp.logical_not(middle_layer))
        def _():
            for m in range(moved):
                result(m).wait_recv()
                for p in range(2):
                    store_fin(p, 2 * m + FIRST, inbox[m, p].astype(jnp.float32))

    def one(s):
        at = pl.ds(s, 1)
        where = pl.ds(pl.multiple_of(s * pairs, pairs), pairs)
        row_weights = row_table[s]
        column_weights = column_table[s]
        real, imag = fin[0, where, :], fin[1, where, :]
        grid = jnp.concatenate(
            [
                jnp.concatenate([real[:, :rows], imag[:, :rows]], axis=1),
                jnp.concatenate([real[:, rows:], imag[:, rows:]], axis=1),
            ],
            axis=0,
        )
        picked = lax.dot_general(
            grid.astype(jnp.bfloat16), column_weights, (((0,), (0,)), ((), ())),
            preferred_element_type=jnp.float32,
        )
        model_real = jnp.sum(picked[:rows] * row_weights, axis=0, keepdims=True)
        model_imag = jnp.sum(picked[rows:] * row_weights, axis=0, keepdims=True)
        cosine, sine = phase[0, at, :], phase[1, at, :]
        res_real = obs_ref[s, 0:1, :] - (model_real * cosine - model_imag * sine)
        res_imag = obs_ref[s, 1:2, :] - (model_real * sine + model_imag * cosine)
        res_ref[s, 0:1, :] = res_real
        res_ref[s, 1:2, :] = res_imag
        w_real = res_real * cosine + res_imag * sine
        w_imag = res_imag * cosine - res_real * sine
        spread_rows = jnp.concatenate([row_weights * w_real, row_weights * w_imag], axis=0).astype(jnp.bfloat16)
        back = lax.dot_general(
            column_weights, spread_rows, (((1,), (1,)), ((), ())), preferred_element_type=jnp.float32
        )
        adj[0, where, :] = jnp.concatenate([back[:pairs, :rows], back[pairs:, :rows]], axis=1)
        adj[1, where, :] = jnp.concatenate([back[:pairs, rows:], back[pairs:, rows:]], axis=1)

    def four(step, carry):
        for k in range(4):
            one(4 * step + k)
        return carry

    lax.fori_loop(0, per // 4, four, 0)

    def slot(p):
        return bits[p] * 2 + bits[1 - p]

    def own_block(unit, p):
        return every.at[unit, p, core, slot(p)]

    def give(m, p):
        ref = own_block(CHUNKS + m, p)
        return remote(ref, ref, ys.at[0], yr.at[m, p], "layer", jnp.where(middle_layer, outer, inner))

    def gather_a(unit, p):
        ref = own_block(unit, p)
        return remote(ref, ref, sa.at[p], da.at[unit, p], "facet", flip(1 - p))

    def gather_b(unit, p):
        ref = every.at[unit, p, core, pl.ds(bits[p] * 2, 2)]
        return remote(ref, ref, sb.at[p], db.at[unit, p], "facet", flip(p))

    def gather_c(unit):
        ref = every.at[unit, :, core]
        return remote(ref, ref, sc.at[0], dc.at[unit], "facet", other)

    def fill(unit, q):
        for p in range(2):
            for t in range(pq):
                piece = adj[p, pl.ds(q * pq + t, per, stride=pairs), :].astype(jnp.bfloat16)
                every[unit, p, core, slot(p), t * per : (t + 1) * per] = piece

    def fill_step(q, carry):
        @pl.when(has_own(q))
        def _():
            fill(q, q)
            for p in range(2):
                gather_a(q, p).start()

        if moved:
            @pl.when(jnp.logical_not(has_own(q)))
            def _():
                m = moved_index(q)
                fill(CHUNKS + m, q)
                for p in range(2):
                    give(m, p).start()

        return carry

    lax.fori_loop(0, CHUNKS, fill_step, 0)

    def back_copy(direction, j, q):
        step = 1 if direction == 0 else -1
        return remote(
            sbuf.at[direction, j, chunk(q)], rbuf.at[direction, j, chunk(q)],
            bs.at[direction, j], br.at[direction, j - 1 + direction, q], "layer", near(step),
        )

    def behind(direction, q):
        return i > bottom(q) if direction == 0 else i < top(q)

    def compute_backward(q, unit, m):
        twr, twi = tw2_ref[0], tw2_ref[1]
        facr, faci = fac[0], fac[1]
        base = chunk(unit).start
        for pair in range(pq):
            where = slice(pair * per, (pair + 1) * per)
            grids = [
                jnp.concatenate(
                    [every[unit, p, device % 2, place(p, device), where] for device in range(8)], axis=0
                ).astype(jnp.float32)
                for p in range(2)
            ]
            ar, ai = grids
            b = jnp.concatenate([ar * facr + ai * faci, ai * facr - ar * faci], axis=0).astype(jnp.bfloat16)
            h = jnp.dot(g2_ref[...], b, preferred_element_type=jnp.float32)
            hr, hi = h[:subgrids], h[subgrids:]
            mixed = jnp.concatenate([hr * twr + hi * twi, hi * twr - hr * twi], axis=1).astype(jnp.bfloat16)
            image = lax.dot_general(
                f2_ref[...], mixed, (((1,), (1,)), ((), ())), preferred_element_type=jnp.float32
            )
            for c in range(2):
                col = q * cq + 2 * pair + c
                ir = image[2 * c * rows : (2 * c + 1) * rows]
                ii = image[(2 * c + 1) * rows : (2 * c + 2) * rows]
                cosine, sine = cs[base + 2 * pair + c, 0], cs[base + 2 * pair + c, 1]
                tr = (BACK_GAIN * (ir * cosine + ii * sine)).astype(jnp.bfloat16)
                ti = (BACK_GAIN * (ii * cosine - ir * sine)).astype(jnp.bfloat16)
                for l in range(n):
                    for part, value in ((0, tr), (1, ti)):
                        piece = value[l * block : (l + 1) * block]
                        if m is not None:
                            total = term[l, col, part].astype(jnp.float32) + piece.astype(jnp.float32)
                            piece = total.astype(jnp.bfloat16)
                        term[l, col, part] = piece

    def run_backward(q, unit, m):
        gather_c(unit).wait_recv()
        compute_backward(q, unit, m)

    def relay(direction, j, q):
        where = chunk(q)

        @pl.when(behind(direction, q))
        def _():
            back_copy(direction, j, q).wait_recv()
            total = term[j, where].astype(jnp.float32) + rbuf[direction, j, where].astype(jnp.float32)
            sbuf[direction, j, where] = total.astype(jnp.bfloat16)

        @pl.when(jnp.logical_not(behind(direction, q)))
        def _():
            sbuf[direction, j, where] = term[j, where]

        back_copy(direction, j, q).start()

    def units_of(q, act):
        live = (q >= 0) & (q < CHUNKS)

        @pl.when(live & has_own(q))
        def _():
            act(q, q, None)

        if moved:
            @pl.when(live & has_extra(q))
            def _():
                m = moved_index(q)
                act(q, CHUNKS + m, m)

    def to_b(q, unit, m):
        for p in range(2):
            gather_a(unit, p).wait_recv()
            gather_b(unit, p).start()

    def to_c(q, unit, m):
        for p in range(2):
            gather_b(unit, p).wait_recv()
        gather_c(unit).start()

    def pass_on(direction, q, inside):
        kind = is_moved(q) if inside else jnp.logical_not(is_moved(q))

        @pl.when((q >= 0) & (q < CHUNKS) & kind & has_own(q))
        def _():
            for d in range(n - 1, 0, -1):
                j = i + d if direction == 0 else i - d

                @pl.when((j < n) & (j >= 0))
                def _():
                    relay(direction, j, q)

    def backward_step(t, carry):
        if moved:
            early = t + EARLY

            @pl.when((early < CHUNKS) & has_extra(early))
            def _():
                m = moved_index(early)
                for p in range(2):
                    give(m, p).wait_recv()
                    gather_a(CHUNKS + m, p).start()

        units_of(t, to_b)
        units_of(t - SPREAD[0], to_c)
        units_of(t - SPREAD[1], run_backward)
        now = t - SPREAD[1]
        for direction in range(2):
            hops = i if direction == 0 else n - 1 - i
            pass_on(direction, now - LAG * hops, False)
            if moved:
                pass_on(direction, now - LAG * (hops - 1), True)

        last = now - LAG * (n - 1)

        @pl.when(last >= 0)
        def _():
            where = chunk(last)

            @pl.when(has_own(last))
            def _():
                for p in range(2):
                    otmp[p] = term[i, where, p].astype(jnp.float32).reshape(cq * block, subgrids)

            @pl.when(jnp.logical_not(has_own(last)))
            def _():
                otmp[...] = jnp.zeros(otmp.shape, jnp.float32)

            for direction in range(2):
                @pl.when(behind(direction, last))
                def _():
                    back_copy(direction, i, last).wait_recv()
                    for p in range(2):
                        got = rbuf[direction, i, where, p].astype(jnp.float32)
                        otmp[p] += got.reshape(cq * block, subgrids)

            for p in range(2):
                for m in range(block):
                    out_ref[p, where, m * subgrids : (m + 1) * subgrids] = otmp[p, pl.ds(m, cq, stride=block), :]

        return carry

    lax.fori_loop(0, CHUNKS + LAG * (n - 1) + SPREAD[1], backward_step, 0)

    def sent(ref, sem):
        remote(ref, ref, sem, angr.at[0], "facet", other).wait_send()

    def drain(count):
        some = pl.ds(0, count)
        sent(contrib.at[some, 0], s0.at[0])
        sent(every.at[some, :, 0], sc.at[0])
        for p in range(2):
            sent(r1.at[some, 0], s1.at[p])
            sent(r2.at[some, 0], s2.at[p])
            sent(every.at[some, 0, 0, 0], sa.at[p])
            sent(every.at[some, 0, 0, pl.ds(0, 2)], sb.at[p])
        chunks = min(count, CHUNKS)
        for direction in range(2):
            for d in range(1, n):
                j = i + d if direction == 0 else i - d

                @pl.when((j < n) & (j >= 0))
                def _():
                    sent(sbuf.at[direction, 0, pl.ds(0, chunks * cq)], bs.at[direction, j])

    for d in range(2):
        target = i + 1 - 2 * d
        inside = (target >= 1) & (target <= n - 2)
        for s in range(n - 1):
            origin = i - s if d == 0 else i + s
            live = (origin >= 0) & (origin <= n - 1) & (target >= 0) & (target <= n - 1)

            @pl.when(live & inside)
            def _():
                sent(buf.at[0], fs.at[d, s])

            @pl.when(live & jnp.logical_not(inside))
            def _():
                sent(buf.at[0, pl.ds(0, (CHUNKS - moved) * cq)], fs.at[d, s])

    @pl.when(middle_layer)
    def _():
        drain(CHUNKS + moved)
        if moved:
            sent(outbox, xs.at[0])

    @pl.when(jnp.logical_not(middle_layer))
    def _():
        drain(CHUNKS - moved)
        if moved:
            sent(angb.at[pl.ds(0, moved * cq)], angs.at[0])
            sent(every.at[pl.ds(0, moved), :, 0, 0], ys.at[0])


def cs_extra(moved, total):
    return total * moved // (CHUNKS + moved)


def fused(n, moved, x, angle, window, u, v, plane, observed, tables, taps, plane_angle, shift):
    _, cols, _ = x.shape
    per, vis = u.shape
    subgrids = tables[1].shape[0] // 2
    rows = tables[0].shape[0] // 2
    block = rows // n
    pairs = cols // 2
    cq = cols // CHUNKS
    units = CHUNKS + moved
    slab = (cq // 2) * per
    lanes = 2 * rows
    vmem = pl.BlockSpec(memory_space=pltpu.VMEM)
    smem = pl.BlockSpec(memory_space=pltpu.SMEM)
    bf = lambda *shape: pltpu.VMEM(shape, jnp.bfloat16)
    f32 = lambda *shape: pltpu.VMEM(shape, jnp.float32)
    dma = lambda *shape: pltpu.SemaphoreType.DMA(shape)
    box = max(moved, 1)
    return pl.pallas_call(
        functools.partial(fused_kernel, n, moved),
        out_shape=(
            jax.ShapeDtypeStruct((per, 2, vis), jnp.float32),
            jax.ShapeDtypeStruct(x.shape, jnp.float32),
        ),
        in_specs=[vmem] * 13 + [smem] * 3,
        out_specs=(vmem, vmem),
        scratch_shapes=[
            bf(n, cols, 2, block, subgrids), bf(cq * units, rows, subgrids), f32(cq * units, 2, rows, subgrids),
            f32(2, subgrids, lanes), f32(2, 2 * cq * block, subgrids), f32(2 * cq * rows, subgrids),
            bf(units, 2, 2, 4, slab, lanes), bf(units, 2, 4, slab, lanes), bf(units, 2, 4, slab, lanes),
            bf(units, 2, 2, slab, lanes), bf(units, 2, 2, slab, lanes), bf(units, 2, slab, lanes),
            bf(box, 2, slab, lanes), bf(box, 2, slab, lanes),
            f32(2, per * pairs, lanes), f32(2, per * pairs, lanes), f32(2, per, vis),
            f32(per, rows, vis), bf(per, cols, vis),
            bf(units, 2, 2, 4, slab, lanes), bf(n, cols, 2, block, subgrids),
            bf(2, n, cols, 2, block, subgrids), bf(2, n, cols, 2, block, subgrids), f32(2, cq * block, subgrids),
            dma(2, n - 1), dma(2, n - 1, CHUNKS), dma(1), dma(box),
            dma(1), dma(units), dma(2), dma(units, 2), dma(2), dma(units, 2), dma(1), dma(box),
            dma(1), dma(box, 2), dma(2), dma(units, 2), dma(2), dma(units, 2), dma(1), dma(units),
            dma(2, n), dma(2, n - 1, CHUNKS),
        ],
        compiler_params=pltpu.CompilerParams(
            collective_id=2, has_side_effects=True, vmem_limit_bytes=60 * 1024 * 1024
        ),
        name="fused_column",
    )(x, angle, window, u, v, plane, observed, *tables, taps, plane_angle, shift)


def local(n, nf, model_strip, screen_angle, facet_window, facet_shift, kernel_taps, plane_angle, u_cell, v_cell, w_plane, observed):
    _, _, cols, length = screen_angle.shape
    per = u_cell.shape[1]
    subgrids = per * nf
    rows = length // subgrids
    block = rows // n
    vmem = pl.BlockSpec(memory_space=pltpu.VMEM)
    fr, fi = dft(rows)
    gr, gi = dft(subgrids)
    turn = 2.0 * np.pi * (np.arange(rows)[:, None] * np.arange(subgrids)[None, :] % length) / length
    twist = np.stack([np.cos(turn), -np.sin(turn)]).astype(np.float32)
    bf = lambda a: jnp.asarray(a.astype(np.float32)).astype(jnp.bfloat16)
    f1 = bf(np.block([[fr, -fi], [fi, fr]]))
    g1 = bf(np.block([[gr, -gi], [gi, gr]]))
    g2 = bf(np.block([[gr.T, gi.T], [-gi.T, gr.T]]))
    zero = np.zeros_like(fr)
    f2 = bf(
        np.block(
            [
                [fr.T, zero, fi.T, zero],
                [-fi.T, zero, fr.T, zero],
                [zero, fr.T, zero, fi.T],
                [zero, -fi.T, zero, fr.T],
            ]
        )
    )
    tw2 = np.ascontiguousarray(np.tile(np.swapaxes(twist, 1, 2), (1, 1, 2)))
    if nf == 8 and n == 4 and per % 16 == 0 and 2 * rows == subgrids == 128 and cols % (2 * CHUNKS) == 0:
        tables = (f1, g1, jnp.asarray(twist), g2, f2, jnp.asarray(tw2))
        residual, gradient = fused(
            n, MOVED, model_strip[0], screen_angle[0, 0], facet_window.reshape(length // subgrids, subgrids),
            u_cell[0], v_cell[0], w_plane[0], observed[0], tables, kernel_taps, plane_angle, facet_shift,
        )
        return (residual[None], gradient[None])
    factor = facet_factor(facet_window[0], facet_shift[0], subgrids)
    x = model_strip[0].reshape(2, cols, block, subgrids).transpose(1, 0, 2, 3)
    angle = screen_angle[0, 0].reshape(cols, rows, subgrids)
    contrib = pl.pallas_call(
        functools.partial(forward_kernel, n),
        out_shape=jax.ShapeDtypeStruct((2, cols // 2, subgrids, 2 * rows), jnp.bfloat16),
        in_specs=[vmem] * 6,
        out_specs=vmem,
        scratch_shapes=[
            pltpu.VMEM((n, cols, 2, block, subgrids), jnp.bfloat16),
            pltpu.SemaphoreType.DMA((2, n - 1, CHUNKS)),
            pltpu.SemaphoreType.DMA((2, n - 1, CHUNKS)),
            pltpu.SemaphoreType.DMA,
        ],
        compiler_params=pltpu.CompilerParams(collective_id=0, has_side_effects=True),
        name="gather_forward",
    )(x, angle, f1, g1, jnp.asarray(twist), factor)
    parts = contrib.reshape(2, cols // 2, nf, per, 2 * rows)
    received = lax.all_to_all(parts, "facet", split_axis=2, concat_axis=2, tiled=True)
    grids = jnp.sum(received.astype(jnp.float32), axis=2)
    grids = grids.reshape(2, cols // 2, per, 2, rows).transpose(2, 1, 3, 0, 4).reshape(per, cols, 2 * rows)
    residual, adjoint = middle(
        grids, u_cell[0], v_cell[0], w_plane[0], observed[0], plane_angle[0], kernel_taps, rows, cols
    )
    adjoint = adjoint.reshape(per, cols // 2, 2, 2, rows).transpose(3, 1, 0, 2, 4).reshape(2, cols // 2, per, 2 * rows)
    every = lax.all_gather(adjoint, "facet", axis=2, tiled=True)
    gradient = pl.pallas_call(
        functools.partial(backward_kernel, n),
        out_shape=jax.ShapeDtypeStruct((cols, 2, block, subgrids), jnp.float32),
        in_specs=[vmem] * 6,
        out_specs=vmem,
        scratch_shapes=[
            pltpu.VMEM((n, cols, 2, block, subgrids), jnp.bfloat16),
            pltpu.VMEM((2, n, cols, 2, block, subgrids), jnp.bfloat16),
            pltpu.VMEM((2, n, cols, 2, block, subgrids), jnp.bfloat16),
            pltpu.SemaphoreType.DMA((2, n, CHUNKS)),
            pltpu.SemaphoreType.DMA((2, n, CHUNKS)),
        ],
        compiler_params=pltpu.CompilerParams(collective_id=1, has_side_effects=True),
        name="backward_scatter",
    )(every, angle, g2, f2, jnp.asarray(tw2), factor)
    gradient = gradient.transpose(1, 0, 2, 3).reshape(1, 2, cols, block * subgrids)
    return (residual[None], gradient)


def solution(mesh):
    return jax.shard_map(
        functools.partial(local, mesh.shape["layer"], mesh.shape["facet"]),
        mesh=mesh,
        in_specs=(
            P("facet", None, None, "layer"),
            P("layer", "facet", None, None),
            P("facet", None),
            P("facet"),
            P(),
            P("layer", None),
            P("layer", "facet", None),
            P("layer", "facet", None),
            P("layer", "facet", None),
            P("layer", "facet", None, None),
        ),
        out_specs=(P("layer", "facet", None, None), P("facet", None, None, "layer")),
        check_vma=False,
    )
```

```python
import functools
import math

import jax
import jax.numpy as jnp
import numpy as np
from jax import lax
from jax.experimental import pallas as pl
from jax.experimental.pallas import tpu as pltpu
from jax.sharding import PartitionSpec as P

MESH = pl.DeviceIdType.MESH
BACK_GAIN = 8.0
CHUNKS = 8
MOVED = 3
FIRST = 3
EARLY = 2
LEAD = 1
HOP = 2
AGES = (1, 3)
SPREAD = 1
LAG = 2


def _fit(values, degree):
    nodes = np.cos(np.pi * (np.arange(64) + 0.5) / 64)
    y = (nodes + 1.0) * 0.5 * np.pi**2
    cheb = np.polynomial.chebyshev.Chebyshev.fit(y, values(np.sqrt(y)), degree, domain=[0, np.pi**2])
    return [float(v) for v in cheb.convert(kind=np.polynomial.Polynomial).coef]


COS = _fit(np.cos, 8)
SIN = _fit(lambda x: np.sinc(x / np.pi), 7)


def cos_sin(x):
    y = x * x
    c = jnp.full_like(y, COS[-1])
    for v in COS[-2::-1]:
        c = c * y + v
    s = jnp.full_like(y, SIN[-1])
    for v in SIN[-2::-1]:
        s = s * y + v
    return c, s * x


def dft(length):
    k = np.arange(length)
    angles = 2.0 * np.pi * ((k[:, None] * k[None, :]) % length) / length
    scale = 1.0 / math.sqrt(length)
    return np.cos(angles) * scale, -np.sin(angles) * scale


def barrier_line(i, n):
    sem = pltpu.get_barrier_semaphore()

    @pl.when(i > 0)
    def _():
        pl.semaphore_signal(sem, inc=1, device_id={"layer": i - 1}, device_id_type=MESH)

    @pl.when(i < n - 1)
    def _():
        pl.semaphore_signal(sem, inc=1, device_id={"layer": i + 1}, device_id_type=MESH)

    peers = jnp.where(i > 0, 1, 0) + jnp.where(i < n - 1, 1, 0)
    pl.semaphore_wait(sem, peers)


def forward_kernel(n, x_ref, ang_ref, f1_ref, g_ref, tw_ref, fac_ref, out_ref, buf, send_sem, recv_sem, own_sem):
    i = lax.axis_index("layer")
    cq = x_ref.shape[0] // CHUNKS
    subgrids = g_ref.shape[0] // 2
    rows = f1_ref.shape[0] // 2
    barrier_line(i, n)
    own = pltpu.make_async_copy(x_ref, buf.at[i], own_sem)
    own.start()

    def copy(direction, s, q):
        step = 1 if direction == 0 else -1
        origin = jnp.clip(i - step * s, 0, n - 1)
        cols = pl.ds(q * cq, cq)
        src = x_ref.at[cols] if s == 0 else buf.at[origin, cols]
        return pltpu.make_async_remote_copy(
            src_ref=src,
            dst_ref=buf.at[origin, cols],
            send_sem=send_sem.at[direction, s, q],
            recv_sem=recv_sem.at[direction, s, q],
            device_id={"layer": jnp.clip(i + step, 0, n - 1)},
            device_id_type=MESH,
        )

    def sends(direction, s):
        if direction == 0:
            return (i - s >= 0) & (i < n - 1)
        return (i + s <= n - 1) & (i > 0)

    def gets(direction, s):
        return i - 1 - s >= 0 if direction == 0 else i + 1 + s <= n - 1

    def compute(q):
        twr, twi = tw_ref[0], tw_ref[1]
        facr, faci = fac_ref[0], fac_ref[1]
        for pair in range(cq // 2):
            halves = []
            for c in (2 * pair, 2 * pair + 1):
                col = q * cq + c
                xr = jnp.concatenate([buf[l, col, 0] for l in range(n)], axis=0).astype(jnp.float32)
                xi = jnp.concatenate([buf[l, col, 1] for l in range(n)], axis=0).astype(jnp.float32)
                cosine, sine = cos_sin(ang_ref[col].astype(jnp.float32))
                x = jnp.concatenate([xr * cosine - xi * sine, xr * sine + xi * cosine], axis=0)
                h = jnp.dot(f1_ref[...], x.astype(jnp.bfloat16), preferred_element_type=jnp.float32)
                hr, hi = h[:rows], h[rows:]
                halves.append(
                    jnp.concatenate([hr * twr - hi * twi, hr * twi + hi * twr], axis=1).astype(jnp.bfloat16)
                )
            both = jnp.concatenate(halves, axis=0)
            spec = lax.dot_general(
                g_ref[...], both, (((1,), (1,)), ((), ())), preferred_element_type=jnp.float32
            )
            sr, si = spec[:subgrids], spec[subgrids:]
            at = q * (cq // 2) + pair
            out_ref[0, at] = (sr * facr - si * faci).astype(jnp.bfloat16)
            out_ref[1, at] = (sr * faci + si * facr).astype(jnp.bfloat16)

    def body(t, carry):
        @pl.when(t < CHUNKS)
        def _():
            for d in range(2):
                @pl.when(sends(d, 0))
                def _():
                    copy(d, 0, t).start()

        for s in range(n - 1):
            q = t - 1 - s
            @pl.when((q >= 0) & (q < CHUNKS))
            def _():
                for d in range(2):
                    @pl.when(gets(d, s))
                    def _():
                        copy(d, s, q).wait_recv()
                        if s + 1 < n - 1:
                            @pl.when(sends(d, s + 1))
                            def _():
                                copy(d, s + 1, q).start()

        @pl.when(t >= n - 1)
        def _():
            compute(t - (n - 1))

        return carry

    own.wait()
    lax.fori_loop(0, CHUNKS + n - 1, body, 0)

    def drain(q, carry):
        for d in range(2):
            for s in range(n - 1):
                @pl.when(sends(d, s))
                def _():
                    copy(d, s, q).wait_send()
        return carry

    lax.fori_loop(0, CHUNKS, drain, 0)


def backward_kernel(n, a_ref, ang_ref, g_ref, f2_ref, tw_ref, fac_ref, out_ref, term, sbuf, rbuf, send_sem, recv_sem):
    i = lax.axis_index("layer")
    cols = ang_ref.shape[0]
    cq = cols // CHUNKS
    fine = g_ref.shape[0] // 2
    rows = ang_ref.shape[1]
    part = rows // n
    barrier_line(i, n)

    def copy(direction, j, q):
        where = pl.ds(q * cq, cq)
        step = 1 if direction == 0 else -1
        return pltpu.make_async_remote_copy(
            src_ref=sbuf.at[direction, j, where],
            dst_ref=rbuf.at[direction, j, where],
            send_sem=send_sem.at[direction, j, q],
            recv_sem=recv_sem.at[direction, j, q],
            device_id={"layer": jnp.clip(i + step, 0, n - 1)},
            device_id_type=MESH,
        )

    def behind(direction):
        return i > 0 if direction == 0 else i < n - 1

    def compute(q):
        twr, twi = tw_ref[0], tw_ref[1]
        facr, faci = fac_ref[0], fac_ref[1]
        for pair in range(cq // 2):
            at = q * (cq // 2) + pair
            ar = a_ref[0, at].astype(jnp.float32)
            ai = a_ref[1, at].astype(jnp.float32)
            b = jnp.concatenate([ar * facr + ai * faci, ai * facr - ar * faci], axis=0).astype(jnp.bfloat16)
            h = jnp.dot(g_ref[...], b, preferred_element_type=jnp.float32)
            hr, hi = h[:fine], h[fine:]
            mixed = jnp.concatenate([hr * twr + hi * twi, hi * twr - hr * twi], axis=1).astype(jnp.bfloat16)
            image = lax.dot_general(
                f2_ref[...], mixed, (((1,), (1,)), ((), ())), preferred_element_type=jnp.float32
            )
            for c in range(2):
                col = q * cq + 2 * pair + c
                ir = image[2 * c * rows : (2 * c + 1) * rows]
                ii = image[(2 * c + 1) * rows : (2 * c + 2) * rows]
                cosine, sine = cos_sin(ang_ref[col].astype(jnp.float32))
                tr = (BACK_GAIN * (ir * cosine + ii * sine)).astype(jnp.bfloat16)
                ti = (BACK_GAIN * (ii * cosine - ir * sine)).astype(jnp.bfloat16)
                for l in range(n):
                    term[l, col, 0] = tr[l * part : (l + 1) * part]
                    term[l, col, 1] = ti[l * part : (l + 1) * part]

    def relay(direction, j, q):
        where = pl.ds(q * cq, cq)

        @pl.when(behind(direction))
        def _():
            copy(direction, j, q).wait_recv()
            total = term[j, where].astype(jnp.float32) + rbuf[direction, j, where].astype(jnp.float32)
            sbuf[direction, j, where] = total.astype(jnp.bfloat16)

        @pl.when(jnp.logical_not(behind(direction)))
        def _():
            sbuf[direction, j, where] = term[j, where]

        copy(direction, j, q).start()

    def body(t, carry):
        @pl.when(t < CHUNKS)
        def _():
            compute(t)

        for direction in range(2):
            q = t - i if direction == 0 else t - (n - 1 - i)

            @pl.when((q >= 0) & (q < CHUNKS))
            def _():
                for d in range(n - 1, 0, -1):
                    j = i + d if direction == 0 else i - d

                    @pl.when((j < n) & (j >= 0))
                    def _():
                        relay(direction, j, q)

        last = t - (n - 1)

        @pl.when(last >= 0)
        def _():
            where = pl.ds(last * cq, cq)
            out_ref[where] = term[i, where].astype(jnp.float32)
            for direction in range(2):
                @pl.when(behind(direction))
                def _():
                    copy(direction, i, last).wait_recv()
                    out_ref[where] += rbuf[direction, i, where].astype(jnp.float32)

        return carry

    lax.fori_loop(0, CHUNKS + n - 1, body, 0)

    def drain(q, carry):
        for direction in range(2):
            for d in range(1, n):
                j = i + d if direction == 0 else i - d

                @pl.when((j < n) & (j >= 0))
                def _():
                    copy(direction, j, q).wait_send()
        return carry

    lax.fori_loop(0, CHUNKS, drain, 0)


def facet_factor(window, shift_cells, subgrids):
    length = window.shape[0]
    rows = length // subgrids
    grid = window.reshape(subgrids, rows)
    grid = jnp.concatenate([grid, grid], axis=1)
    high = lax.broadcasted_iota(jnp.int32, grid.shape, 0)
    low = lax.broadcasted_iota(jnp.int32, grid.shape, 1) % rows
    turn_count = (high * rows + low) * shift_cells % length
    angles = 2.0 * math.pi / length * turn_count.astype(jnp.float32)
    return jnp.stack([grid * jnp.cos(angles), -grid * jnp.sin(angles)])


def spread(cells, length, taps):
    count = taps.shape[0]
    lanes = jnp.arange(length, dtype=jnp.int32)
    offset = (lanes - cells[..., None] + (count // 2 + length)) % length
    out = jnp.zeros(offset.shape, jnp.float32)
    for t in range(count):
        out = out + jnp.where(offset == t, taps[t], 0.0)
    return out


def middle(grids, u, v, plane, observed, angle, taps, rows, cols):
    row_weights = spread(u, rows, taps)
    column_weights = spread(v, cols, taps).astype(jnp.bfloat16)
    picked = jnp.einsum("sjc,sck->sjk", column_weights, grids.astype(jnp.bfloat16), preferred_element_type=jnp.float32)
    model_real = jnp.sum(picked[..., :rows] * row_weights, axis=2)
    model_imag = jnp.sum(picked[..., rows:] * row_weights, axis=2)
    pick = plane[..., None] == jnp.arange(angle.shape[0], dtype=jnp.int32)
    cosine = jnp.sum(jnp.where(pick, jnp.cos(angle), 0.0), axis=2)
    sine = jnp.sum(jnp.where(pick, jnp.sin(angle), 0.0), axis=2)
    res_real = observed[:, 0] - (model_real * cosine - model_imag * sine)
    res_imag = observed[:, 1] - (model_real * sine + model_imag * cosine)
    w_real = res_real * cosine + res_imag * sine
    w_imag = res_imag * cosine - res_real * sine
    spread_rows = jnp.concatenate(
        [w_real[..., None] * row_weights, w_imag[..., None] * row_weights], axis=2
    ).astype(jnp.bfloat16)
    adjoint = jnp.einsum("sjc,sjk->sck", column_weights, spread_rows, preferred_element_type=jnp.float32)
    return jnp.stack([res_real, res_imag], axis=1), adjoint.astype(jnp.bfloat16)


def fused_kernel(
    n, moved, *refs,
):
    sources, (taps_ref, pang_ref, shift_ref, res_ref, out_ref), held = refs[:13], refs[13:18], refs[18:31]
    (x_ref, ang_ref, win_ref, u_ref, v_ref, plane_ref, obs_ref, f1_ref, g1_ref, tw_ref, g2_ref, f2_ref, tw2_ref) = held
    (
    buf, angb, cs, fac, tmpx, tmpa, contrib, r0, acc0, r1, outbox, inbox, fin, adj, phase, row_table, column_table,
    every, term, sbuf, rbuf, otmp,
    fs, fr, angs, angr, s0, d0, s1, d1, xs, xr, ys, yr, sa, da, sc, dc, bs, br, load,
    ) = refs[31:]
    loads = [pltpu.make_async_copy(a, b, load.at[k]) for k, (a, b) in enumerate(zip(sources, held))]
    for one_load in loads:
        one_load.start()
    cols, rows = angb.shape[0] - cs_extra(moved, angb.shape[0]), angb.shape[1]
    lanes = 2 * rows
    subgrids = g1_ref.shape[0] // 2
    block = rows // n
    per, vis = u_ref.shape
    pairs = cols // 2
    cq = cols // CHUNKS
    pq = cq // 2
    i = lax.axis_index("layer")
    f = lax.axis_index("facet")
    core = lax.rem(f, 2)
    chip = lax.div(f, 2)
    bits = (lax.rem(chip, 2), lax.div(chip, 2))
    other = f + 1 - 2 * core
    middle_layer = (i >= 1) & (i <= n - 2)

    def chip_of(k):
        b0 = 1 - bits[0] if k & 1 else bits[0]
        b1 = 1 - bits[1] if k & 2 else bits[1]
        return b0 + 2 * b1

    def peer_of(k):
        return 2 * chip_of(k) + core

    def near(step):
        return jnp.clip(i + step, 0, n - 1)

    inner = jnp.where(i == 0, 1, n - 2)
    outer = jnp.where(i == 1, 0, n - 1)

    barrier = pltpu.get_barrier_semaphore()
    for peer in (other, peer_of(1), peer_of(2), peer_of(3)):
        pl.semaphore_signal(barrier, inc=1, device_id={"facet": peer}, device_id_type=MESH)

    @pl.when(i > 0)
    def _():
        pl.semaphore_signal(barrier, inc=1, device_id={"layer": i - 1}, device_id_type=MESH)

    @pl.when(i < n - 1)
    def _():
        pl.semaphore_signal(barrier, inc=1, device_id={"layer": i + 1}, device_id_type=MESH)

    pl.semaphore_wait(barrier, 4 + jnp.where(i > 0, 1, 0) + jnp.where(i < n - 1, 1, 0))

    def is_moved(q):
        return (lax.rem(q, 2) == 1) & (q >= FIRST) & (q < FIRST + 2 * moved)

    def moved_index(q):
        return lax.div(q - FIRST, 2)

    def bottom(q):
        return jnp.where(is_moved(q), 1, 0)

    def top(q):
        return jnp.where(is_moved(q), n - 2, n - 1)

    def has_own(q):
        return (i >= bottom(q)) & (i <= top(q))

    def has_extra(q):
        return middle_layer & is_moved(q)

    def remote(src, dst, send, recv, axis, device):
        return pltpu.make_async_remote_copy(
            src_ref=src, dst_ref=dst, send_sem=send, recv_sem=recv, device_id={axis: device}, device_id_type=MESH
        )

    def chunk(q):
        return pl.ds(pl.multiple_of(q * cq, cq), cq)

    def copy(direction, s, q):
        step = 1 if direction == 0 else -1
        origin = jnp.clip(i - step * s, 0, n - 1)
        ref = buf.at[origin, chunk(q)]
        return remote(ref, ref, fs.at[direction, s], fr.at[direction, s, q], "layer", near(step))

    def sends(direction, s, q):
        if direction == 0:
            return (i - s >= 0) & (i + 1 <= top(q))
        return (i + s <= n - 1) & (i - 1 >= bottom(q))

    def gets(direction, s, q):
        if direction == 0:
            return (i - 1 - s >= 0) & (i <= top(q))
        return (i + 1 + s <= n - 1) & (i >= bottom(q))

    def send_own(q):
        for d in range(2):
            @pl.when(sends(d, 0, q))
            def _():
                copy(d, 0, q).start()

    def angle_copy(m):
        src = angb.at[chunk(2 * m + FIRST)]
        dst = angb.at[chunk(CHUNKS + m)]
        return remote(src, dst, angs.at[0], angr.at[m], "layer", inner)

    def relayout(g, carry):
        at = pl.ds(pl.multiple_of(g * 2 * cq, 2 * cq), 2 * cq)
        for p in range(2):
            v = x_ref[p, at, :].astype(jnp.float32)
            for m in range(block):
                tmpx[p, pl.ds(m, 2 * cq, stride=block), :] = v[:, m * subgrids : (m + 1) * subgrids]
            buf[i, at, p] = tmpx[p].reshape(2 * cq, block, subgrids).astype(jnp.bfloat16)

        for k in range(2):
            @pl.when(jnp.logical_not(middle_layer) | (2 * g + k < LEAD))
            def _():
                send_own(2 * g + k)

        @pl.when(jnp.logical_not(middle_layer))
        def _():
            angle_relayout(g)

        return carry

    def angle_relayout(g):
        at = pl.ds(pl.multiple_of(g * 2 * cq, 2 * cq), 2 * cq)
        for m in range(rows):
            piece = ang_ref[at, m * subgrids : (m + 1) * subgrids].astype(jnp.float32)
            tmpa[pl.ds(m, 2 * cq, stride=rows), :] = piece
        angb[at] = tmpa[...].reshape(2 * cq, rows, subgrids).astype(jnp.bfloat16)

        if moved:
            m = g - FIRST // 2

            @pl.when(jnp.logical_not(middle_layer) & (m >= 0) & (m < moved))
            def _():
                angle_copy(m).start()

    loads[0].wait()
    loads[1].wait()
    lax.fori_loop(0, CHUNKS // 2, relayout, 0)
    for one_load in loads[2:]:
        one_load.wait()

    window = win_ref[...]
    rolled = pltpu.roll(window, rows, axis=1)
    left = lax.broadcasted_iota(jnp.int32, window.shape, 1) < rows
    fac[0, pl.ds(0, subgrids // 2, stride=2), :] = jnp.where(left, window, rolled)
    fac[0, pl.ds(1, subgrids // 2, stride=2), :] = jnp.where(left, rolled, window)
    grid = fac[0]
    length = subgrids * rows
    high = lax.broadcasted_iota(jnp.int32, grid.shape, 0)
    low = lax.broadcasted_iota(jnp.int32, grid.shape, 1)
    low = jnp.where(low < rows, low, low - rows)
    turns = lax.rem((high * rows + low) * shift_ref[0], length)
    turns = jnp.where(turns * 2 >= length, turns - length, turns)
    cosine, sine = cos_sin(turns.astype(jnp.float32) * (2.0 * math.pi / length))
    fac[0] = grid * cosine
    fac[1] = -grid * sine

    plane = plane_ref[...]
    angle = jnp.zeros(plane.shape, jnp.float32)
    for k in range(pang_ref.shape[1]):
        angle = jnp.where(plane == k, pang_ref[0, k], angle)
    cosine, sine = cos_sin(angle)
    phase[0] = cosine
    phase[1] = sine

    def weights(cells, position, size):
        count = taps_ref.shape[0]
        offset = position - cells + count // 2
        offset = jnp.where(offset < 0, offset + size, jnp.where(offset >= size, offset - size, offset))
        out = jnp.zeros(offset.shape, jnp.float32)
        for t in range(count):
            out = jnp.where(offset == t, taps_ref[t], out)
        return out

    def prepare(s):
        at = pl.ds(s, 1)
        row = lax.broadcasted_iota(jnp.int32, (rows, vis), 0)
        half = lax.broadcasted_iota(jnp.int32, (pairs, vis), 0)
        col = jnp.concatenate([2 * half, 2 * half + 1], axis=0)
        row_table[s] = weights(u_ref[at, :], row, rows)
        column_table[s] = weights(v_ref[at, :], col, cols).astype(jnp.bfloat16)

    def compute_forward(q, unit):
        twr, twi = tw_ref[0], tw_ref[1]
        facr, faci = fac[0], fac[1]
        base = chunk(unit).start
        for pair in range(pq):
            halves = []
            for c in (2 * pair, 2 * pair + 1):
                col = q * cq + c
                xr_ = jnp.concatenate([buf[l, col, 0] for l in range(n)], axis=0).astype(jnp.float32)
                xi_ = jnp.concatenate([buf[l, col, 1] for l in range(n)], axis=0).astype(jnp.float32)
                cosine, sine = cos_sin(angb[base + c].astype(jnp.float32))
                cs[base + c, 0] = cosine
                cs[base + c, 1] = sine
                x = jnp.concatenate([xr_ * cosine - xi_ * sine, xr_ * sine + xi_ * cosine], axis=0)
                h = jnp.dot(f1_ref[...], x.astype(jnp.bfloat16), preferred_element_type=jnp.float32)
                hr, hi = h[:rows], h[rows:]
                halves.append(
                    jnp.concatenate([hr * twr - hi * twi, hr * twi + hi * twr], axis=1).astype(jnp.bfloat16)
                )
            both = jnp.concatenate(halves, axis=0)
            spec = lax.dot_general(
                g1_ref[...], both, (((1,), (1,)), ((), ())), preferred_element_type=jnp.float32
            )
            sr, si = spec[:subgrids], spec[subgrids:]
            parts = ((sr * facr - si * faci).astype(jnp.bfloat16), (sr * faci + si * facr).astype(jnp.bfloat16))
            for p in range(2):
                for device in range(8):
                    contrib[unit, device % 2, device // 2, p, pair * per : (pair + 1) * per] = parts[p][
                        device * per : (device + 1) * per
                    ]

    def stage0(unit):
        return remote(contrib.at[unit, 1 - core], r0.at[unit], s0.at[0], d0.at[unit], "facet", other)

    def stage1(unit, k):
        src = acc0.at[unit, chip_of(k)]
        return remote(src, r1.at[unit, k - 1], s1.at[k - 1], d1.at[unit, k - 1], "facet", peer_of(k))

    def result(m):
        return remote(outbox.at[m], inbox.at[m], xs.at[0], xr.at[m], "layer", jnp.where(middle_layer, outer, inner))

    def add0(unit):
        stage0(unit).wait_recv()
        total = contrib[unit, core].astype(jnp.float32) + r0[unit].astype(jnp.float32)
        acc0[unit] = total.astype(jnp.bfloat16)
        for k in (3, 1, 2):
            stage1(unit, k).start()

    def store_fin(p, q, total):
        for t in range(pq):
            fin[p, pl.ds(q * pq + t, per, stride=pairs), :] = total[t * per : (t + 1) * per]

    def add2(q, unit, m):
        for k in (1, 2, 3):
            stage1(unit, k).wait_recv()
        for p in range(2):
            total = acc0[unit, chip, p].astype(jnp.float32)
            for k in range(3):
                total = total + r1[unit, k, p].astype(jnp.float32)
            if m is None:
                store_fin(p, q, total)
            else:
                outbox[m, p] = total.astype(jnp.bfloat16)
        if m is not None:
            result(m).start()

    def at_age(t, age, act):
        q = t - ready - age
        m = moved_index(q)
        live = (q >= 0) & (q < CHUNKS)

        @pl.when(live & has_own(q))
        def _():
            act(q, q, None)

        if moved:
            @pl.when(live & has_extra(q))
            def _():
                act(q, CHUNKS + m, m)

    def run_forward(q, unit, m):
        if m is not None:
            angle_copy(m).wait_recv()
        compute_forward(q, unit)
        stage0(unit).start()

    ready = 1 + HOP * (n - 2 - jnp.where(middle_layer, 1, 0))

    def forward_step(t, carry):
        @pl.when((t + LEAD < CHUNKS) & middle_layer)
        def _():
            send_own(t + LEAD)

        @pl.when((t < CHUNKS // 2) & middle_layer)
        def _():
            angle_relayout(t)

        for s in range(n - 1):
            q = t - 1 - HOP * s

            @pl.when((q >= 0) & (q < CHUNKS))
            def _():
                for d in range(2):
                    @pl.when(gets(d, s, q))
                    def _():
                        copy(d, s, q).wait_recv()
                        if s + 1 < n - 1:
                            @pl.when(sends(d, s + 1, q))
                            def _():
                                copy(d, s + 1, q).start()

        @pl.when(t < per // 4)
        def _():
            for k in range(4):
                prepare(4 * t + k)

        at_age(t, AGES[1], add2)
        at_age(t, AGES[0], lambda q, unit, m: add0(unit))
        at_age(t, 0, run_forward)
        return carry

    lax.fori_loop(0, CHUNKS + 1 + HOP * (n - 2) + AGES[1], forward_step, 0)

    if moved:
        @pl.when(jnp.logical_not(middle_layer))
        def _():
            for m in range(moved):
                result(m).wait_recv()
                for p in range(2):
                    store_fin(p, 2 * m + FIRST, inbox[m, p].astype(jnp.float32))

    def one(s):
        at = pl.ds(s, 1)
        where = pl.ds(pl.multiple_of(s * pairs, pairs), pairs)
        row_weights = row_table[s]
        column_weights = column_table[s]
        real, imag = fin[0, where, :], fin[1, where, :]
        grid = jnp.concatenate(
            [
                jnp.concatenate([real[:, :rows], imag[:, :rows]], axis=1),
                jnp.concatenate([real[:, rows:], imag[:, rows:]], axis=1),
            ],
            axis=0,
        )
        picked = lax.dot_general(
            grid.astype(jnp.bfloat16), column_weights, (((0,), (0,)), ((), ())),
            preferred_element_type=jnp.float32,
        )
        model_real = jnp.sum(picked[:rows] * row_weights, axis=0, keepdims=True)
        model_imag = jnp.sum(picked[rows:] * row_weights, axis=0, keepdims=True)
        cosine, sine = phase[0, at, :], phase[1, at, :]
        res_real = obs_ref[s, 0:1, :] - (model_real * cosine - model_imag * sine)
        res_imag = obs_ref[s, 1:2, :] - (model_real * sine + model_imag * cosine)
        res_ref[s, 0:1, :] = res_real
        res_ref[s, 1:2, :] = res_imag
        w_real = res_real * cosine + res_imag * sine
        w_imag = res_imag * cosine - res_real * sine
        spread_rows = jnp.concatenate([row_weights * w_real, row_weights * w_imag], axis=0).astype(jnp.bfloat16)
        back = lax.dot_general(
            column_weights, spread_rows, (((1,), (1,)), ((), ())), preferred_element_type=jnp.float32
        )
        adj[0, where, :] = jnp.concatenate([back[:pairs, :rows], back[pairs:, :rows]], axis=1)
        adj[1, where, :] = jnp.concatenate([back[:pairs, rows:], back[pairs:, rows:]], axis=1)

    def four(step, carry):
        for k in range(4):
            one(4 * step + k)
        return carry

    lax.fori_loop(0, per // 4, four, 0)

    def own_block(unit):
        return every.at[unit, core, chip]

    def give(m):
        ref = own_block(CHUNKS + m)
        return remote(ref, ref, ys.at[0], yr.at[m], "layer", jnp.where(middle_layer, outer, inner))

    def gather(unit, k):
        ref = own_block(unit)
        return remote(ref, ref, sa.at[k - 1], da.at[unit, k - 1], "facet", peer_of(k))

    def gather_core(unit):
        ref = every.at[unit, core]
        return remote(ref, ref, sc.at[0], dc.at[unit], "facet", other)

    def spread_out(unit):
        for k in (3, 1, 2):
            gather(unit, k).start()

    def fill(unit, q):
        for p in range(2):
            for t in range(pq):
                piece = adj[p, pl.ds(q * pq + t, per, stride=pairs), :].astype(jnp.bfloat16)
                every[unit, core, chip, p, t * per : (t + 1) * per] = piece

    def fill_step(q, carry):
        @pl.when(has_own(q))
        def _():
            fill(q, q)
            spread_out(q)

        if moved:
            @pl.when(jnp.logical_not(has_own(q)))
            def _():
                m = moved_index(q)
                fill(CHUNKS + m, q)
                give(m).start()

        return carry

    lax.fori_loop(0, CHUNKS, fill_step, 0)

    def back_copy(direction, j, q):
        step = 1 if direction == 0 else -1
        return remote(
            sbuf.at[direction, j, chunk(q)], rbuf.at[direction, j, chunk(q)],
            bs.at[direction, j], br.at[direction, j - 1 + direction, q], "layer", near(step),
        )

    def behind(direction, q):
        return i > bottom(q) if direction == 0 else i < top(q)

    def compute_backward(q, unit, m):
        twr, twi = tw2_ref[0], tw2_ref[1]
        facr, faci = fac[0], fac[1]
        base = chunk(unit).start
        for pair in range(pq):
            where = slice(pair * per, (pair + 1) * per)
            grids = [
                jnp.concatenate(
                    [every[unit, device % 2, device // 2, p, where] for device in range(8)], axis=0
                ).astype(jnp.float32)
                for p in range(2)
            ]
            ar, ai = grids
            b = jnp.concatenate([ar * facr + ai * faci, ai * facr - ar * faci], axis=0).astype(jnp.bfloat16)
            h = jnp.dot(g2_ref[...], b, preferred_element_type=jnp.float32)
            hr, hi = h[:subgrids], h[subgrids:]
            mixed = jnp.concatenate([hr * twr + hi * twi, hi * twr - hr * twi], axis=1).astype(jnp.bfloat16)
            image = lax.dot_general(
                f2_ref[...], mixed, (((1,), (1,)), ((), ())), preferred_element_type=jnp.float32
            )
            for c in range(2):
                col = q * cq + 2 * pair + c
                ir = image[2 * c * rows : (2 * c + 1) * rows]
                ii = image[(2 * c + 1) * rows : (2 * c + 2) * rows]
                cosine, sine = cs[base + 2 * pair + c, 0], cs[base + 2 * pair + c, 1]
                tr = (BACK_GAIN * (ir * cosine + ii * sine)).astype(jnp.bfloat16)
                ti = (BACK_GAIN * (ii * cosine - ir * sine)).astype(jnp.bfloat16)
                for l in range(n):
                    for part, value in ((0, tr), (1, ti)):
                        piece = value[l * block : (l + 1) * block]
                        if m is not None:
                            total = term[l, col, part].astype(jnp.float32) + piece.astype(jnp.float32)
                            piece = total.astype(jnp.bfloat16)
                        term[l, col, part] = piece

    def run_backward(q, unit, m):
        gather_core(unit).wait_recv()
        compute_backward(q, unit, m)

    def relay(direction, j, q):
        where = chunk(q)

        @pl.when(behind(direction, q))
        def _():
            back_copy(direction, j, q).wait_recv()
            total = term[j, where].astype(jnp.float32) + rbuf[direction, j, where].astype(jnp.float32)
            sbuf[direction, j, where] = total.astype(jnp.bfloat16)

        @pl.when(jnp.logical_not(behind(direction, q)))
        def _():
            sbuf[direction, j, where] = term[j, where]

        back_copy(direction, j, q).start()

    def units_of(q, act):
        live = (q >= 0) & (q < CHUNKS)

        @pl.when(live & has_own(q))
        def _():
            act(q, q, None)

        if moved:
            @pl.when(live & has_extra(q))
            def _():
                m = moved_index(q)
                act(q, CHUNKS + m, m)

    def to_core(q, unit, m):
        for k in (1, 2, 3):
            gather(unit, k).wait_recv()
        gather_core(unit).start()

    def pass_on(direction, q, inside):
        kind = is_moved(q) if inside else jnp.logical_not(is_moved(q))

        @pl.when((q >= 0) & (q < CHUNKS) & kind & has_own(q))
        def _():
            for d in range(n - 1, 0, -1):
                j = i + d if direction == 0 else i - d

                @pl.when((j < n) & (j >= 0))
                def _():
                    relay(direction, j, q)

    def backward_step(t, carry):
        if moved:
            early = t + EARLY

            @pl.when((early < CHUNKS) & has_extra(early))
            def _():
                m = moved_index(early)
                give(m).wait_recv()
                spread_out(CHUNKS + m)

        units_of(t, to_core)
        units_of(t - SPREAD, run_backward)
        now = t - SPREAD
        for direction in range(2):
            hops = i if direction == 0 else n - 1 - i
            pass_on(direction, now - LAG * hops, False)
            if moved:
                pass_on(direction, now - LAG * (hops - 1), True)

        last = now - LAG * (n - 1)

        @pl.when(last >= 0)
        def _():
            where = chunk(last)

            @pl.when(has_own(last))
            def _():
                for p in range(2):
                    otmp[p] = term[i, where, p].astype(jnp.float32).reshape(cq * block, subgrids)

            @pl.when(jnp.logical_not(has_own(last)))
            def _():
                otmp[...] = jnp.zeros(otmp.shape, jnp.float32)

            for direction in range(2):
                @pl.when(behind(direction, last))
                def _():
                    back_copy(direction, i, last).wait_recv()
                    for p in range(2):
                        got = rbuf[direction, i, where, p].astype(jnp.float32)
                        otmp[p] += got.reshape(cq * block, subgrids)

            for p in range(2):
                for m in range(block):
                    out_ref[p, where, m * subgrids : (m + 1) * subgrids] = otmp[p, pl.ds(m, cq, stride=block), :]

        return carry

    lax.fori_loop(0, CHUNKS + LAG * (n - 1) + SPREAD, backward_step, 0)

    def sent(ref, sem):
        remote(ref, ref, sem, angr.at[0], "facet", other).wait_send()

    def drain(count):
        some = pl.ds(0, count)
        sent(contrib.at[some, 0], s0.at[0])
        sent(every.at[some, 0], sc.at[0])
        for k in range(3):
            sent(r1.at[some, 0], s1.at[k])
            sent(every.at[some, 0, 0], sa.at[k])
        chunks = min(count, CHUNKS)
        for direction in range(2):
            for d in range(1, n):
                j = i + d if direction == 0 else i - d

                @pl.when((j < n) & (j >= 0))
                def _():
                    sent(sbuf.at[direction, 0, pl.ds(0, chunks * cq)], bs.at[direction, j])

    for d in range(2):
        target = i + 1 - 2 * d
        inside = (target >= 1) & (target <= n - 2)
        for s in range(n - 1):
            origin = i - s if d == 0 else i + s
            live = (origin >= 0) & (origin <= n - 1) & (target >= 0) & (target <= n - 1)

            @pl.when(live & inside)
            def _():
                sent(buf.at[0], fs.at[d, s])

            @pl.when(live & jnp.logical_not(inside))
            def _():
                sent(buf.at[0, pl.ds(0, (CHUNKS - moved) * cq)], fs.at[d, s])

    @pl.when(middle_layer)
    def _():
        drain(CHUNKS + moved)
        if moved:
            sent(outbox, xs.at[0])

    @pl.when(jnp.logical_not(middle_layer))
    def _():
        drain(CHUNKS - moved)
        if moved:
            sent(angb.at[pl.ds(0, moved * cq)], angs.at[0])
            sent(every.at[pl.ds(0, moved), 0, 0], ys.at[0])


def cs_extra(moved, total):
    return total * moved // (CHUNKS + moved)


def fused(n, moved, x, angle, window, u, v, plane, observed, tables, taps, plane_angle, shift):
    _, cols, _ = x.shape
    per, vis = u.shape
    subgrids = tables[1].shape[0] // 2
    rows = tables[0].shape[0] // 2
    block = rows // n
    pairs = cols // 2
    cq = cols // CHUNKS
    units = CHUNKS + moved
    slab = (cq // 2) * per
    lanes = 2 * rows
    vmem = pl.BlockSpec(memory_space=pltpu.VMEM)
    smem = pl.BlockSpec(memory_space=pltpu.SMEM)
    bf = lambda *shape: pltpu.VMEM(shape, jnp.bfloat16)
    f32 = lambda *shape: pltpu.VMEM(shape, jnp.float32)
    dma = lambda *shape: pltpu.SemaphoreType.DMA(shape)
    box = max(moved, 1)
    arrays = (x, angle, window, u, v, plane, observed, *tables)
    return pl.pallas_call(
        functools.partial(fused_kernel, n, moved),
        out_shape=(
            jax.ShapeDtypeStruct((per, 2, vis), jnp.float32),
            jax.ShapeDtypeStruct(x.shape, jnp.float32),
        ),
        in_specs=[pl.BlockSpec(memory_space=pltpu.HBM)] * 13 + [smem] * 3,
        out_specs=(vmem, vmem),
        scratch_shapes=[
            *[pltpu.VMEM(a.shape, a.dtype) for a in arrays],
            bf(n, cols, 2, block, subgrids), bf(cq * units, rows, subgrids), f32(cq * units, 2, rows, subgrids),
            f32(2, subgrids, lanes), f32(2, 2 * cq * block, subgrids), f32(2 * cq * rows, subgrids),
            bf(units, 2, 4, 2, slab, lanes), bf(units, 4, 2, slab, lanes), bf(units, 4, 2, slab, lanes),
            bf(units, 3, 2, slab, lanes),
            bf(box, 2, slab, lanes), bf(box, 2, slab, lanes),
            f32(2, per * pairs, lanes), f32(2, per * pairs, lanes), f32(2, per, vis),
            f32(per, rows, vis), bf(per, cols, vis),
            bf(units, 2, 4, 2, slab, lanes), bf(n, cols, 2, block, subgrids),
            bf(2, n, cols, 2, block, subgrids), bf(2, n, cols, 2, block, subgrids), f32(2, cq * block, subgrids),
            dma(2, n - 1), dma(2, n - 1, CHUNKS), dma(1), dma(box),
            dma(1), dma(units), dma(3), dma(units, 3), dma(1), dma(box),
            dma(1), dma(box), dma(3), dma(units, 3), dma(1), dma(units),
            dma(2, n), dma(2, n - 1, CHUNKS), dma(13),
        ],
        compiler_params=pltpu.CompilerParams(
            collective_id=2, has_side_effects=True, vmem_limit_bytes=60 * 1024 * 1024
        ),
        name="fused_column",
    )(*arrays, taps, plane_angle, shift)


def local(n, nf, model_strip, screen_angle, facet_window, facet_shift, kernel_taps, plane_angle, u_cell, v_cell, w_plane, observed):
    _, _, cols, length = screen_angle.shape
    per = u_cell.shape[1]
    subgrids = per * nf
    rows = length // subgrids
    block = rows // n
    vmem = pl.BlockSpec(memory_space=pltpu.VMEM)
    fr, fi = dft(rows)
    gr, gi = dft(subgrids)
    turn = 2.0 * np.pi * (np.arange(rows)[:, None] * np.arange(subgrids)[None, :] % length) / length
    twist = np.stack([np.cos(turn), -np.sin(turn)]).astype(np.float32)
    bf = lambda a: jnp.asarray(a.astype(np.float32)).astype(jnp.bfloat16)
    f1 = bf(np.block([[fr, -fi], [fi, fr]]))
    g1 = bf(np.block([[gr, -gi], [gi, gr]]))
    g2 = bf(np.block([[gr.T, gi.T], [-gi.T, gr.T]]))
    zero = np.zeros_like(fr)
    f2 = bf(
        np.block(
            [
                [fr.T, zero, fi.T, zero],
                [-fi.T, zero, fr.T, zero],
                [zero, fr.T, zero, fi.T],
                [zero, -fi.T, zero, fr.T],
            ]
        )
    )
    tw2 = np.ascontiguousarray(np.tile(np.swapaxes(twist, 1, 2), (1, 1, 2)))
    if nf == 8 and n == 4 and per % 16 == 0 and 2 * rows == subgrids == 128 and cols % (2 * CHUNKS) == 0:
        tables = (f1, g1, jnp.asarray(twist), g2, f2, jnp.asarray(tw2))
        residual, gradient = fused(
            n, MOVED, model_strip[0], screen_angle[0, 0], facet_window.reshape(length // subgrids, subgrids),
            u_cell[0], v_cell[0], w_plane[0], observed[0], tables, kernel_taps, plane_angle, facet_shift,
        )
        return (residual[None], gradient[None])
    factor = facet_factor(facet_window[0], facet_shift[0], subgrids)
    x = model_strip[0].reshape(2, cols, block, subgrids).transpose(1, 0, 2, 3)
    angle = screen_angle[0, 0].reshape(cols, rows, subgrids)
    contrib = pl.pallas_call(
        functools.partial(forward_kernel, n),
        out_shape=jax.ShapeDtypeStruct((2, cols // 2, subgrids, 2 * rows), jnp.bfloat16),
        in_specs=[vmem] * 6,
        out_specs=vmem,
        scratch_shapes=[
            pltpu.VMEM((n, cols, 2, block, subgrids), jnp.bfloat16),
            pltpu.SemaphoreType.DMA((2, n - 1, CHUNKS)),
            pltpu.SemaphoreType.DMA((2, n - 1, CHUNKS)),
            pltpu.SemaphoreType.DMA,
        ],
        compiler_params=pltpu.CompilerParams(collective_id=0, has_side_effects=True),
        name="gather_forward",
    )(x, angle, f1, g1, jnp.asarray(twist), factor)
    parts = contrib.reshape(2, cols // 2, nf, per, 2 * rows)
    received = lax.all_to_all(parts, "facet", split_axis=2, concat_axis=2, tiled=True)
    grids = jnp.sum(received.astype(jnp.float32), axis=2)
    grids = grids.reshape(2, cols // 2, per, 2, rows).transpose(2, 1, 3, 0, 4).reshape(per, cols, 2 * rows)
    residual, adjoint = middle(
        grids, u_cell[0], v_cell[0], w_plane[0], observed[0], plane_angle[0], kernel_taps, rows, cols
    )
    adjoint = adjoint.reshape(per, cols // 2, 2, 2, rows).transpose(3, 1, 0, 2, 4).reshape(2, cols // 2, per, 2 * rows)
    every = lax.all_gather(adjoint, "facet", axis=2, tiled=True)
    gradient = pl.pallas_call(
        functools.partial(backward_kernel, n),
        out_shape=jax.ShapeDtypeStruct((cols, 2, block, subgrids), jnp.float32),
        in_specs=[vmem] * 6,
        out_specs=vmem,
        scratch_shapes=[
            pltpu.VMEM((n, cols, 2, block, subgrids), jnp.bfloat16),
            pltpu.VMEM((2, n, cols, 2, block, subgrids), jnp.bfloat16),
            pltpu.VMEM((2, n, cols, 2, block, subgrids), jnp.bfloat16),
            pltpu.SemaphoreType.DMA((2, n, CHUNKS)),
            pltpu.SemaphoreType.DMA((2, n, CHUNKS)),
        ],
        compiler_params=pltpu.CompilerParams(collective_id=1, has_side_effects=True),
        name="backward_scatter",
    )(every, angle, g2, f2, jnp.asarray(tw2), factor)
    gradient = gradient.transpose(1, 0, 2, 3).reshape(1, 2, cols, block * subgrids)
    return (residual[None], gradient)


def solution(mesh):
    return jax.shard_map(
        functools.partial(local, mesh.shape["layer"], mesh.shape["facet"]),
        mesh=mesh,
        in_specs=(
            P("facet", None, None, "layer"),
            P("layer", "facet", None, None),
            P("facet", None),
            P("facet"),
            P(),
            P("layer", None),
            P("layer", "facet", None),
            P("layer", "facet", None),
            P("layer", "facet", None),
            P("layer", "facet", None, None),
        ),
        out_specs=(P("layer", "facet", None, None), P("facet", None, None, "layer")),
        check_vma=False,
    )
```

```python
import functools
import math

import jax
import jax.numpy as jnp
import numpy as np
from jax import lax
from jax.experimental import pallas as pl
from jax.experimental.pallas import tpu as pltpu
from jax.sharding import PartitionSpec as P

MESH = pl.DeviceIdType.MESH
BACK_GAIN = 8.0
CHUNKS = 8
MOVED = 3
FIRST = 3
EARLY = 2
LEAD = 1
HOP = 2
AGES = (1, 3)
SPREAD = 1
LAG = 2


def _fit(values, degree):
    nodes = np.cos(np.pi * (np.arange(64) + 0.5) / 64)
    y = (nodes + 1.0) * 0.5 * np.pi**2
    cheb = np.polynomial.chebyshev.Chebyshev.fit(y, values(np.sqrt(y)), degree, domain=[0, np.pi**2])
    return [float(v) for v in cheb.convert(kind=np.polynomial.Polynomial).coef]


COS = _fit(np.cos, 8)
SIN = _fit(lambda x: np.sinc(x / np.pi), 7)


def cos_sin(x):
    y = x * x
    c = jnp.full_like(y, COS[-1])
    for v in COS[-2::-1]:
        c = c * y + v
    s = jnp.full_like(y, SIN[-1])
    for v in SIN[-2::-1]:
        s = s * y + v
    return c, s * x


def dft(length):
    k = np.arange(length)
    angles = 2.0 * np.pi * ((k[:, None] * k[None, :]) % length) / length
    scale = 1.0 / math.sqrt(length)
    return np.cos(angles) * scale, -np.sin(angles) * scale


def barrier_line(i, n):
    sem = pltpu.get_barrier_semaphore()

    @pl.when(i > 0)
    def _():
        pl.semaphore_signal(sem, inc=1, device_id={"layer": i - 1}, device_id_type=MESH)

    @pl.when(i < n - 1)
    def _():
        pl.semaphore_signal(sem, inc=1, device_id={"layer": i + 1}, device_id_type=MESH)

    peers = jnp.where(i > 0, 1, 0) + jnp.where(i < n - 1, 1, 0)
    pl.semaphore_wait(sem, peers)


def forward_kernel(n, x_ref, ang_ref, f1_ref, g_ref, tw_ref, fac_ref, out_ref, buf, send_sem, recv_sem, own_sem):
    i = lax.axis_index("layer")
    cq = x_ref.shape[0] // CHUNKS
    subgrids = g_ref.shape[0] // 2
    rows = f1_ref.shape[0] // 2
    barrier_line(i, n)
    own = pltpu.make_async_copy(x_ref, buf.at[i], own_sem)
    own.start()

    def copy(direction, s, q):
        step = 1 if direction == 0 else -1
        origin = jnp.clip(i - step * s, 0, n - 1)
        cols = pl.ds(q * cq, cq)
        src = x_ref.at[cols] if s == 0 else buf.at[origin, cols]
        return pltpu.make_async_remote_copy(
            src_ref=src,
            dst_ref=buf.at[origin, cols],
            send_sem=send_sem.at[direction, s, q],
            recv_sem=recv_sem.at[direction, s, q],
            device_id={"layer": jnp.clip(i + step, 0, n - 1)},
            device_id_type=MESH,
        )

    def sends(direction, s):
        if direction == 0:
            return (i - s >= 0) & (i < n - 1)
        return (i + s <= n - 1) & (i > 0)

    def gets(direction, s):
        return i - 1 - s >= 0 if direction == 0 else i + 1 + s <= n - 1

    def compute(q):
        twr, twi = tw_ref[0], tw_ref[1]
        facr, faci = fac_ref[0], fac_ref[1]
        for pair in range(cq // 2):
            halves = []
            for c in (2 * pair, 2 * pair + 1):
                col = q * cq + c
                xr = jnp.concatenate([buf[l, col, 0] for l in range(n)], axis=0).astype(jnp.float32)
                xi = jnp.concatenate([buf[l, col, 1] for l in range(n)], axis=0).astype(jnp.float32)
                cosine, sine = cos_sin(ang_ref[col].astype(jnp.float32))
                x = jnp.concatenate([xr * cosine - xi * sine, xr * sine + xi * cosine], axis=0)
                h = jnp.dot(f1_ref[...], x.astype(jnp.bfloat16), preferred_element_type=jnp.float32)
                hr, hi = h[:rows], h[rows:]
                halves.append(
                    jnp.concatenate([hr * twr - hi * twi, hr * twi + hi * twr], axis=1).astype(jnp.bfloat16)
                )
            both = jnp.concatenate(halves, axis=0)
            spec = lax.dot_general(
                g_ref[...], both, (((1,), (1,)), ((), ())), preferred_element_type=jnp.float32
            )
            sr, si = spec[:subgrids], spec[subgrids:]
            at = q * (cq // 2) + pair
            out_ref[0, at] = (sr * facr - si * faci).astype(jnp.bfloat16)
            out_ref[1, at] = (sr * faci + si * facr).astype(jnp.bfloat16)

    def body(t, carry):
        @pl.when(t < CHUNKS)
        def _():
            for d in range(2):
                @pl.when(sends(d, 0))
                def _():
                    copy(d, 0, t).start()

        for s in range(n - 1):
            q = t - 1 - s
            @pl.when((q >= 0) & (q < CHUNKS))
            def _():
                for d in range(2):
                    @pl.when(gets(d, s))
                    def _():
                        copy(d, s, q).wait_recv()
                        if s + 1 < n - 1:
                            @pl.when(sends(d, s + 1))
                            def _():
                                copy(d, s + 1, q).start()

        @pl.when(t >= n - 1)
        def _():
            compute(t - (n - 1))

        return carry

    own.wait()
    lax.fori_loop(0, CHUNKS + n - 1, body, 0)

    def drain(q, carry):
        for d in range(2):
            for s in range(n - 1):
                @pl.when(sends(d, s))
                def _():
                    copy(d, s, q).wait_send()
        return carry

    lax.fori_loop(0, CHUNKS, drain, 0)


def backward_kernel(n, a_ref, ang_ref, g_ref, f2_ref, tw_ref, fac_ref, out_ref, term, sbuf, rbuf, send_sem, recv_sem):
    i = lax.axis_index("layer")
    cols = ang_ref.shape[0]
    cq = cols // CHUNKS
    fine = g_ref.shape[0] // 2
    rows = ang_ref.shape[1]
    part = rows // n
    barrier_line(i, n)

    def copy(direction, j, q):
        where = pl.ds(q * cq, cq)
        step = 1 if direction == 0 else -1
        return pltpu.make_async_remote_copy(
            src_ref=sbuf.at[direction, j, where],
            dst_ref=rbuf.at[direction, j, where],
            send_sem=send_sem.at[direction, j, q],
            recv_sem=recv_sem.at[direction, j, q],
            device_id={"layer": jnp.clip(i + step, 0, n - 1)},
            device_id_type=MESH,
        )

    def behind(direction):
        return i > 0 if direction == 0 else i < n - 1

    def compute(q):
        twr, twi = tw_ref[0], tw_ref[1]
        facr, faci = fac_ref[0], fac_ref[1]
        for pair in range(cq // 2):
            at = q * (cq // 2) + pair
            ar = a_ref[0, at].astype(jnp.float32)
            ai = a_ref[1, at].astype(jnp.float32)
            b = jnp.concatenate([ar * facr + ai * faci, ai * facr - ar * faci], axis=0).astype(jnp.bfloat16)
            h = jnp.dot(g_ref[...], b, preferred_element_type=jnp.float32)
            hr, hi = h[:fine], h[fine:]
            mixed = jnp.concatenate([hr * twr + hi * twi, hi * twr - hr * twi], axis=1).astype(jnp.bfloat16)
            image = lax.dot_general(
                f2_ref[...], mixed, (((1,), (1,)), ((), ())), preferred_element_type=jnp.float32
            )
            for c in range(2):
                col = q * cq + 2 * pair + c
                ir = image[2 * c * rows : (2 * c + 1) * rows]
                ii = image[(2 * c + 1) * rows : (2 * c + 2) * rows]
                cosine, sine = cos_sin(ang_ref[col].astype(jnp.float32))
                tr = (BACK_GAIN * (ir * cosine + ii * sine)).astype(jnp.bfloat16)
                ti = (BACK_GAIN * (ii * cosine - ir * sine)).astype(jnp.bfloat16)
                for l in range(n):
                    term[l, col, 0] = tr[l * part : (l + 1) * part]
                    term[l, col, 1] = ti[l * part : (l + 1) * part]

    def relay(direction, j, q):
        where = pl.ds(q * cq, cq)

        @pl.when(behind(direction))
        def _():
            copy(direction, j, q).wait_recv()
            total = term[j, where].astype(jnp.float32) + rbuf[direction, j, where].astype(jnp.float32)
            sbuf[direction, j, where] = total.astype(jnp.bfloat16)

        @pl.when(jnp.logical_not(behind(direction)))
        def _():
            sbuf[direction, j, where] = term[j, where]

        copy(direction, j, q).start()

    def body(t, carry):
        @pl.when(t < CHUNKS)
        def _():
            compute(t)

        for direction in range(2):
            q = t - i if direction == 0 else t - (n - 1 - i)

            @pl.when((q >= 0) & (q < CHUNKS))
            def _():
                for d in range(n - 1, 0, -1):
                    j = i + d if direction == 0 else i - d

                    @pl.when((j < n) & (j >= 0))
                    def _():
                        relay(direction, j, q)

        last = t - (n - 1)

        @pl.when(last >= 0)
        def _():
            where = pl.ds(last * cq, cq)
            out_ref[where] = term[i, where].astype(jnp.float32)
            for direction in range(2):
                @pl.when(behind(direction))
                def _():
                    copy(direction, i, last).wait_recv()
                    out_ref[where] += rbuf[direction, i, where].astype(jnp.float32)

        return carry

    lax.fori_loop(0, CHUNKS + n - 1, body, 0)

    def drain(q, carry):
        for direction in range(2):
            for d in range(1, n):
                j = i + d if direction == 0 else i - d

                @pl.when((j < n) & (j >= 0))
                def _():
                    copy(direction, j, q).wait_send()
        return carry

    lax.fori_loop(0, CHUNKS, drain, 0)


def facet_factor(window, shift_cells, subgrids):
    length = window.shape[0]
    rows = length // subgrids
    grid = window.reshape(subgrids, rows)
    grid = jnp.concatenate([grid, grid], axis=1)
    high = lax.broadcasted_iota(jnp.int32, grid.shape, 0)
    low = lax.broadcasted_iota(jnp.int32, grid.shape, 1) % rows
    turn_count = (high * rows + low) * shift_cells % length
    angles = 2.0 * math.pi / length * turn_count.astype(jnp.float32)
    return jnp.stack([grid * jnp.cos(angles), -grid * jnp.sin(angles)])


def spread(cells, length, taps):
    count = taps.shape[0]
    lanes = jnp.arange(length, dtype=jnp.int32)
    offset = (lanes - cells[..., None] + (count // 2 + length)) % length
    out = jnp.zeros(offset.shape, jnp.float32)
    for t in range(count):
        out = out + jnp.where(offset == t, taps[t], 0.0)
    return out


def middle(grids, u, v, plane, observed, angle, taps, rows, cols):
    row_weights = spread(u, rows, taps)
    column_weights = spread(v, cols, taps).astype(jnp.bfloat16)
    picked = jnp.einsum("sjc,sck->sjk", column_weights, grids.astype(jnp.bfloat16), preferred_element_type=jnp.float32)
    model_real = jnp.sum(picked[..., :rows] * row_weights, axis=2)
    model_imag = jnp.sum(picked[..., rows:] * row_weights, axis=2)
    pick = plane[..., None] == jnp.arange(angle.shape[0], dtype=jnp.int32)
    cosine = jnp.sum(jnp.where(pick, jnp.cos(angle), 0.0), axis=2)
    sine = jnp.sum(jnp.where(pick, jnp.sin(angle), 0.0), axis=2)
    res_real = observed[:, 0] - (model_real * cosine - model_imag * sine)
    res_imag = observed[:, 1] - (model_real * sine + model_imag * cosine)
    w_real = res_real * cosine + res_imag * sine
    w_imag = res_imag * cosine - res_real * sine
    spread_rows = jnp.concatenate(
        [w_real[..., None] * row_weights, w_imag[..., None] * row_weights], axis=2
    ).astype(jnp.bfloat16)
    adjoint = jnp.einsum("sjc,sjk->sck", column_weights, spread_rows, preferred_element_type=jnp.float32)
    return jnp.stack([res_real, res_imag], axis=1), adjoint.astype(jnp.bfloat16)


def fused_kernel(
    n, moved, *refs,
):
    sources, (taps_ref, pang_ref, shift_ref, res_out, grad_out), held = refs[:13], refs[13:18], refs[18:31]
    (x_ref, ang_ref, win_ref, u_ref, v_ref, plane_ref, obs_ref, f1_ref, g1_ref, tw_ref, g2_ref, f2_ref, tw2_ref) = held
    (
    buf, angb, cs, fac, tmpx, tmpa, contrib, r0, acc0, r1, outbox, inbox, fin, adj, phase, row_table, column_table,
    every, term, sbuf, rbuf, otmp,
    fs, fr, angs, angr, s0, d0, s1, d1, xs, xr, ys, yr, sa, da, sc, dc, bs, br, load, store, res_ref, out_ref,
    ) = refs[31:]
    loads = [pltpu.make_async_copy(a, b, load.at[k]) for k, (a, b) in enumerate(zip(sources, held))]
    for one_load in loads:
        one_load.start()
    cols, rows = angb.shape[0] - cs_extra(moved, angb.shape[0]), angb.shape[1]
    lanes = 2 * rows
    subgrids = g1_ref.shape[0] // 2
    block = rows // n
    per, vis = u_ref.shape
    pairs = cols // 2
    cq = cols // CHUNKS
    pq = cq // 2
    i = lax.axis_index("layer")
    f = lax.axis_index("facet")
    core = lax.rem(f, 2)
    chip = lax.div(f, 2)
    bits = (lax.rem(chip, 2), lax.div(chip, 2))
    other = f + 1 - 2 * core
    middle_layer = (i >= 1) & (i <= n - 2)

    def chip_of(k):
        b0 = 1 - bits[0] if k & 1 else bits[0]
        b1 = 1 - bits[1] if k & 2 else bits[1]
        return b0 + 2 * b1

    def peer_of(k):
        return 2 * chip_of(k) + core

    def near(step):
        return jnp.clip(i + step, 0, n - 1)

    inner = jnp.where(i == 0, 1, n - 2)
    outer = jnp.where(i == 1, 0, n - 1)

    barrier = pltpu.get_barrier_semaphore()
    for peer in (other, peer_of(1), peer_of(2), peer_of(3)):
        pl.semaphore_signal(barrier, inc=1, device_id={"facet": peer}, device_id_type=MESH)

    @pl.when(i > 0)
    def _():
        pl.semaphore_signal(barrier, inc=1, device_id={"layer": i - 1}, device_id_type=MESH)

    @pl.when(i < n - 1)
    def _():
        pl.semaphore_signal(barrier, inc=1, device_id={"layer": i + 1}, device_id_type=MESH)

    pl.semaphore_wait(barrier, 4 + jnp.where(i > 0, 1, 0) + jnp.where(i < n - 1, 1, 0))

    def is_moved(q):
        return (lax.rem(q, 2) == 1) & (q >= FIRST) & (q < FIRST + 2 * moved)

    def moved_index(q):
        return lax.div(q - FIRST, 2)

    def bottom(q):
        return jnp.where(is_moved(q), 1, 0)

    def top(q):
        return jnp.where(is_moved(q), n - 2, n - 1)

    def has_own(q):
        return (i >= bottom(q)) & (i <= top(q))

    def has_extra(q):
        return middle_layer & is_moved(q)

    def remote(src, dst, send, recv, axis, device):
        return pltpu.make_async_remote_copy(
            src_ref=src, dst_ref=dst, send_sem=send, recv_sem=recv, device_id={axis: device}, device_id_type=MESH
        )

    def chunk(q):
        return pl.ds(pl.multiple_of(q * cq, cq), cq)

    def copy(direction, s, q):
        step = 1 if direction == 0 else -1
        origin = jnp.clip(i - step * s, 0, n - 1)
        ref = buf.at[origin, chunk(q)]
        return remote(ref, ref, fs.at[direction, s], fr.at[direction, s, q], "layer", near(step))

    def sends(direction, s, q):
        if direction == 0:
            return (i - s >= 0) & (i + 1 <= top(q))
        return (i + s <= n - 1) & (i - 1 >= bottom(q))

    def gets(direction, s, q):
        if direction == 0:
            return (i - 1 - s >= 0) & (i <= top(q))
        return (i + 1 + s <= n - 1) & (i >= bottom(q))

    def send_own(q):
        for d in range(2):
            @pl.when(sends(d, 0, q))
            def _():
                copy(d, 0, q).start()

    def angle_copy(m):
        src = angb.at[chunk(2 * m + FIRST)]
        dst = angb.at[chunk(CHUNKS + m)]
        return remote(src, dst, angs.at[0], angr.at[m], "layer", inner)

    def relayout(g, carry):
        at = pl.ds(pl.multiple_of(g * 2 * cq, 2 * cq), 2 * cq)
        for p in range(2):
            v = x_ref[p, at, :].astype(jnp.float32)
            for m in range(block):
                tmpx[p, pl.ds(m, 2 * cq, stride=block), :] = v[:, m * subgrids : (m + 1) * subgrids]
            buf[i, at, p] = tmpx[p].reshape(2 * cq, block, subgrids).astype(jnp.bfloat16)

        for k in range(2):
            @pl.when(jnp.logical_not(middle_layer) | (2 * g + k < LEAD))
            def _():
                send_own(2 * g + k)

        @pl.when(jnp.logical_not(middle_layer))
        def _():
            angle_relayout(g)

        return carry

    def angle_relayout(g):
        at = pl.ds(pl.multiple_of(g * 2 * cq, 2 * cq), 2 * cq)
        for m in range(rows):
            piece = ang_ref[at, m * subgrids : (m + 1) * subgrids].astype(jnp.float32)
            tmpa[pl.ds(m, 2 * cq, stride=rows), :] = piece
        angb[at] = tmpa[...].reshape(2 * cq, rows, subgrids).astype(jnp.bfloat16)

        if moved:
            m = g - FIRST // 2

            @pl.when(jnp.logical_not(middle_layer) & (m >= 0) & (m < moved))
            def _():
                angle_copy(m).start()

    loads[0].wait()
    loads[1].wait()
    lax.fori_loop(0, CHUNKS // 2, relayout, 0)
    for one_load in loads[2:]:
        one_load.wait()

    window = win_ref[...]
    rolled = pltpu.roll(window, rows, axis=1)
    left = lax.broadcasted_iota(jnp.int32, window.shape, 1) < rows
    fac[0, pl.ds(0, subgrids // 2, stride=2), :] = jnp.where(left, window, rolled)
    fac[0, pl.ds(1, subgrids // 2, stride=2), :] = jnp.where(left, rolled, window)
    grid = fac[0]
    length = subgrids * rows
    high = lax.broadcasted_iota(jnp.int32, grid.shape, 0)
    low = lax.broadcasted_iota(jnp.int32, grid.shape, 1)
    low = jnp.where(low < rows, low, low - rows)
    turns = lax.rem((high * rows + low) * shift_ref[0], length)
    turns = jnp.where(turns * 2 >= length, turns - length, turns)
    cosine, sine = cos_sin(turns.astype(jnp.float32) * (2.0 * math.pi / length))
    fac[0] = grid * cosine
    fac[1] = -grid * sine

    plane = plane_ref[...]
    angle = jnp.zeros(plane.shape, jnp.float32)
    for k in range(pang_ref.shape[1]):
        angle = jnp.where(plane == k, pang_ref[0, k], angle)
    cosine, sine = cos_sin(angle)
    phase[0] = cosine
    phase[1] = sine

    def weights(cells, position, size):
        count = taps_ref.shape[0]
        offset = position - cells + count // 2
        offset = jnp.where(offset < 0, offset + size, jnp.where(offset >= size, offset - size, offset))
        out = jnp.zeros(offset.shape, jnp.float32)
        for t in range(count):
            out = jnp.where(offset == t, taps_ref[t], out)
        return out

    def prepare(s):
        at = pl.ds(s, 1)
        row = lax.broadcasted_iota(jnp.int32, (rows, vis), 0)
        half = lax.broadcasted_iota(jnp.int32, (pairs, vis), 0)
        col = jnp.concatenate([2 * half, 2 * half + 1], axis=0)
        row_table[s] = weights(u_ref[at, :], row, rows)
        column_table[s] = weights(v_ref[at, :], col, cols).astype(jnp.bfloat16)

    def compute_forward(q, unit):
        twr, twi = tw_ref[0], tw_ref[1]
        facr, faci = fac[0], fac[1]
        base = chunk(unit).start
        for pair in range(pq):
            halves = []
            for c in (2 * pair, 2 * pair + 1):
                col = q * cq + c
                xr_ = jnp.concatenate([buf[l, col, 0] for l in range(n)], axis=0).astype(jnp.float32)
                xi_ = jnp.concatenate([buf[l, col, 1] for l in range(n)], axis=0).astype(jnp.float32)
                cosine, sine = cos_sin(angb[base + c].astype(jnp.float32))
                cs[base + c, 0] = cosine
                cs[base + c, 1] = sine
                x = jnp.concatenate([xr_ * cosine - xi_ * sine, xr_ * sine + xi_ * cosine], axis=0)
                h = jnp.dot(f1_ref[...], x.astype(jnp.bfloat16), preferred_element_type=jnp.float32)
                hr, hi = h[:rows], h[rows:]
                halves.append(
                    jnp.concatenate([hr * twr - hi * twi, hr * twi + hi * twr], axis=1).astype(jnp.bfloat16)
                )
            both = jnp.concatenate(halves, axis=0)
            spec = lax.dot_general(
                g1_ref[...], both, (((1,), (1,)), ((), ())), preferred_element_type=jnp.float32
            )
            sr, si = spec[:subgrids], spec[subgrids:]
            parts = ((sr * facr - si * faci).astype(jnp.bfloat16), (sr * faci + si * facr).astype(jnp.bfloat16))
            for p in range(2):
                for device in range(8):
                    contrib[unit, device % 2, device // 2, p, pair * per : (pair + 1) * per] = parts[p][
                        device * per : (device + 1) * per
                    ]

    def stage0(unit):
        return remote(contrib.at[unit, 1 - core], r0.at[unit], s0.at[0], d0.at[unit], "facet", other)

    def stage1(unit, k):
        src = acc0.at[unit, chip_of(k)]
        return remote(src, r1.at[unit, k - 1], s1.at[k - 1], d1.at[unit, k - 1], "facet", peer_of(k))

    def result(m):
        return remote(outbox.at[m], inbox.at[m], xs.at[0], xr.at[m], "layer", jnp.where(middle_layer, outer, inner))

    def add0(unit):
        stage0(unit).wait_recv()
        total = contrib[unit, core].astype(jnp.float32) + r0[unit].astype(jnp.float32)
        acc0[unit] = total.astype(jnp.bfloat16)
        for k in (3, 1, 2):
            stage1(unit, k).start()

    def store_fin(p, q, total):
        for t in range(pq):
            fin[p, pl.ds(q * pq + t, per, stride=pairs), :] = total[t * per : (t + 1) * per]

    def add2(q, unit, m):
        for k in (1, 2, 3):
            stage1(unit, k).wait_recv()
        for p in range(2):
            total = acc0[unit, chip, p].astype(jnp.float32)
            for k in range(3):
                total = total + r1[unit, k, p].astype(jnp.float32)
            if m is None:
                store_fin(p, q, total)
            else:
                outbox[m, p] = total.astype(jnp.bfloat16)
        if m is not None:
            result(m).start()

    def at_age(t, age, act):
        q = t - ready - age
        m = moved_index(q)
        live = (q >= 0) & (q < CHUNKS)

        @pl.when(live & has_own(q))
        def _():
            act(q, q, None)

        if moved:
            @pl.when(live & has_extra(q))
            def _():
                act(q, CHUNKS + m, m)

    def run_forward(q, unit, m):
        if m is not None:
            angle_copy(m).wait_recv()
        compute_forward(q, unit)
        stage0(unit).start()

    ready = 1 + HOP * (n - 2 - jnp.where(middle_layer, 1, 0))

    def forward_step(t, carry):
        @pl.when((t + LEAD < CHUNKS) & middle_layer)
        def _():
            send_own(t + LEAD)

        @pl.when((t < CHUNKS // 2) & middle_layer)
        def _():
            angle_relayout(t)

        for s in range(n - 1):
            q = t - 1 - HOP * s

            @pl.when((q >= 0) & (q < CHUNKS))
            def _():
                for d in range(2):
                    @pl.when(gets(d, s, q))
                    def _():
                        copy(d, s, q).wait_recv()
                        if s + 1 < n - 1:
                            @pl.when(sends(d, s + 1, q))
                            def _():
                                copy(d, s + 1, q).start()

        @pl.when(t < per // 4)
        def _():
            for k in range(4):
                prepare(4 * t + k)

        at_age(t, AGES[1], add2)
        at_age(t, AGES[0], lambda q, unit, m: add0(unit))
        at_age(t, 0, run_forward)
        return carry

    lax.fori_loop(0, CHUNKS + 1 + HOP * (n - 2) + AGES[1], forward_step, 0)

    if moved:
        @pl.when(jnp.logical_not(middle_layer))
        def _():
            for m in range(moved):
                result(m).wait_recv()
                for p in range(2):
                    store_fin(p, 2 * m + FIRST, inbox[m, p].astype(jnp.float32))

    def one(s):
        at = pl.ds(s, 1)
        where = pl.ds(pl.multiple_of(s * pairs, pairs), pairs)
        row_weights = row_table[s]
        column_weights = column_table[s]
        real, imag = fin[0, where, :], fin[1, where, :]
        grid = jnp.concatenate(
            [
                jnp.concatenate([real[:, :rows], imag[:, :rows]], axis=1),
                jnp.concatenate([real[:, rows:], imag[:, rows:]], axis=1),
            ],
            axis=0,
        )
        picked = lax.dot_general(
            grid.astype(jnp.bfloat16), column_weights, (((0,), (0,)), ((), ())),
            preferred_element_type=jnp.float32,
        )
        model_real = jnp.sum(picked[:rows] * row_weights, axis=0, keepdims=True)
        model_imag = jnp.sum(picked[rows:] * row_weights, axis=0, keepdims=True)
        cosine, sine = phase[0, at, :], phase[1, at, :]
        res_real = obs_ref[s, 0:1, :] - (model_real * cosine - model_imag * sine)
        res_imag = obs_ref[s, 1:2, :] - (model_real * sine + model_imag * cosine)
        res_ref[s, 0:1, :] = res_real
        res_ref[s, 1:2, :] = res_imag
        w_real = res_real * cosine + res_imag * sine
        w_imag = res_imag * cosine - res_real * sine
        spread_rows = jnp.concatenate([row_weights * w_real, row_weights * w_imag], axis=0).astype(jnp.bfloat16)
        back = lax.dot_general(
            column_weights, spread_rows, (((1,), (1,)), ((), ())), preferred_element_type=jnp.float32
        )
        adj[0, where, :] = jnp.concatenate([back[:pairs, :rows], back[pairs:, :rows]], axis=1)
        adj[1, where, :] = jnp.concatenate([back[:pairs, rows:], back[pairs:, rows:]], axis=1)

    def eight(step, carry):
        for k in range(8):
            one(8 * step + k)
        return carry

    lax.fori_loop(0, per // 8, eight, 0)
    pltpu.make_async_copy(res_ref, res_out, store.at[0]).start()

    def own_block(unit):
        return every.at[unit, core, chip]

    def give(m):
        ref = own_block(CHUNKS + m)
        return remote(ref, ref, ys.at[0], yr.at[m], "layer", jnp.where(middle_layer, outer, inner))

    def gather(unit, k):
        ref = own_block(unit)
        return remote(ref, ref, sa.at[k - 1], da.at[unit, k - 1], "facet", peer_of(k))

    def gather_core(unit):
        ref = every.at[unit, core]
        return remote(ref, ref, sc.at[0], dc.at[unit], "facet", other)

    def spread_out(unit):
        for k in (3, 1, 2):
            gather(unit, k).start()

    def fill(unit, q):
        for p in range(2):
            for t in range(pq):
                piece = adj[p, pl.ds(q * pq + t, per, stride=pairs), :].astype(jnp.bfloat16)
                every[unit, core, chip, p, t * per : (t + 1) * per] = piece

    def fill_step(q, carry):
        @pl.when(has_own(q))
        def _():
            fill(q, q)
            spread_out(q)

        if moved:
            @pl.when(jnp.logical_not(has_own(q)))
            def _():
                m = moved_index(q)
                fill(CHUNKS + m, q)
                give(m).start()

        return carry

    lax.fori_loop(0, CHUNKS, fill_step, 0)

    def back_copy(direction, j, q):
        step = 1 if direction == 0 else -1
        return remote(
            sbuf.at[direction, j, chunk(q)], rbuf.at[direction, j, chunk(q)],
            bs.at[direction, j], br.at[direction, j - 1 + direction, q], "layer", near(step),
        )

    def behind(direction, q):
        return i > bottom(q) if direction == 0 else i < top(q)

    def compute_backward(q, unit, m):
        twr, twi = tw2_ref[0], tw2_ref[1]
        facr, faci = fac[0], fac[1]
        base = chunk(unit).start
        for pair in range(pq):
            where = slice(pair * per, (pair + 1) * per)
            grids = [
                jnp.concatenate(
                    [every[unit, device % 2, device // 2, p, where] for device in range(8)], axis=0
                ).astype(jnp.float32)
                for p in range(2)
            ]
            ar, ai = grids
            b = jnp.concatenate([ar * facr + ai * faci, ai * facr - ar * faci], axis=0).astype(jnp.bfloat16)
            h = jnp.dot(g2_ref[...], b, preferred_element_type=jnp.float32)
            hr, hi = h[:subgrids], h[subgrids:]
            mixed = jnp.concatenate([hr * twr + hi * twi, hi * twr - hr * twi], axis=1).astype(jnp.bfloat16)
            image = lax.dot_general(
                f2_ref[...], mixed, (((1,), (1,)), ((), ())), preferred_element_type=jnp.float32
            )
            for c in range(2):
                col = q * cq + 2 * pair + c
                ir = image[2 * c * rows : (2 * c + 1) * rows]
                ii = image[(2 * c + 1) * rows : (2 * c + 2) * rows]
                cosine, sine = cs[base + 2 * pair + c, 0], cs[base + 2 * pair + c, 1]
                tr = (BACK_GAIN * (ir * cosine + ii * sine)).astype(jnp.bfloat16)
                ti = (BACK_GAIN * (ii * cosine - ir * sine)).astype(jnp.bfloat16)
                for l in range(n):
                    for part, value in ((0, tr), (1, ti)):
                        piece = value[l * block : (l + 1) * block]
                        if m is not None:
                            total = term[l, col, part].astype(jnp.float32) + piece.astype(jnp.float32)
                            piece = total.astype(jnp.bfloat16)
                        term[l, col, part] = piece

    def run_backward(q, unit, m):
        gather_core(unit).wait_recv()
        compute_backward(q, unit, m)

    def relay(direction, j, q):
        where = chunk(q)

        @pl.when(behind(direction, q))
        def _():
            back_copy(direction, j, q).wait_recv()
            total = term[j, where].astype(jnp.float32) + rbuf[direction, j, where].astype(jnp.float32)
            sbuf[direction, j, where] = total.astype(jnp.bfloat16)

        @pl.when(jnp.logical_not(behind(direction, q)))
        def _():
            sbuf[direction, j, where] = term[j, where]

        back_copy(direction, j, q).start()

    def units_of(q, act):
        live = (q >= 0) & (q < CHUNKS)

        @pl.when(live & has_own(q))
        def _():
            act(q, q, None)

        if moved:
            @pl.when(live & has_extra(q))
            def _():
                m = moved_index(q)
                act(q, CHUNKS + m, m)

    def to_core(q, unit, m):
        for k in (1, 2, 3):
            gather(unit, k).wait_recv()
        gather_core(unit).start()

    def pass_on(direction, q, inside):
        kind = is_moved(q) if inside else jnp.logical_not(is_moved(q))

        @pl.when((q >= 0) & (q < CHUNKS) & kind & has_own(q))
        def _():
            for d in range(n - 1, 0, -1):
                j = i + d if direction == 0 else i - d

                @pl.when((j < n) & (j >= 0))
                def _():
                    relay(direction, j, q)

    def backward_step(t, carry):
        if moved:
            early = t + EARLY

            @pl.when((early < CHUNKS) & has_extra(early))
            def _():
                m = moved_index(early)
                give(m).wait_recv()
                spread_out(CHUNKS + m)

        units_of(t, to_core)
        units_of(t - SPREAD, run_backward)
        now = t - SPREAD
        for direction in range(2):
            hops = i if direction == 0 else n - 1 - i
            pass_on(direction, now - LAG * hops, False)
            if moved:
                pass_on(direction, now - LAG * (hops - 1), True)

        last = now - LAG * (n - 1)

        @pl.when(last >= 0)
        def _():
            where = chunk(last)

            @pl.when(has_own(last))
            def _():
                for p in range(2):
                    otmp[p] = term[i, where, p].astype(jnp.float32).reshape(cq * block, subgrids)

            @pl.when(jnp.logical_not(has_own(last)))
            def _():
                otmp[...] = jnp.zeros(otmp.shape, jnp.float32)

            for direction in range(2):
                @pl.when(behind(direction, last))
                def _():
                    back_copy(direction, i, last).wait_recv()
                    for p in range(2):
                        got = rbuf[direction, i, where, p].astype(jnp.float32)
                        otmp[p] += got.reshape(cq * block, subgrids)

            for p in range(2):
                for m in range(block):
                    out_ref[p, where, m * subgrids : (m + 1) * subgrids] = otmp[p, pl.ds(m, cq, stride=block), :]

            pltpu.make_async_copy(out_ref.at[:, where], grad_out.at[:, where], store.at[1]).start()

        return carry

    lax.fori_loop(0, CHUNKS + LAG * (n - 1) + SPREAD, backward_step, 0)

    pltpu.make_async_copy(res_ref, res_out, store.at[0]).wait()
    pltpu.make_async_copy(out_ref, grad_out, store.at[1]).wait()

    def sent(ref, sem):
        remote(ref, ref, sem, angr.at[0], "facet", other).wait_send()

    def drain(count):
        some = pl.ds(0, count)
        sent(contrib.at[some, 0], s0.at[0])
        sent(every.at[some, 0], sc.at[0])
        for k in range(3):
            sent(r1.at[some, 0], s1.at[k])
            sent(every.at[some, 0, 0], sa.at[k])
        chunks = min(count, CHUNKS)
        for direction in range(2):
            for d in range(1, n):
                j = i + d if direction == 0 else i - d

                @pl.when((j < n) & (j >= 0))
                def _():
                    sent(sbuf.at[direction, 0, pl.ds(0, chunks * cq)], bs.at[direction, j])

    for d in range(2):
        target = i + 1 - 2 * d
        inside = (target >= 1) & (target <= n - 2)
        for s in range(n - 1):
            origin = i - s if d == 0 else i + s
            live = (origin >= 0) & (origin <= n - 1) & (target >= 0) & (target <= n - 1)

            @pl.when(live & inside)
            def _():
                sent(buf.at[0], fs.at[d, s])

            @pl.when(live & jnp.logical_not(inside))
            def _():
                sent(buf.at[0, pl.ds(0, (CHUNKS - moved) * cq)], fs.at[d, s])

    @pl.when(middle_layer)
    def _():
        drain(CHUNKS + moved)
        if moved:
            sent(outbox, xs.at[0])

    @pl.when(jnp.logical_not(middle_layer))
    def _():
        drain(CHUNKS - moved)
        if moved:
            sent(angb.at[pl.ds(0, moved * cq)], angs.at[0])
            sent(every.at[pl.ds(0, moved), 0, 0], ys.at[0])


def cs_extra(moved, total):
    return total * moved // (CHUNKS + moved)


def fused(n, moved, x, angle, window, u, v, plane, observed, tables, taps, plane_angle, shift):
    _, cols, _ = x.shape
    per, vis = u.shape
    subgrids = tables[1].shape[0] // 2
    rows = tables[0].shape[0] // 2
    block = rows // n
    pairs = cols // 2
    cq = cols // CHUNKS
    units = CHUNKS + moved
    slab = (cq // 2) * per
    lanes = 2 * rows
    vmem = pl.BlockSpec(memory_space=pltpu.VMEM)
    smem = pl.BlockSpec(memory_space=pltpu.SMEM)
    bf = lambda *shape: pltpu.VMEM(shape, jnp.bfloat16)
    f32 = lambda *shape: pltpu.VMEM(shape, jnp.float32)
    dma = lambda *shape: pltpu.SemaphoreType.DMA(shape)
    box = max(moved, 1)
    arrays = (x, angle, window, u, v, plane, observed, *tables)
    return pl.pallas_call(
        functools.partial(fused_kernel, n, moved),
        out_shape=(
            jax.ShapeDtypeStruct((per, 2, vis), jnp.float32),
            jax.ShapeDtypeStruct(x.shape, jnp.float32),
        ),
        in_specs=[pl.BlockSpec(memory_space=pltpu.HBM)] * 13 + [smem] * 3,
        out_specs=(pl.BlockSpec(memory_space=pltpu.HBM),) * 2,
        scratch_shapes=[
            *[pltpu.VMEM(a.shape, a.dtype) for a in arrays],
            bf(n, cols, 2, block, subgrids), bf(cq * units, rows, subgrids), f32(cq * units, 2, rows, subgrids),
            f32(2, subgrids, lanes), f32(2, 2 * cq * block, subgrids), f32(2 * cq * rows, subgrids),
            bf(units, 2, 4, 2, slab, lanes), bf(units, 4, 2, slab, lanes), bf(units, 4, 2, slab, lanes),
            bf(units, 3, 2, slab, lanes),
            bf(box, 2, slab, lanes), bf(box, 2, slab, lanes),
            f32(2, per * pairs, lanes), f32(2, per * pairs, lanes), f32(2, per, vis),
            f32(per, rows, vis), bf(per, cols, vis),
            bf(units, 2, 4, 2, slab, lanes), bf(n, cols, 2, block, subgrids),
            bf(2, n, cols, 2, block, subgrids), bf(2, n, cols, 2, block, subgrids), f32(2, cq * block, subgrids),
            dma(2, n - 1), dma(2, n - 1, CHUNKS), dma(1), dma(box),
            dma(1), dma(units), dma(3), dma(units, 3), dma(1), dma(box),
            dma(1), dma(box), dma(3), dma(units, 3), dma(1), dma(units),
            dma(2, n), dma(2, n - 1, CHUNKS), dma(13), dma(2),
            f32(per, 2, vis), f32(*x.shape),
        ],
        compiler_params=pltpu.CompilerParams(
            collective_id=2, has_side_effects=True, vmem_limit_bytes=60 * 1024 * 1024
        ),
        name="fused_column",
    )(*arrays, taps, plane_angle, shift)


def local(n, nf, model_strip, screen_angle, facet_window, facet_shift, kernel_taps, plane_angle, u_cell, v_cell, w_plane, observed):
    _, _, cols, length = screen_angle.shape
    per = u_cell.shape[1]
    subgrids = per * nf
    rows = length // subgrids
    block = rows // n
    vmem = pl.BlockSpec(memory_space=pltpu.VMEM)
    fr, fi = dft(rows)
    gr, gi = dft(subgrids)
    turn = 2.0 * np.pi * (np.arange(rows)[:, None] * np.arange(subgrids)[None, :] % length) / length
    twist = np.stack([np.cos(turn), -np.sin(turn)]).astype(np.float32)
    bf = lambda a: jnp.asarray(a.astype(np.float32)).astype(jnp.bfloat16)
    f1 = bf(np.block([[fr, -fi], [fi, fr]]))
    g1 = bf(np.block([[gr, -gi], [gi, gr]]))
    g2 = bf(np.block([[gr.T, gi.T], [-gi.T, gr.T]]))
    zero = np.zeros_like(fr)
    f2 = bf(
        np.block(
            [
                [fr.T, zero, fi.T, zero],
                [-fi.T, zero, fr.T, zero],
                [zero, fr.T, zero, fi.T],
                [zero, -fi.T, zero, fr.T],
            ]
        )
    )
    tw2 = np.ascontiguousarray(np.tile(np.swapaxes(twist, 1, 2), (1, 1, 2)))
    if nf == 8 and n == 4 and per % 16 == 0 and 2 * rows == subgrids == 128 and cols % (2 * CHUNKS) == 0:
        tables = (f1, g1, jnp.asarray(twist), g2, f2, jnp.asarray(tw2))
        residual, gradient = fused(
            n, MOVED, model_strip[0], screen_angle[0, 0], facet_window.reshape(length // subgrids, subgrids),
            u_cell[0], v_cell[0], w_plane[0], observed[0], tables, kernel_taps, plane_angle, facet_shift,
        )
        return (residual[None], gradient[None])
    factor = facet_factor(facet_window[0], facet_shift[0], subgrids)
    x = model_strip[0].reshape(2, cols, block, subgrids).transpose(1, 0, 2, 3)
    angle = screen_angle[0, 0].reshape(cols, rows, subgrids)
    contrib = pl.pallas_call(
        functools.partial(forward_kernel, n),
        out_shape=jax.ShapeDtypeStruct((2, cols // 2, subgrids, 2 * rows), jnp.bfloat16),
        in_specs=[vmem] * 6,
        out_specs=vmem,
        scratch_shapes=[
            pltpu.VMEM((n, cols, 2, block, subgrids), jnp.bfloat16),
            pltpu.SemaphoreType.DMA((2, n - 1, CHUNKS)),
            pltpu.SemaphoreType.DMA((2, n - 1, CHUNKS)),
            pltpu.SemaphoreType.DMA,
        ],
        compiler_params=pltpu.CompilerParams(collective_id=0, has_side_effects=True),
        name="gather_forward",
    )(x, angle, f1, g1, jnp.asarray(twist), factor)
    parts = contrib.reshape(2, cols // 2, nf, per, 2 * rows)
    received = lax.all_to_all(parts, "facet", split_axis=2, concat_axis=2, tiled=True)
    grids = jnp.sum(received.astype(jnp.float32), axis=2)
    grids = grids.reshape(2, cols // 2, per, 2, rows).transpose(2, 1, 3, 0, 4).reshape(per, cols, 2 * rows)
    residual, adjoint = middle(
        grids, u_cell[0], v_cell[0], w_plane[0], observed[0], plane_angle[0], kernel_taps, rows, cols
    )
    adjoint = adjoint.reshape(per, cols // 2, 2, 2, rows).transpose(3, 1, 0, 2, 4).reshape(2, cols // 2, per, 2 * rows)
    every = lax.all_gather(adjoint, "facet", axis=2, tiled=True)
    gradient = pl.pallas_call(
        functools.partial(backward_kernel, n),
        out_shape=jax.ShapeDtypeStruct((cols, 2, block, subgrids), jnp.float32),
        in_specs=[vmem] * 6,
        out_specs=vmem,
        scratch_shapes=[
            pltpu.VMEM((n, cols, 2, block, subgrids), jnp.bfloat16),
            pltpu.VMEM((2, n, cols, 2, block, subgrids), jnp.bfloat16),
            pltpu.VMEM((2, n, cols, 2, block, subgrids), jnp.bfloat16),
            pltpu.SemaphoreType.DMA((2, n, CHUNKS)),
            pltpu.SemaphoreType.DMA((2, n, CHUNKS)),
        ],
        compiler_params=pltpu.CompilerParams(collective_id=1, has_side_effects=True),
        name="backward_scatter",
    )(every, angle, g2, f2, jnp.asarray(tw2), factor)
    gradient = gradient.transpose(1, 0, 2, 3).reshape(1, 2, cols, block * subgrids)
    return (residual[None], gradient)


def solution(mesh):
    return jax.shard_map(
        functools.partial(local, mesh.shape["layer"], mesh.shape["facet"]),
        mesh=mesh,
        in_specs=(
            P("facet", None, None, "layer"),
            P("layer", "facet", None, None),
            P("facet", None),
            P("facet"),
            P(),
            P("layer", None),
            P("layer", "facet", None),
            P("layer", "facet", None),
            P("layer", "facet", None),
            P("layer", "facet", None, None),
        ),
        out_specs=(P("layer", "facet", None, None), P("facet", None, None, "layer")),
        check_vma=False,
    )
```

```python
import functools
import math

import jax
import jax.numpy as jnp
import numpy as np
from jax import lax
from jax.experimental import pallas as pl
from jax.experimental.pallas import tpu as pltpu
from jax.sharding import PartitionSpec as P

MESH = pl.DeviceIdType.MESH
BACK_GAIN = 8.0
CHUNKS = 8
MOVED = 3
FIRST = 3
EARLY = 2
LEAD = 1
HOP = 2
AGES = (1, 3)
SPREAD = 1
LAG = 2


def _fit(values, degree):
    nodes = np.cos(np.pi * (np.arange(64) + 0.5) / 64)
    y = (nodes + 1.0) * 0.5 * np.pi**2
    cheb = np.polynomial.chebyshev.Chebyshev.fit(y, values(np.sqrt(y)), degree, domain=[0, np.pi**2])
    return [float(v) for v in cheb.convert(kind=np.polynomial.Polynomial).coef]


COS = _fit(np.cos, 8)
SIN = _fit(lambda x: np.sinc(x / np.pi), 7)


def cos_sin(x):
    y = x * x
    c = jnp.full_like(y, COS[-1])
    for v in COS[-2::-1]:
        c = c * y + v
    s = jnp.full_like(y, SIN[-1])
    for v in SIN[-2::-1]:
        s = s * y + v
    return c, s * x


def dft(length):
    k = np.arange(length)
    angles = 2.0 * np.pi * ((k[:, None] * k[None, :]) % length) / length
    scale = 1.0 / math.sqrt(length)
    return np.cos(angles) * scale, -np.sin(angles) * scale


def barrier_line(i, n):
    sem = pltpu.get_barrier_semaphore()

    @pl.when(i > 0)
    def _():
        pl.semaphore_signal(sem, inc=1, device_id={"layer": i - 1}, device_id_type=MESH)

    @pl.when(i < n - 1)
    def _():
        pl.semaphore_signal(sem, inc=1, device_id={"layer": i + 1}, device_id_type=MESH)

    peers = jnp.where(i > 0, 1, 0) + jnp.where(i < n - 1, 1, 0)
    pl.semaphore_wait(sem, peers)


def forward_kernel(n, x_ref, ang_ref, f1_ref, g_ref, tw_ref, fac_ref, out_ref, buf, send_sem, recv_sem, own_sem):
    i = lax.axis_index("layer")
    cq = x_ref.shape[0] // CHUNKS
    subgrids = g_ref.shape[0] // 2
    rows = f1_ref.shape[0] // 2
    barrier_line(i, n)
    own = pltpu.make_async_copy(x_ref, buf.at[i], own_sem)
    own.start()

    def copy(direction, s, q):
        step = 1 if direction == 0 else -1
        origin = jnp.clip(i - step * s, 0, n - 1)
        cols = pl.ds(q * cq, cq)
        src = x_ref.at[cols] if s == 0 else buf.at[origin, cols]
        return pltpu.make_async_remote_copy(
            src_ref=src,
            dst_ref=buf.at[origin, cols],
            send_sem=send_sem.at[direction, s, q],
            recv_sem=recv_sem.at[direction, s, q],
            device_id={"layer": jnp.clip(i + step, 0, n - 1)},
            device_id_type=MESH,
        )

    def sends(direction, s):
        if direction == 0:
            return (i - s >= 0) & (i < n - 1)
        return (i + s <= n - 1) & (i > 0)

    def gets(direction, s):
        return i - 1 - s >= 0 if direction == 0 else i + 1 + s <= n - 1

    def compute(q):
        twr, twi = tw_ref[0], tw_ref[1]
        facr, faci = fac_ref[0], fac_ref[1]
        for pair in range(cq // 2):
            halves = []
            for c in (2 * pair, 2 * pair + 1):
                col = q * cq + c
                xr = jnp.concatenate([buf[l, col, 0] for l in range(n)], axis=0).astype(jnp.float32)
                xi = jnp.concatenate([buf[l, col, 1] for l in range(n)], axis=0).astype(jnp.float32)
                cosine, sine = cos_sin(ang_ref[col].astype(jnp.float32))
                x = jnp.concatenate([xr * cosine - xi * sine, xr * sine + xi * cosine], axis=0)
                h = jnp.dot(f1_ref[...], x.astype(jnp.bfloat16), preferred_element_type=jnp.float32)
                hr, hi = h[:rows], h[rows:]
                halves.append(
                    jnp.concatenate([hr * twr - hi * twi, hr * twi + hi * twr], axis=1).astype(jnp.bfloat16)
                )
            both = jnp.concatenate(halves, axis=0)
            spec = lax.dot_general(
                g_ref[...], both, (((1,), (1,)), ((), ())), preferred_element_type=jnp.float32
            )
            sr, si = spec[:subgrids], spec[subgrids:]
            at = q * (cq // 2) + pair
            out_ref[0, at] = (sr * facr - si * faci).astype(jnp.bfloat16)
            out_ref[1, at] = (sr * faci + si * facr).astype(jnp.bfloat16)

    def body(t, carry):
        @pl.when(t < CHUNKS)
        def _():
            for d in range(2):
                @pl.when(sends(d, 0))
                def _():
                    copy(d, 0, t).start()

        for s in range(n - 1):
            q = t - 1 - s
            @pl.when((q >= 0) & (q < CHUNKS))
            def _():
                for d in range(2):
                    @pl.when(gets(d, s))
                    def _():
                        copy(d, s, q).wait_recv()
                        if s + 1 < n - 1:
                            @pl.when(sends(d, s + 1))
                            def _():
                                copy(d, s + 1, q).start()

        @pl.when(t >= n - 1)
        def _():
            compute(t - (n - 1))

        return carry

    own.wait()
    lax.fori_loop(0, CHUNKS + n - 1, body, 0)

    def drain(q, carry):
        for d in range(2):
            for s in range(n - 1):
                @pl.when(sends(d, s))
                def _():
                    copy(d, s, q).wait_send()
        return carry

    lax.fori_loop(0, CHUNKS, drain, 0)


def backward_kernel(n, a_ref, ang_ref, g_ref, f2_ref, tw_ref, fac_ref, out_ref, term, sbuf, rbuf, send_sem, recv_sem):
    i = lax.axis_index("layer")
    cols = ang_ref.shape[0]
    cq = cols // CHUNKS
    fine = g_ref.shape[0] // 2
    rows = ang_ref.shape[1]
    part = rows // n
    barrier_line(i, n)

    def copy(direction, j, q):
        where = pl.ds(q * cq, cq)
        step = 1 if direction == 0 else -1
        return pltpu.make_async_remote_copy(
            src_ref=sbuf.at[direction, j, where],
            dst_ref=rbuf.at[direction, j, where],
            send_sem=send_sem.at[direction, j, q],
            recv_sem=recv_sem.at[direction, j, q],
            device_id={"layer": jnp.clip(i + step, 0, n - 1)},
            device_id_type=MESH,
        )

    def behind(direction):
        return i > 0 if direction == 0 else i < n - 1

    def compute(q):
        twr, twi = tw_ref[0], tw_ref[1]
        facr, faci = fac_ref[0], fac_ref[1]
        for pair in range(cq // 2):
            at = q * (cq // 2) + pair
            ar = a_ref[0, at].astype(jnp.float32)
            ai = a_ref[1, at].astype(jnp.float32)
            b = jnp.concatenate([ar * facr + ai * faci, ai * facr - ar * faci], axis=0).astype(jnp.bfloat16)
            h = jnp.dot(g_ref[...], b, preferred_element_type=jnp.float32)
            hr, hi = h[:fine], h[fine:]
            mixed = jnp.concatenate([hr * twr + hi * twi, hi * twr - hr * twi], axis=1).astype(jnp.bfloat16)
            image = lax.dot_general(
                f2_ref[...], mixed, (((1,), (1,)), ((), ())), preferred_element_type=jnp.float32
            )
            for c in range(2):
                col = q * cq + 2 * pair + c
                ir = image[2 * c * rows : (2 * c + 1) * rows]
                ii = image[(2 * c + 1) * rows : (2 * c + 2) * rows]
                cosine, sine = cos_sin(ang_ref[col].astype(jnp.float32))
                tr = (BACK_GAIN * (ir * cosine + ii * sine)).astype(jnp.bfloat16)
                ti = (BACK_GAIN * (ii * cosine - ir * sine)).astype(jnp.bfloat16)
                for l in range(n):
                    term[l, col, 0] = tr[l * part : (l + 1) * part]
                    term[l, col, 1] = ti[l * part : (l + 1) * part]

    def relay(direction, j, q):
        where = pl.ds(q * cq, cq)

        @pl.when(behind(direction))
        def _():
            copy(direction, j, q).wait_recv()
            total = term[j, where].astype(jnp.float32) + rbuf[direction, j, where].astype(jnp.float32)
            sbuf[direction, j, where] = total.astype(jnp.bfloat16)

        @pl.when(jnp.logical_not(behind(direction)))
        def _():
            sbuf[direction, j, where] = term[j, where]

        copy(direction, j, q).start()

    def body(t, carry):
        @pl.when(t < CHUNKS)
        def _():
            compute(t)

        for direction in range(2):
            q = t - i if direction == 0 else t - (n - 1 - i)

            @pl.when((q >= 0) & (q < CHUNKS))
            def _():
                for d in range(n - 1, 0, -1):
                    j = i + d if direction == 0 else i - d

                    @pl.when((j < n) & (j >= 0))
                    def _():
                        relay(direction, j, q)

        last = t - (n - 1)

        @pl.when(last >= 0)
        def _():
            where = pl.ds(last * cq, cq)
            out_ref[where] = term[i, where].astype(jnp.float32)
            for direction in range(2):
                @pl.when(behind(direction))
                def _():
                    copy(direction, i, last).wait_recv()
                    out_ref[where] += rbuf[direction, i, where].astype(jnp.float32)

        return carry

    lax.fori_loop(0, CHUNKS + n - 1, body, 0)

    def drain(q, carry):
        for direction in range(2):
            for d in range(1, n):
                j = i + d if direction == 0 else i - d

                @pl.when((j < n) & (j >= 0))
                def _():
                    copy(direction, j, q).wait_send()
        return carry

    lax.fori_loop(0, CHUNKS, drain, 0)


def facet_factor(window, shift_cells, subgrids):
    length = window.shape[0]
    rows = length // subgrids
    grid = window.reshape(subgrids, rows)
    grid = jnp.concatenate([grid, grid], axis=1)
    high = lax.broadcasted_iota(jnp.int32, grid.shape, 0)
    low = lax.broadcasted_iota(jnp.int32, grid.shape, 1) % rows
    turn_count = (high * rows + low) * shift_cells % length
    angles = 2.0 * math.pi / length * turn_count.astype(jnp.float32)
    return jnp.stack([grid * jnp.cos(angles), -grid * jnp.sin(angles)])


def spread(cells, length, taps):
    count = taps.shape[0]
    lanes = jnp.arange(length, dtype=jnp.int32)
    offset = (lanes - cells[..., None] + (count // 2 + length)) % length
    out = jnp.zeros(offset.shape, jnp.float32)
    for t in range(count):
        out = out + jnp.where(offset == t, taps[t], 0.0)
    return out


def middle(grids, u, v, plane, observed, angle, taps, rows, cols):
    row_weights = spread(u, rows, taps)
    column_weights = spread(v, cols, taps).astype(jnp.bfloat16)
    picked = jnp.einsum("sjc,sck->sjk", column_weights, grids.astype(jnp.bfloat16), preferred_element_type=jnp.float32)
    model_real = jnp.sum(picked[..., :rows] * row_weights, axis=2)
    model_imag = jnp.sum(picked[..., rows:] * row_weights, axis=2)
    pick = plane[..., None] == jnp.arange(angle.shape[0], dtype=jnp.int32)
    cosine = jnp.sum(jnp.where(pick, jnp.cos(angle), 0.0), axis=2)
    sine = jnp.sum(jnp.where(pick, jnp.sin(angle), 0.0), axis=2)
    res_real = observed[:, 0] - (model_real * cosine - model_imag * sine)
    res_imag = observed[:, 1] - (model_real * sine + model_imag * cosine)
    w_real = res_real * cosine + res_imag * sine
    w_imag = res_imag * cosine - res_real * sine
    spread_rows = jnp.concatenate(
        [w_real[..., None] * row_weights, w_imag[..., None] * row_weights], axis=2
    ).astype(jnp.bfloat16)
    adjoint = jnp.einsum("sjc,sjk->sck", column_weights, spread_rows, preferred_element_type=jnp.float32)
    return jnp.stack([res_real, res_imag], axis=1), adjoint.astype(jnp.bfloat16)


def fused_kernel(
    n, moved, *refs,
):
    sources, (taps_ref, pang_ref, shift_ref, res_out, grad_out), held = refs[:13], refs[13:18], refs[18:31]
    (x_ref, ang_ref, win_ref, u_ref, v_ref, plane_ref, obs_ref, f1_ref, g1_ref, tw_ref, g2_ref, f2_ref, tw2_ref) = held
    (
    buf, angb, cs, fac, tmpx, tmpa, contrib, r0, acc0, r1, outbox, inbox, fin, adj, phase, row_table, column_table,
    every, term, sbuf, rbuf, otmp,
    fs, fr, angs, angr, s0, d0, s1, d1, xs, xr, ys, yr, sa, da, sc, dc, bs, br, load, store, res_ref, out_ref,
    ) = refs[31:]
    loads = [pltpu.make_async_copy(a, b, load.at[k]) for k, (a, b) in enumerate(zip(sources, held))]
    for one_load in loads:
        one_load.start()
    cols, rows = angb.shape[0] - cs_extra(moved, angb.shape[0]), angb.shape[1]
    lanes = 2 * rows
    subgrids = g1_ref.shape[0] // 2
    block = rows // n
    per, vis = u_ref.shape
    pairs = cols // 2
    cq = cols // CHUNKS
    pq = cq // 2
    i = lax.axis_index("layer")
    f = lax.axis_index("facet")
    core = lax.rem(f, 2)
    chip = lax.div(f, 2)
    bits = (lax.rem(chip, 2), lax.div(chip, 2))
    other = f + 1 - 2 * core
    middle_layer = (i >= 1) & (i <= n - 2)

    def chip_of(k):
        b0 = 1 - bits[0] if k & 1 else bits[0]
        b1 = 1 - bits[1] if k & 2 else bits[1]
        return b0 + 2 * b1

    def peer_of(k):
        return 2 * chip_of(k) + core

    def near(step):
        return jnp.clip(i + step, 0, n - 1)

    inner = jnp.where(i == 0, 1, n - 2)
    outer = jnp.where(i == 1, 0, n - 1)

    barrier = pltpu.get_barrier_semaphore()
    for peer in (other, peer_of(1), peer_of(2), peer_of(3)):
        pl.semaphore_signal(barrier, inc=1, device_id={"facet": peer}, device_id_type=MESH)

    @pl.when(i > 0)
    def _():
        pl.semaphore_signal(barrier, inc=1, device_id={"layer": i - 1}, device_id_type=MESH)

    @pl.when(i < n - 1)
    def _():
        pl.semaphore_signal(barrier, inc=1, device_id={"layer": i + 1}, device_id_type=MESH)

    pl.semaphore_wait(barrier, 4 + jnp.where(i > 0, 1, 0) + jnp.where(i < n - 1, 1, 0))

    def is_moved(q):
        return (lax.rem(q, 2) == 1) & (q >= FIRST) & (q < FIRST + 2 * moved)

    def moved_index(q):
        return lax.div(q - FIRST, 2)

    def bottom(q):
        return jnp.where(is_moved(q), 1, 0)

    def top(q):
        return jnp.where(is_moved(q), n - 2, n - 1)

    def has_own(q):
        return (i >= bottom(q)) & (i <= top(q))

    def has_extra(q):
        return middle_layer & is_moved(q)

    def remote(src, dst, send, recv, axis, device):
        return pltpu.make_async_remote_copy(
            src_ref=src, dst_ref=dst, send_sem=send, recv_sem=recv, device_id={axis: device}, device_id_type=MESH
        )

    def chunk(q):
        return pl.ds(pl.multiple_of(q * cq, cq), cq)

    def copy(direction, s, q):
        step = 1 if direction == 0 else -1
        origin = jnp.clip(i - step * s, 0, n - 1)
        ref = buf.at[origin, chunk(q)]
        return remote(ref, ref, fs.at[direction, s], fr.at[direction, s, q], "layer", near(step))

    def sends(direction, s, q):
        if direction == 0:
            return (i - s >= 0) & (i + 1 <= top(q))
        return (i + s <= n - 1) & (i - 1 >= bottom(q))

    def gets(direction, s, q):
        if direction == 0:
            return (i - 1 - s >= 0) & (i <= top(q))
        return (i + 1 + s <= n - 1) & (i >= bottom(q))

    def send_own(q):
        for d in range(2):
            @pl.when(sends(d, 0, q))
            def _():
                copy(d, 0, q).start()

    def angle_copy(m):
        src = angb.at[chunk(2 * m + FIRST)]
        dst = angb.at[chunk(CHUNKS + m)]
        return remote(src, dst, angs.at[0], angr.at[m], "layer", inner)

    def relayout(g, carry):
        at = pl.ds(pl.multiple_of(g * 2 * cq, 2 * cq), 2 * cq)
        for p in range(2):
            v = x_ref[p, at, :].astype(jnp.float32)
            for m in range(block):
                tmpx[p, pl.ds(m, 2 * cq, stride=block), :] = v[:, m * subgrids : (m + 1) * subgrids]
            buf[i, at, p] = tmpx[p].reshape(2 * cq, block, subgrids).astype(jnp.bfloat16)

        for k in range(2):
            @pl.when(jnp.logical_not(middle_layer) | (2 * g + k < LEAD))
            def _():
                send_own(2 * g + k)

        @pl.when(jnp.logical_not(middle_layer))
        def _():
            angle_relayout(g)

        return carry

    def angle_relayout(g):
        at = pl.ds(pl.multiple_of(g * 2 * cq, 2 * cq), 2 * cq)
        for m in range(rows):
            piece = ang_ref[at, m * subgrids : (m + 1) * subgrids].astype(jnp.float32)
            tmpa[pl.ds(m, 2 * cq, stride=rows), :] = piece
        angb[at] = tmpa[...].reshape(2 * cq, rows, subgrids).astype(jnp.bfloat16)

        if moved:
            m = g - FIRST // 2

            @pl.when(jnp.logical_not(middle_layer) & (m >= 0) & (m < moved))
            def _():
                angle_copy(m).start()

    loads[0].wait()
    loads[1].wait()
    lax.fori_loop(0, CHUNKS // 2, relayout, 0)
    for one_load in loads[2:]:
        one_load.wait()

    window = win_ref[...]
    rolled = pltpu.roll(window, rows, axis=1)
    left = lax.broadcasted_iota(jnp.int32, window.shape, 1) < rows
    fac[0, pl.ds(0, subgrids // 2, stride=2), :] = jnp.where(left, window, rolled)
    fac[0, pl.ds(1, subgrids // 2, stride=2), :] = jnp.where(left, rolled, window)
    grid = fac[0]
    length = subgrids * rows
    high = lax.broadcasted_iota(jnp.int32, grid.shape, 0)
    low = lax.broadcasted_iota(jnp.int32, grid.shape, 1)
    low = jnp.where(low < rows, low, low - rows)
    turns = lax.rem((high * rows + low) * shift_ref[0], length)
    turns = jnp.where(turns * 2 >= length, turns - length, turns)
    cosine, sine = cos_sin(turns.astype(jnp.float32) * (2.0 * math.pi / length))
    fac[0] = grid * cosine
    fac[1] = -grid * sine

    plane = plane_ref[...]
    angle = jnp.zeros(plane.shape, jnp.float32)
    for k in range(pang_ref.shape[1]):
        angle = jnp.where(plane == k, pang_ref[0, k], angle)
    cosine, sine = cos_sin(angle)
    phase[0] = cosine
    phase[1] = sine

    def weights(cells, position, size):
        count = taps_ref.shape[0]
        offset = position - cells + count // 2
        offset = jnp.where(offset < 0, offset + size, jnp.where(offset >= size, offset - size, offset))
        out = jnp.zeros(offset.shape, jnp.float32)
        for t in range(count):
            out = jnp.where(offset == t, taps_ref[t], out)
        return out

    def prepare(s):
        at = pl.ds(s, 1)
        row = lax.broadcasted_iota(jnp.int32, (rows, vis), 0)
        half = lax.broadcasted_iota(jnp.int32, (pairs, vis), 0)
        col = jnp.concatenate([2 * half, 2 * half + 1], axis=0)
        row_table[s] = weights(u_ref[at, :], row, rows)
        column_table[s] = weights(v_ref[at, :], col, cols).astype(jnp.bfloat16)

    def compute_forward(q, unit):
        twr, twi = tw_ref[0], tw_ref[1]
        facr, faci = fac[0], fac[1]
        base = chunk(unit).start
        for pair in range(pq):
            halves = []
            for c in (2 * pair, 2 * pair + 1):
                col = q * cq + c
                xr_ = jnp.concatenate([buf[l, col, 0] for l in range(n)], axis=0).astype(jnp.float32)
                xi_ = jnp.concatenate([buf[l, col, 1] for l in range(n)], axis=0).astype(jnp.float32)
                cosine, sine = cos_sin(angb[base + c].astype(jnp.float32))
                cs[base + c, 0] = cosine
                cs[base + c, 1] = sine
                x = jnp.concatenate([xr_ * cosine - xi_ * sine, xr_ * sine + xi_ * cosine], axis=0)
                h = jnp.dot(f1_ref[...], x.astype(jnp.bfloat16), preferred_element_type=jnp.float32)
                hr, hi = h[:rows], h[rows:]
                halves.append(
                    jnp.concatenate([hr * twr - hi * twi, hr * twi + hi * twr], axis=1).astype(jnp.bfloat16)
                )
            both = jnp.concatenate(halves, axis=0)
            spec = lax.dot_general(
                g1_ref[...], both, (((1,), (1,)), ((), ())), preferred_element_type=jnp.float32
            )
            sr, si = spec[:subgrids], spec[subgrids:]
            parts = ((sr * facr - si * faci).astype(jnp.bfloat16), (sr * faci + si * facr).astype(jnp.bfloat16))
            for p in range(2):
                for device in range(8):
                    contrib[unit, device % 2, device // 2, p, pair * per : (pair + 1) * per] = parts[p][
                        device * per : (device + 1) * per
                    ]

    def stage0(unit):
        return remote(contrib.at[unit, 1 - core], r0.at[unit], s0.at[0], d0.at[unit], "facet", other)

    def stage1(unit, k):
        src = acc0.at[unit, chip_of(k)]
        return remote(src, r1.at[unit, k - 1], s1.at[k - 1], d1.at[unit, k - 1], "facet", peer_of(k))

    def result(m):
        return remote(outbox.at[m], inbox.at[m], xs.at[0], xr.at[m], "layer", jnp.where(middle_layer, outer, inner))

    def add0(unit):
        stage0(unit).wait_recv()
        total = contrib[unit, core].astype(jnp.float32) + r0[unit].astype(jnp.float32)
        acc0[unit] = total.astype(jnp.bfloat16)
        for k in (3, 1, 2):
            stage1(unit, k).start()

    def store_fin(p, q, total):
        for t in range(pq):
            fin[p, pl.ds(q * pq + t, per, stride=pairs), :] = total[t * per : (t + 1) * per]

    def add2(q, unit, m):
        for k in (1, 2, 3):
            stage1(unit, k).wait_recv()
        for p in range(2):
            total = acc0[unit, chip, p].astype(jnp.float32)
            for k in range(3):
                total = total + r1[unit, k, p].astype(jnp.float32)
            if m is None:
                store_fin(p, q, total)
            else:
                outbox[m, p] = total.astype(jnp.bfloat16)
        if m is not None:
            result(m).start()

    def at_age(t, age, act):
        q = t - ready - age
        m = moved_index(q)
        live = (q >= 0) & (q < CHUNKS)

        @pl.when(live & has_own(q))
        def _():
            act(q, q, None)

        if moved:
            @pl.when(live & has_extra(q))
            def _():
                act(q, CHUNKS + m, m)

    def run_forward(q, unit, m):
        if m is not None:
            angle_copy(m).wait_recv()
        compute_forward(q, unit)
        stage0(unit).start()

    ready = 1 + HOP * (n - 2 - jnp.where(middle_layer, 1, 0))

    def forward_step(t, carry):
        @pl.when((t + LEAD < CHUNKS) & middle_layer)
        def _():
            send_own(t + LEAD)

        @pl.when((t < CHUNKS // 2) & middle_layer)
        def _():
            angle_relayout(t)

        for s in range(n - 1):
            q = t - 1 - HOP * s

            @pl.when((q >= 0) & (q < CHUNKS))
            def _():
                for d in range(2):
                    @pl.when(gets(d, s, q))
                    def _():
                        copy(d, s, q).wait_recv()
                        if s + 1 < n - 1:
                            @pl.when(sends(d, s + 1, q))
                            def _():
                                copy(d, s + 1, q).start()

        @pl.when(t < per // 4)
        def _():
            for k in range(4):
                prepare(4 * t + k)

        at_age(t, AGES[1], add2)
        at_age(t, AGES[0], lambda q, unit, m: add0(unit))
        at_age(t, 0, run_forward)
        return carry

    lax.fori_loop(0, CHUNKS + 1 + HOP * (n - 2) + AGES[1], forward_step, 0)

    if moved:
        @pl.when(jnp.logical_not(middle_layer))
        def _():
            for m in range(moved):
                result(m).wait_recv()
                for p in range(2):
                    store_fin(p, 2 * m + FIRST, inbox[m, p].astype(jnp.float32))

    def one(s):
        at = pl.ds(s, 1)
        where = pl.ds(pl.multiple_of(s * pairs, pairs), pairs)
        row_weights = row_table[s]
        column_weights = column_table[s]
        real, imag = fin[0, where, :], fin[1, where, :]
        grid = jnp.concatenate(
            [
                jnp.concatenate([real[:, :rows], imag[:, :rows]], axis=1),
                jnp.concatenate([real[:, rows:], imag[:, rows:]], axis=1),
            ],
            axis=0,
        )
        picked = lax.dot_general(
            grid.astype(jnp.bfloat16), column_weights, (((0,), (0,)), ((), ())),
            preferred_element_type=jnp.float32,
        )
        model_real = jnp.sum(picked[:rows] * row_weights, axis=0, keepdims=True)
        model_imag = jnp.sum(picked[rows:] * row_weights, axis=0, keepdims=True)
        cosine, sine = phase[0, at, :], phase[1, at, :]
        res_real = obs_ref[s, 0:1, :] - (model_real * cosine - model_imag * sine)
        res_imag = obs_ref[s, 1:2, :] - (model_real * sine + model_imag * cosine)
        res_ref[s, 0:1, :] = res_real
        res_ref[s, 1:2, :] = res_imag
        w_real = res_real * cosine + res_imag * sine
        w_imag = res_imag * cosine - res_real * sine
        spread_rows = jnp.concatenate([row_weights * w_real, row_weights * w_imag], axis=0).astype(jnp.bfloat16)
        back = lax.dot_general(
            column_weights, spread_rows, (((1,), (1,)), ((), ())), preferred_element_type=jnp.float32
        )
        adj[0, where, :] = jnp.concatenate([back[:pairs, :rows], back[pairs:, :rows]], axis=1)
        adj[1, where, :] = jnp.concatenate([back[:pairs, rows:], back[pairs:, rows:]], axis=1)

    def block_of(step, carry):
        for k in range(16):
            one(16 * step + k)
        return carry

    lax.fori_loop(0, per // 16, block_of, 0)
    pltpu.make_async_copy(res_ref, res_out, store.at[0]).start()

    def own_block(unit):
        return every.at[unit, core, chip]

    def give(m):
        ref = own_block(CHUNKS + m)
        return remote(ref, ref, ys.at[0], yr.at[m], "layer", jnp.where(middle_layer, outer, inner))

    def gather(unit, k):
        ref = own_block(unit)
        return remote(ref, ref, sa.at[k - 1], da.at[unit, k - 1], "facet", peer_of(k))

    def gather_core(unit):
        ref = every.at[unit, core]
        return remote(ref, ref, sc.at[0], dc.at[unit], "facet", other)

    def spread_out(unit):
        for k in (3, 1, 2):
            gather(unit, k).start()

    def fill(unit, q):
        for p in range(2):
            for t in range(pq):
                piece = adj[p, pl.ds(q * pq + t, per, stride=pairs), :].astype(jnp.bfloat16)
                every[unit, core, chip, p, t * per : (t + 1) * per] = piece

    def fill_step(q, carry):
        @pl.when(has_own(q))
        def _():
            fill(q, q)
            spread_out(q)

        if moved:
            @pl.when(jnp.logical_not(has_own(q)))
            def _():
                m = moved_index(q)
                fill(CHUNKS + m, q)
                give(m).start()

        return carry

    lax.fori_loop(0, CHUNKS, fill_step, 0)

    def back_copy(direction, j, q):
        step = 1 if direction == 0 else -1
        return remote(
            sbuf.at[direction, j, chunk(q)], rbuf.at[direction, j, chunk(q)],
            bs.at[direction, j], br.at[direction, j - 1 + direction, q], "layer", near(step),
        )

    def behind(direction, q):
        return i > bottom(q) if direction == 0 else i < top(q)

    def compute_backward(q, unit, m):
        twr, twi = tw2_ref[0], tw2_ref[1]
        facr, faci = fac[0], fac[1]
        base = chunk(unit).start
        for pair in range(pq):
            where = slice(pair * per, (pair + 1) * per)
            grids = [
                jnp.concatenate(
                    [every[unit, device % 2, device // 2, p, where] for device in range(8)], axis=0
                ).astype(jnp.float32)
                for p in range(2)
            ]
            ar, ai = grids
            b = jnp.concatenate([ar * facr + ai * faci, ai * facr - ar * faci], axis=0).astype(jnp.bfloat16)
            h = jnp.dot(g2_ref[...], b, preferred_element_type=jnp.float32)
            hr, hi = h[:subgrids], h[subgrids:]
            mixed = jnp.concatenate([hr * twr + hi * twi, hi * twr - hr * twi], axis=1).astype(jnp.bfloat16)
            image = lax.dot_general(
                f2_ref[...], mixed, (((1,), (1,)), ((), ())), preferred_element_type=jnp.float32
            )
            for c in range(2):
                col = q * cq + 2 * pair + c
                ir = image[2 * c * rows : (2 * c + 1) * rows]
                ii = image[(2 * c + 1) * rows : (2 * c + 2) * rows]
                cosine, sine = cs[base + 2 * pair + c, 0], cs[base + 2 * pair + c, 1]
                tr = (BACK_GAIN * (ir * cosine + ii * sine)).astype(jnp.bfloat16)
                ti = (BACK_GAIN * (ii * cosine - ir * sine)).astype(jnp.bfloat16)
                for l in range(n):
                    for part, value in ((0, tr), (1, ti)):
                        piece = value[l * block : (l + 1) * block]
                        if m is not None:
                            total = term[l, col, part].astype(jnp.float32) + piece.astype(jnp.float32)
                            piece = total.astype(jnp.bfloat16)
                        term[l, col, part] = piece

    def run_backward(q, unit, m):
        gather_core(unit).wait_recv()
        compute_backward(q, unit, m)

    def relay(direction, j, q):
        where = chunk(q)

        @pl.when(behind(direction, q))
        def _():
            back_copy(direction, j, q).wait_recv()
            total = term[j, where].astype(jnp.float32) + rbuf[direction, j, where].astype(jnp.float32)
            sbuf[direction, j, where] = total.astype(jnp.bfloat16)

        @pl.when(jnp.logical_not(behind(direction, q)))
        def _():
            sbuf[direction, j, where] = term[j, where]

        back_copy(direction, j, q).start()

    def units_of(q, act):
        live = (q >= 0) & (q < CHUNKS)

        @pl.when(live & has_own(q))
        def _():
            act(q, q, None)

        if moved:
            @pl.when(live & has_extra(q))
            def _():
                m = moved_index(q)
                act(q, CHUNKS + m, m)

    def to_core(q, unit, m):
        for k in (1, 2, 3):
            gather(unit, k).wait_recv()
        gather_core(unit).start()

    def pass_on(direction, q, inside):
        kind = is_moved(q) if inside else jnp.logical_not(is_moved(q))

        @pl.when((q >= 0) & (q < CHUNKS) & kind & has_own(q))
        def _():
            for d in range(n - 1, 0, -1):
                j = i + d if direction == 0 else i - d

                @pl.when((j < n) & (j >= 0))
                def _():
                    relay(direction, j, q)

    def backward_step(t, carry):
        if moved:
            early = t + EARLY

            @pl.when((early < CHUNKS) & has_extra(early))
            def _():
                m = moved_index(early)
                give(m).wait_recv()
                spread_out(CHUNKS + m)

        units_of(t, to_core)
        units_of(t - SPREAD, run_backward)
        now = t - SPREAD
        for direction in range(2):
            hops = i if direction == 0 else n - 1 - i
            pass_on(direction, now - LAG * hops, False)
            if moved:
                pass_on(direction, now - LAG * (hops - 1), True)

        last = now - LAG * (n - 1)

        @pl.when(last >= 0)
        def _():
            where = chunk(last)

            @pl.when(has_own(last))
            def _():
                for p in range(2):
                    otmp[p] = term[i, where, p].astype(jnp.float32).reshape(cq * block, subgrids)

            @pl.when(jnp.logical_not(has_own(last)))
            def _():
                otmp[...] = jnp.zeros(otmp.shape, jnp.float32)

            for direction in range(2):
                @pl.when(behind(direction, last))
                def _():
                    back_copy(direction, i, last).wait_recv()
                    for p in range(2):
                        got = rbuf[direction, i, where, p].astype(jnp.float32)
                        otmp[p] += got.reshape(cq * block, subgrids)

            for p in range(2):
                for m in range(block):
                    out_ref[p, where, m * subgrids : (m + 1) * subgrids] = otmp[p, pl.ds(m, cq, stride=block), :]

            pltpu.make_async_copy(out_ref.at[:, where], grad_out.at[:, where], store.at[1]).start()

        return carry

    lax.fori_loop(0, CHUNKS + LAG * (n - 1) + SPREAD, backward_step, 0)

    pltpu.make_async_copy(res_ref, res_out, store.at[0]).wait()
    pltpu.make_async_copy(out_ref, grad_out, store.at[1]).wait()

    def sent(ref, sem):
        remote(ref, ref, sem, angr.at[0], "facet", other).wait_send()

    def drain(count):
        some = pl.ds(0, count)
        sent(contrib.at[some, 0], s0.at[0])
        sent(every.at[some, 0], sc.at[0])
        for k in range(3):
            sent(r1.at[some, 0], s1.at[k])
            sent(every.at[some, 0, 0], sa.at[k])
        chunks = min(count, CHUNKS)
        for direction in range(2):
            for d in range(1, n):
                j = i + d if direction == 0 else i - d

                @pl.when((j < n) & (j >= 0))
                def _():
                    sent(sbuf.at[direction, 0, pl.ds(0, chunks * cq)], bs.at[direction, j])

    for d in range(2):
        target = i + 1 - 2 * d
        inside = (target >= 1) & (target <= n - 2)
        for s in range(n - 1):
            origin = i - s if d == 0 else i + s
            live = (origin >= 0) & (origin <= n - 1) & (target >= 0) & (target <= n - 1)

            @pl.when(live & inside)
            def _():
                sent(buf.at[0], fs.at[d, s])

            @pl.when(live & jnp.logical_not(inside))
            def _():
                sent(buf.at[0, pl.ds(0, (CHUNKS - moved) * cq)], fs.at[d, s])

    @pl.when(middle_layer)
    def _():
        drain(CHUNKS + moved)
        if moved:
            sent(outbox, xs.at[0])

    @pl.when(jnp.logical_not(middle_layer))
    def _():
        drain(CHUNKS - moved)
        if moved:
            sent(angb.at[pl.ds(0, moved * cq)], angs.at[0])
            sent(every.at[pl.ds(0, moved), 0, 0], ys.at[0])


def cs_extra(moved, total):
    return total * moved // (CHUNKS + moved)


def fused(n, moved, x, angle, window, u, v, plane, observed, tables, taps, plane_angle, shift):
    _, cols, _ = x.shape
    per, vis = u.shape
    subgrids = tables[1].shape[0] // 2
    rows = tables[0].shape[0] // 2
    block = rows // n
    pairs = cols // 2
    cq = cols // CHUNKS
    units = CHUNKS + moved
    slab = (cq // 2) * per
    lanes = 2 * rows
    vmem = pl.BlockSpec(memory_space=pltpu.VMEM)
    smem = pl.BlockSpec(memory_space=pltpu.SMEM)
    bf = lambda *shape: pltpu.VMEM(shape, jnp.bfloat16)
    f32 = lambda *shape: pltpu.VMEM(shape, jnp.float32)
    dma = lambda *shape: pltpu.SemaphoreType.DMA(shape)
    box = max(moved, 1)
    arrays = (x, angle, window, u, v, plane, observed, *tables)
    return pl.pallas_call(
        functools.partial(fused_kernel, n, moved),
        out_shape=(
            jax.ShapeDtypeStruct((per, 2, vis), jnp.float32),
            jax.ShapeDtypeStruct(x.shape, jnp.float32),
        ),
        in_specs=[pl.BlockSpec(memory_space=pltpu.HBM)] * 13 + [smem] * 3,
        out_specs=(pl.BlockSpec(memory_space=pltpu.HBM),) * 2,
        scratch_shapes=[
            *[pltpu.VMEM(a.shape, a.dtype) for a in arrays],
            bf(n, cols, 2, block, subgrids), bf(cq * units, rows, subgrids), f32(cq * units, 2, rows, subgrids),
            f32(2, subgrids, lanes), f32(2, 2 * cq * block, subgrids), f32(2 * cq * rows, subgrids),
            bf(units, 2, 4, 2, slab, lanes), bf(units, 4, 2, slab, lanes), bf(units, 4, 2, slab, lanes),
            bf(units, 3, 2, slab, lanes),
            bf(box, 2, slab, lanes), bf(box, 2, slab, lanes),
            f32(2, per * pairs, lanes), f32(2, per * pairs, lanes), f32(2, per, vis),
            f32(per, rows, vis), bf(per, cols, vis),
            bf(units, 2, 4, 2, slab, lanes), bf(n, cols, 2, block, subgrids),
            bf(2, n, cols, 2, block, subgrids), bf(2, n, cols, 2, block, subgrids), f32(2, cq * block, subgrids),
            dma(2, n - 1), dma(2, n - 1, CHUNKS), dma(1), dma(box),
            dma(1), dma(units), dma(3), dma(units, 3), dma(1), dma(box),
            dma(1), dma(box), dma(3), dma(units, 3), dma(1), dma(units),
            dma(2, n), dma(2, n - 1, CHUNKS), dma(13), dma(2),
            f32(per, 2, vis), f32(*x.shape),
        ],
        compiler_params=pltpu.CompilerParams(
            collective_id=2, has_side_effects=True, vmem_limit_bytes=60 * 1024 * 1024
        ),
        name="fused_column",
    )(*arrays, taps, plane_angle, shift)


def local(n, nf, model_strip, screen_angle, facet_window, facet_shift, kernel_taps, plane_angle, u_cell, v_cell, w_plane, observed):
    _, _, cols, length = screen_angle.shape
    per = u_cell.shape[1]
    subgrids = per * nf
    rows = length // subgrids
    block = rows // n
    vmem = pl.BlockSpec(memory_space=pltpu.VMEM)
    fr, fi = dft(rows)
    gr, gi = dft(subgrids)
    turn = 2.0 * np.pi * (np.arange(rows)[:, None] * np.arange(subgrids)[None, :] % length) / length
    twist = np.stack([np.cos(turn), -np.sin(turn)]).astype(np.float32)
    bf = lambda a: jnp.asarray(a.astype(np.float32)).astype(jnp.bfloat16)
    f1 = bf(np.block([[fr, -fi], [fi, fr]]))
    g1 = bf(np.block([[gr, -gi], [gi, gr]]))
    g2 = bf(np.block([[gr.T, gi.T], [-gi.T, gr.T]]))
    zero = np.zeros_like(fr)
    f2 = bf(
        np.block(
            [
                [fr.T, zero, fi.T, zero],
                [-fi.T, zero, fr.T, zero],
                [zero, fr.T, zero, fi.T],
                [zero, -fi.T, zero, fr.T],
            ]
        )
    )
    tw2 = np.ascontiguousarray(np.tile(np.swapaxes(twist, 1, 2), (1, 1, 2)))
    if nf == 8 and n == 4 and per % 16 == 0 and 2 * rows == subgrids == 128 and cols % (2 * CHUNKS) == 0:
        tables = (f1, g1, jnp.asarray(twist), g2, f2, jnp.asarray(tw2))
        residual, gradient = fused(
            n, MOVED, model_strip[0], screen_angle[0, 0], facet_window.reshape(length // subgrids, subgrids),
            u_cell[0], v_cell[0], w_plane[0], observed[0], tables, kernel_taps, plane_angle, facet_shift,
        )
        return (residual[None], gradient[None])
    factor = facet_factor(facet_window[0], facet_shift[0], subgrids)
    x = model_strip[0].reshape(2, cols, block, subgrids).transpose(1, 0, 2, 3)
    angle = screen_angle[0, 0].reshape(cols, rows, subgrids)
    contrib = pl.pallas_call(
        functools.partial(forward_kernel, n),
        out_shape=jax.ShapeDtypeStruct((2, cols // 2, subgrids, 2 * rows), jnp.bfloat16),
        in_specs=[vmem] * 6,
        out_specs=vmem,
        scratch_shapes=[
            pltpu.VMEM((n, cols, 2, block, subgrids), jnp.bfloat16),
            pltpu.SemaphoreType.DMA((2, n - 1, CHUNKS)),
            pltpu.SemaphoreType.DMA((2, n - 1, CHUNKS)),
            pltpu.SemaphoreType.DMA,
        ],
        compiler_params=pltpu.CompilerParams(collective_id=0, has_side_effects=True),
        name="gather_forward",
    )(x, angle, f1, g1, jnp.asarray(twist), factor)
    parts = contrib.reshape(2, cols // 2, nf, per, 2 * rows)
    received = lax.all_to_all(parts, "facet", split_axis=2, concat_axis=2, tiled=True)
    grids = jnp.sum(received.astype(jnp.float32), axis=2)
    grids = grids.reshape(2, cols // 2, per, 2, rows).transpose(2, 1, 3, 0, 4).reshape(per, cols, 2 * rows)
    residual, adjoint = middle(
        grids, u_cell[0], v_cell[0], w_plane[0], observed[0], plane_angle[0], kernel_taps, rows, cols
    )
    adjoint = adjoint.reshape(per, cols // 2, 2, 2, rows).transpose(3, 1, 0, 2, 4).reshape(2, cols // 2, per, 2 * rows)
    every = lax.all_gather(adjoint, "facet", axis=2, tiled=True)
    gradient = pl.pallas_call(
        functools.partial(backward_kernel, n),
        out_shape=jax.ShapeDtypeStruct((cols, 2, block, subgrids), jnp.float32),
        in_specs=[vmem] * 6,
        out_specs=vmem,
        scratch_shapes=[
            pltpu.VMEM((n, cols, 2, block, subgrids), jnp.bfloat16),
            pltpu.VMEM((2, n, cols, 2, block, subgrids), jnp.bfloat16),
            pltpu.VMEM((2, n, cols, 2, block, subgrids), jnp.bfloat16),
            pltpu.SemaphoreType.DMA((2, n, CHUNKS)),
            pltpu.SemaphoreType.DMA((2, n, CHUNKS)),
        ],
        compiler_params=pltpu.CompilerParams(collective_id=1, has_side_effects=True),
        name="backward_scatter",
    )(every, angle, g2, f2, jnp.asarray(tw2), factor)
    gradient = gradient.transpose(1, 0, 2, 3).reshape(1, 2, cols, block * subgrids)
    return (residual[None], gradient)


def solution(mesh):
    return jax.shard_map(
        functools.partial(local, mesh.shape["layer"], mesh.shape["facet"]),
        mesh=mesh,
        in_specs=(
            P("facet", None, None, "layer"),
            P("layer", "facet", None, None),
            P("facet", None),
            P("facet"),
            P(),
            P("layer", None),
            P("layer", "facet", None),
            P("layer", "facet", None),
            P("layer", "facet", None),
            P("layer", "facet", None, None),
        ),
        out_specs=(P("layer", "facet", None, None), P("facet", None, None, "layer")),
        check_vma=False,
    )
```
